32 devices in a mesh: dp: 8 (over z, y), fsdp: 4 (over x, core).
Axes of the slice: x: 2, y: 2, z: 4, core: 2. Of those that a mesh axis runs over, the one named last changes fastest.
Arguments:
- tokens: bfloat16 [8192, 768], P(('dp', 'fsdp')), may hold values from -6 to 6
- out_grad: bfloat16 [8192, 768], P(('dp', 'fsdp')), may hold values from -6 to 6
- mlm_mask: int32 [8192], P(('dp', 'fsdp')), may hold values 0 or 1
- live_mask: int32 [8192], P(('dp', 'fsdp')), may hold values 0 or 1
- doc_lengths: int32 [64, 4], P(('dp', 'fsdp')), may hold values from 1 to 64, 128 in all within a row
- layout_buckets: int32 [2, 8192, 128], P(None, ('dp', 'fsdp')), may hold values from 0 to 31
- attn_in: bfloat16 [2, 768, 2304], P(None, 'fsdp'), may hold values from -0.21875 to 0.21875
- attn_out: bfloat16 [2, 768, 768], P(None, 'fsdp'), may hold values from -0.875 to 0.875
- ffn_in: bfloat16 [2, 768, 3072], P(None, 'fsdp'), may hold values from -0.21875 to 0.21875
- ffn_out: bfloat16 [2, 3072, 768], P(None, 'fsdp'), may hold values from -0.109375 to 0.109375
- biases: bfloat16 [2, 6, 768], P(None, None, 'fsdp'), may hold values from -1 to 1
- ffn_in_bias: bfloat16 [2, 3072], P(None, 'fsdp'), may hold values from -1 to 1
- gains: bfloat16 [2, 2, 768], P(None, None, 'fsdp'), may hold values from 0.5 to 1.5
- tables: bfloat16 [2, 3, 32, 12], P(None, None, 'fsdp'), may hold values from -4 to 4
Outputs:
- layer_out: bfloat16 [2, 8192, 768], P(None, ('dp', 'fsdp'))
- input_grad: float32 [8192, 768], P(('dp', 'fsdp'))
- grad_attn_in: float32 [2, 768, 2304], P(None, 'fsdp')
- grad_attn_out: float32 [2, 768, 768], P(None, 'fsdp')
- grad_ffn_in: float32 [2, 768, 3072], P(None, 'fsdp')
- grad_ffn_out: float32 [2, 3072, 768], P(None, 'fsdp')
- grad_biases: float32 [2, 6, 768], P(None, None, 'fsdp')
- grad_ffn_in_bias: float32 [2, 3072], P(None, 'fsdp')
- grad_gains: float32 [2, 2, 768], P(None, None, 'fsdp')
- grad_tables: float32 [2, 3, 32, 12], P(None, None, 'fsdp')
The draws below stay inside these ranges and needn't reach their ends.
Inputs may be any that keep to these rules, and one draw needn't show every extreme that they name: `doc_lengths`: the 4 lengths of each window sum to 128. `live_mask`: 1 marks a real token, 0 padding. `mlm_mask`: 1 marks a position whose output receives a gradient.
All inputs are finite; a program needn't handle non-finite values. No bound on the sum of `mlm_mask` or of `live_mask` on one device may be relied on, other than what follows from the above.
Results may differ from the reference program's by a relative error of at most 0.025.
Values may be sent and summed in bfloat16 or wider, within the bound.
A program may use at most 256 MiB of HBM per device.

```python
import math
import jax
import jax.numpy as jnp
import numpy as np
from jax import lax

D = 768
H = 12
DH = 64
FF = 3072
NB = 32
WIN = 128
DOCS = 4
LAYERS = 2
WINDOWS = 64
TOKENS = 8192


def with_ends(values, stream_key, smallest, top_value):
    index_at = [jax.random.randint(jax.random.fold_in(stream_key, axis), (), 0, length) for axis, length in enumerate(values.shape)]
    longest = values.shape.index(max(values.shape))
    next_to = index_at[:longest] + [(index_at[longest] + 1) % values.shape[longest]] + index_at[longest + 1:]
    return values.at[tuple(index_at)].set(smallest).at[tuple(next_to)].set(top_value)


def levels(key, shape, shards, low, largest):
    def one(dim, blocks):
        draws = jax.random.uniform(jax.random.fold_in(jax.random.fold_in(key, 6), dim), (blocks,), jnp.float32, low / len(shards), largest / len(shards))
        return jnp.repeat(jnp.exp(draws), shape[dim] // blocks).reshape((-1,) + (1,) * (len(shape) - dim - 1))

    gain = one(*shards[0])
    for cut in shards[1:]:
        gain = gain * one(*cut)
    return gain


def length_profile(number_of, total, reach, lean):
    portions = [(1 << 20) // math.isqrt(standing ** lean) + 1 for standing in range(2, number_of + 1)]
    rest, counts = total - reach - (number_of - 1), [1] * (number_of - 1)
    while rest > 0:
        free = [i for i in range(number_of - 1) if counts[i] < reach]
        mass, left = sum([portions[i] for i in free]), rest
        for i in free:
            extra = min(reach - counts[i], max(1, left * portions[i] // mass), rest)
            counts[i] = counts[i] + extra
            rest = rest - extra
    return np.array([reach] + counts)


def uneven_parts(key, amount, total, reach, skew):
    if amount == 2:
        one = jax.random.randint(key, (), max(1, total - reach), min(reach, total - 1) + 1)
        return jnp.stack([one, total - one])
    lengths = jnp.asarray(length_profile(amount, total, reach, skew), jnp.int32)
    pairs = (amount - 1) // 2
    donor, receiver = lengths[1:1 + 2 * pairs:2], lengths[2:2 + 2 * pairs:2]
    room = jnp.minimum(donor - 1, reach - receiver)
    moved = jax.random.randint(jax.random.fold_in(key, 1), (pairs,), 0, 1 << 20) % (room + 1)
    lengths = lengths.at[1:1 + 2 * pairs:2].set(donor - moved).at[2:2 + 2 * pairs:2].set(receiver + moved)
    return lengths[jax.random.permutation(jax.random.fold_in(key, 2), amount)]


def normal_values(rng, shape, scale, reach, shards=(), kind=jnp.bfloat16):
    array = jax.random.normal(rng, shape, jnp.float32) * scale
    if len(shards) > 0:
        array = levels(rng, shape, shards, -0.22, 0.18) * array
    return jnp.clip(array, min=-reach, max=reach).astype(kind)


def setup_inputs(seed: int = 0) -> dict:
    key_list = jax.random.split(jax.random.key(seed), 15)
    return {
        "tokens": normal_values(key_list[0], (TOKENS, D), 1.0, 6.0, ((0, 32),)),
        "out_grad": normal_values(key_list[1], (TOKENS, D), 1.0, 6.0, ((0, 32),)),
        "mlm_mask": with_ends((jax.random.randint(key_list[2], (TOKENS,), 0, 20) < 3).astype(jnp.int32), jax.random.fold_in(key_list[2], 1), 0, 1),
        "live_mask": with_ends((jax.random.randint(key_list[3], (TOKENS,), 0, 8) < 7).astype(jnp.int32), jax.random.fold_in(key_list[3], 1), 0, 1),
        "doc_lengths": jax.vmap(lambda own: uneven_parts(own, DOCS, WIN, WIN // 2, 2))(jax.random.split(key_list[4], WINDOWS)).reshape((WINDOWS, DOCS)).astype(jnp.int32),
        "layout_buckets": with_ends(jax.random.randint(key_list[5], (2, TOKENS, WIN), 0, NB), jax.random.fold_in(key_list[5], 1), 0, NB - 1).astype(jnp.int32),
        "attn_in": normal_values(key_list[6], (LAYERS, D, 3 * D), D ** -0.5, 0.21875, ((1, 4),)),
        "attn_out": normal_values(key_list[7], (LAYERS, D, D), (D // 16) ** -0.5, 0.875, ((1, 4),)),
        "ffn_in": normal_values(key_list[8], (LAYERS, D, FF), D ** -0.5, 0.21875, ((1, 4),)),
        "ffn_out": normal_values(key_list[9], (LAYERS, FF, D), FF ** -0.5, 0.109375, ((1, 4),)),
        "biases": normal_values(key_list[10], (LAYERS, 6, D), 0.2, 1.0, ((2, 4),)),
        "ffn_in_bias": normal_values(key_list[11], (LAYERS, FF), 0.2, 1.0, ((1, 4),)),
        "gains": jnp.clip(1.0 + 0.1 * jax.random.normal(key_list[12], (LAYERS, 2, D), jnp.float32), 0.5, 1.5).astype(jnp.bfloat16),
        "tables": normal_values(key_list[13], (LAYERS, 3, NB, H), 1.0, 4.0, ((2, 4),)),
    }


@jax.custom_vjp
def low(v):
    return lax.optimization_barrier(v.astype(jnp.bfloat16)).astype(jnp.float32)

@jax.custom_vjp
def low_back(v):
    return v

def low_keep(v):
    return (low(v), None)

def low_pass(kept, grad):
    return (grad,)

def back_keep(v):
    return (v, None)

def back_low(kept, grad):
    return (low(grad),)
low.defvjp(low_keep, low_pass)
low_back.defvjp(back_keep, back_low)

def exact_gelu(values):
    return jax.nn.gelu(values, approximate=False)

def matmul(left, right):
    return jnp.dot(left, right, precision=lax.Precision.HIGHEST)

def layer_norm(values, gain_row, shift_row):
    centre = values - lax.optimization_barrier(jnp.mean(values, axis=-1, keepdims=True))
    spread = lax.optimization_barrier(jnp.mean(centre * centre, axis=-1, keepdims=True))
    return centre * lax.rsqrt(spread + 1e-05) * gain_row + shift_row

def pair_bias(bias_table, layout_rows):
    positions = jnp.arange(WIN, dtype=jnp.int32)
    offset = jnp.clip(positions[None, :] - positions[:, None], -(NB // 2), NB // 2 - 1) + NB // 2
    linear = bias_table[0][offset]
    across = bias_table[1][layout_rows[0]] + bias_table[2][layout_rows[1]]
    return jnp.transpose(linear[None] + across, (0, 3, 1, 2))

def one_layer(inputs, weights, pair_mask, layout_rows):
    w_in, w_out, w_up, w_down, shifts, up_shift, gain_rows, bias_table = weights
    windows = inputs.shape[0] // WIN
    scaling = DH ** (-0.5)
    projected = matmul(inputs, w_in)
    query_rows = low(low_back((projected[:, :D] + shifts[0]) * scaling)).reshape(windows, WIN, H, DH)
    key_rows = low(low_back(projected[:, D:2 * D])).reshape(windows, WIN, H, DH)
    value_rows = low(low_back(projected[:, 2 * D:] + shifts[1])).reshape(windows, WIN, H, DH)
    scores = jnp.einsum('wihd,wjhd->whij', query_rows, key_rows, precision=lax.Precision.HIGHEST)
    scores = scores + pair_bias(bias_table, layout_rows)
    scores = low_back(jnp.where(pair_mask[:, None] > 0, scores, -1e+30))
    highest = lax.optimization_barrier(jnp.max(scores, axis=-1, keepdims=True))
    exponent = jnp.exp(scores - highest)
    probs = low(exponent / lax.optimization_barrier(jnp.sum(exponent, axis=-1, keepdims=True)))
    mixed_rows = jnp.einsum('whij,wjhd->wihd', probs, value_rows, precision=lax.Precision.HIGHEST)
    mixed_rows = low(low_back(mixed_rows.reshape(windows * WIN, D)))
    attended = low_back(matmul(mixed_rows, w_out) + shifts[2])
    first_norm = layer_norm(inputs + attended, gain_rows[0], shifts[3])
    hidden = low_back(matmul(low(first_norm), w_up) + up_shift)
    active = low(exact_gelu(hidden))
    branch = low_back(matmul(active, w_down) + shifts[4])
    return layer_norm(first_norm + branch, gain_rows[1], shifts[5])

def stack_layers(inputs, params, pair_mask, layout_rows):
    results = []
    current = inputs
    for layer_index in range(LAYERS):
        weights = tuple((array_item[layer_index] for array_item in params))
        result = one_layer(current, weights, pair_mask, layout_rows)
        results.append(result)
        if layer_index + 1 < LAYERS:
            current = low(result)
    return jnp.stack(results)

def reference(tokens, out_grad, mlm_mask, live_mask, doc_lengths, layout_buckets, attn_in, attn_out, ffn_in, ffn_out, biases, ffn_in_bias, gains, tables):
    windows = TOKENS // WIN
    group_size = math.gcd(windows, max(1, 4096 // WIN))
    group_count = windows // group_size
    positions = jnp.arange(WIN, dtype=jnp.int32)
    doc_ends = jnp.cumsum(doc_lengths, axis=1)
    document = lax.optimization_barrier(jnp.sum((positions[None, :, None] >= doc_ends[:, None, :]).astype(jnp.int32), axis=2))
    live_rows = live_mask.reshape(windows, WIN) == 1
    diagonal = positions[:, None] == positions[None, :]
    pair_mask = ((document[:, :, None] == document[:, None, :]) & (live_rows[:, None, :] | diagonal[None])).astype(jnp.int32)
    pair_mask = pair_mask.reshape(group_count, group_size, WIN, WIN)
    layout_rows = jnp.moveaxis(layout_buckets.reshape(2, group_count, group_size, WIN, WIN), 1, 0)
    first_input = tokens.astype(jnp.float32).reshape(group_count, group_size * WIN, D)
    params = tuple((array_item.astype(jnp.float32) for array_item in (attn_in, attn_out, ffn_in, ffn_out, biases, ffn_in_bias, gains, tables)))

    def forward(start_values, param_values):

        def run(group_item):
            group_input, group_mask, group_layout = group_item
            return jax.checkpoint(stack_layers)(group_input, param_values, group_mask, group_layout)
        return lax.map(run, (start_values, pair_mask, layout_rows))
    layer_values, pullback = jax.vjp(forward, first_input, params)
    last_grad = out_grad.astype(jnp.float32) * mlm_mask.astype(jnp.float32)[:, None]
    last_grad = last_grad.reshape(group_count, 1, group_size * WIN, D)
    earlier = jnp.zeros((group_count, LAYERS - 1, group_size * WIN, D), jnp.float32)
    cotangent = jnp.concatenate([earlier, last_grad], axis=1)
    grad_start, grad_params = pullback(cotangent)
    layer_out = jnp.moveaxis(layer_values, 1, 0).reshape(LAYERS, TOKENS, D).astype(jnp.bfloat16)
    input_grad = grad_start.reshape(TOKENS, D)
    return (layer_out, input_grad, grad_params[0], grad_params[1], grad_params[2], grad_params[3], grad_params[4], grad_params[5], grad_params[6], grad_params[7])
```

```python
import functools

import jax
import jax.numpy as jnp
from jax import lax
from jax.experimental import pallas as pl
from jax.experimental.pallas import tpu as pltpu
from jax.sharding import PartitionSpec as P

H = 12
DH = 64
NB = 32
WIN = 128


EPSILON = 1e-05
LAG = 2


def exact_gelu(values):
    return jax.nn.gelu(values, approximate=False)


def norm_forward(values, gain_row, shift_row):
    centre = values - jnp.mean(values, axis=-1, keepdims=True)
    spread = jnp.mean(centre * centre, axis=-1, keepdims=True)
    inverse = lax.rsqrt(spread + EPSILON)
    normed = centre * inverse
    return (normed * gain_row + shift_row, normed, inverse)


def norm_backward(incoming, normed, inverse, gain_row):
    scaled = incoming * gain_row
    centred = (
        scaled
        - jnp.mean(scaled, axis=-1, keepdims=True)
        - normed * jnp.mean(scaled * normed, axis=-1, keepdims=True)
    )
    return (centred * inverse, jnp.sum(incoming * normed, axis=0), jnp.sum(incoming, axis=0))


def geometry(doc_lengths, live_mask, layout_buckets):
    windows = doc_lengths.shape[0]
    positions = jnp.arange(WIN, dtype=jnp.int32)
    doc_ends = jnp.cumsum(doc_lengths, axis=1)
    document = jnp.sum((positions[None, :, None] >= doc_ends[:, None, :]).astype(jnp.int32), axis=2)
    live_rows = live_mask.reshape(windows, WIN) == 1
    diagonal = positions[:, None] == positions[None, :]
    pair_mask = (document[:, :, None] == document[:, None, :]) & (
        live_rows[:, None, :] | diagonal[None]
    )
    offset = jnp.clip(positions[None, :] - positions[:, None], -(NB // 2), NB // 2 - 1) + NB // 2
    buckets = jnp.arange(NB, dtype=jnp.int32)
    linear = (offset[None] == buckets[:, None, None]).astype(jnp.bfloat16)
    layout_rows = layout_buckets.reshape(2, windows, WIN, WIN)
    across = (layout_rows[:, :, None] == buckets[None, None, :, None, None]).astype(jnp.bfloat16)
    return (pair_mask, linear, across)


def pair_terms_of(bias_table, linear, across):
    terms = jnp.einsum("bij,bh->hij", linear, bias_table[0], preferred_element_type=jnp.float32)[
        None
    ]
    terms = terms + jnp.einsum(
        "wbij,bh->whij", across[0], bias_table[1], preferred_element_type=jnp.float32
    )
    return terms + jnp.einsum(
        "wbij,bh->whij", across[1], bias_table[2], preferred_element_type=jnp.float32
    )


def masked_scores(query_rows, key_rows, pair_terms, pair_mask):
    scores = (
        jnp.einsum("wihd,wjhd->whij", query_rows, key_rows, preferred_element_type=jnp.float32)
        + pair_terms
    )
    return jnp.where(pair_mask[:, None], scores, -1e30)


def fetch_forward(w_in, w_out, w_up, w_down, shifts, up_shift, gain_rows, bias_table):
    return (
        lax.all_gather(w_in, "fsdp", axis=0, tiled=True),
        lax.all_gather(w_out, "fsdp", axis=0, tiled=True),
        lax.all_gather(w_up, "fsdp", axis=0, tiled=True),
        lax.all_gather(w_down, "fsdp", axis=0, tiled=True),
        lax.all_gather(shifts, "fsdp", axis=1, tiled=True),
        lax.all_gather(up_shift, "fsdp", axis=0, tiled=True),
        lax.all_gather(gain_rows, "fsdp", axis=1, tiled=True),
        lax.all_gather(bias_table, "fsdp", axis=1, tiled=True),
    )


def layer_forward(inputs, weights, pair_mask, linear, across):
    w_in, w_out, w_up, w_down, shifts, up_shift, gain_rows, bias_table = weights
    shifts = shifts.astype(jnp.float32)
    gain_rows = gain_rows.astype(jnp.float32)
    rows = inputs.shape[0]
    windows = rows // WIN
    width = w_out.shape[0]
    scaling = DH ** (-0.5)
    projected = jnp.dot(inputs, w_in, preferred_element_type=jnp.float32)
    query_rows = (
        ((projected[:, :width] + shifts[0]) * scaling)
        .astype(jnp.bfloat16)
        .reshape(windows, WIN, H, DH)
    )
    key_rows = projected[:, width : 2 * width].astype(jnp.bfloat16).reshape(windows, WIN, H, DH)
    value_rows = (
        (projected[:, 2 * width :] + shifts[1]).astype(jnp.bfloat16).reshape(windows, WIN, H, DH)
    )
    pair_terms = pair_terms_of(bias_table, linear, across)
    scores = masked_scores(query_rows, key_rows, pair_terms, pair_mask)
    highest = jnp.max(scores, axis=-1, keepdims=True)
    exponent = jnp.exp(scores - highest)
    denominator = jnp.sum(exponent, axis=-1, keepdims=True)
    probs = exponent / denominator
    log_total = highest + jnp.log(denominator)
    mixed_rows = jnp.einsum(
        "whij,wjhd->wihd",
        probs.astype(jnp.bfloat16),
        value_rows,
        preferred_element_type=jnp.float32,
    )
    mixed_rows = mixed_rows.reshape(rows, width).astype(jnp.bfloat16)
    attended = jnp.dot(mixed_rows, w_out, preferred_element_type=jnp.float32) + shifts[2]
    first_norm, normed_first, inverse_first = norm_forward(
        inputs.astype(jnp.float32) + attended, gain_rows[0], shifts[3]
    )
    first_low = first_norm.astype(jnp.bfloat16)
    hidden = jnp.dot(first_low, w_up, preferred_element_type=jnp.float32) + up_shift.astype(
        jnp.float32
    )
    active = exact_gelu(hidden).astype(jnp.bfloat16)
    branch = jnp.dot(active, w_down, preferred_element_type=jnp.float32) + shifts[4]
    result, normed_second, inverse_second = norm_forward(
        first_norm + branch, gain_rows[1], shifts[5]
    )
    kept = (
        query_rows,
        key_rows,
        value_rows,
        pair_terms,
        log_total,
        mixed_rows,
        normed_first,
        inverse_first,
        first_low,
        hidden,
        active,
        normed_second,
        inverse_second,
    )
    return (result, kept)


def layer_backward(incoming, inputs, weights, kept, pair_mask, linear, across):
    w_in, w_out, w_up, w_down, shifts, up_shift, gain_rows, bias_table = weights
    gain_rows = gain_rows.astype(jnp.float32)
    (
        query_rows,
        key_rows,
        value_rows,
        pair_terms,
        log_total,
        mixed_rows,
        normed_first,
        inverse_first,
        first_low,
        hidden,
        active,
        normed_second,
        inverse_second,
    ) = kept
    rows = inputs.shape[0]
    width = w_out.shape[0]
    windows = rows // WIN
    scaling = DH ** (-0.5)
    grad_second, grad_gain_second, grad_shift_second = norm_backward(
        incoming, normed_second, inverse_second, gain_rows[1]
    )
    branch_low = grad_second.astype(jnp.bfloat16)
    grad_down = jnp.einsum("nf,nd->fd", active, branch_low, preferred_element_type=jnp.float32)
    grad_branch_shift = jnp.sum(branch_low.astype(jnp.float32), axis=0)
    grad_active = jnp.einsum("nd,fd->nf", branch_low, w_down, preferred_element_type=jnp.float32)
    hidden_low = jax.vjp(exact_gelu, hidden)[1](grad_active)[0].astype(jnp.bfloat16)
    grad_up = jnp.einsum("nd,nf->df", first_low, hidden_low, preferred_element_type=jnp.float32)
    grad_up_shift = jnp.sum(hidden_low.astype(jnp.float32), axis=0)
    grad_first = grad_second + jnp.einsum(
        "nf,df->nd", hidden_low, w_up, preferred_element_type=jnp.float32
    )
    grad_attended, grad_gain_first, grad_shift_first = norm_backward(
        grad_first, normed_first, inverse_first, gain_rows[0]
    )
    attended_low = grad_attended.astype(jnp.bfloat16)
    grad_out_weight = jnp.einsum(
        "nd,ne->de", mixed_rows, attended_low, preferred_element_type=jnp.float32
    )
    grad_attended_shift = jnp.sum(attended_low.astype(jnp.float32), axis=0)
    grad_mixed = jnp.einsum("ne,de->nd", attended_low, w_out, preferred_element_type=jnp.float32)
    grad_mixed = grad_mixed.astype(jnp.bfloat16).reshape(windows, WIN, H, DH)
    scores = masked_scores(query_rows, key_rows, pair_terms, pair_mask)
    probs = jnp.exp(scores - log_total)
    grad_probs = jnp.einsum(
        "wihd,wjhd->whij", grad_mixed, value_rows, preferred_element_type=jnp.float32
    )
    grad_value = jnp.einsum(
        "whij,wihd->wjhd",
        probs.astype(jnp.bfloat16),
        grad_mixed,
        preferred_element_type=jnp.float32,
    ).astype(jnp.bfloat16)
    grad_scores = (
        probs * (grad_probs - jnp.sum(probs * grad_probs, axis=-1, keepdims=True))
    ).astype(jnp.bfloat16)
    grad_query = (
        jnp.einsum(
            "whij,wjhd->wihd", grad_scores, key_rows, preferred_element_type=jnp.float32
        ).astype(jnp.bfloat16)
        * scaling
    )
    grad_key = jnp.einsum(
        "whij,wihd->wjhd", grad_scores, query_rows, preferred_element_type=jnp.float32
    ).astype(jnp.bfloat16)
    grad_qkv = jnp.concatenate(
        [
            grad_query.reshape(rows, width),
            grad_key.reshape(rows, width),
            grad_value.reshape(rows, width),
        ],
        axis=1,
    )
    grad_in_weight = jnp.einsum("nd,ne->de", inputs, grad_qkv, preferred_element_type=jnp.float32)
    grad_linear = jnp.einsum(
        "bij,whij->bh", linear, grad_scores, preferred_element_type=jnp.float32
    )
    grad_across_x = jnp.einsum(
        "wbij,whij->bh", across[0], grad_scores, preferred_element_type=jnp.float32
    )
    grad_across_y = jnp.einsum(
        "wbij,whij->bh", across[1], grad_scores, preferred_element_type=jnp.float32
    )
    grad_table = jnp.stack([grad_linear, grad_across_x, grad_across_y])
    grad_inputs = grad_attended + jnp.einsum(
        "ne,de->nd", grad_qkv, w_in, preferred_element_type=jnp.float32
    )
    grad_query_shift = jnp.sum(grad_query.reshape(rows, width).astype(jnp.float32), axis=0)
    grad_value_shift = jnp.sum(grad_value.reshape(rows, width).astype(jnp.float32), axis=0)
    grad_shifts = jnp.stack(
        [
            grad_query_shift,
            grad_value_shift,
            grad_attended_shift,
            grad_shift_first,
            grad_branch_shift,
            grad_shift_second,
        ]
    )
    grad_gain_rows = jnp.stack([grad_gain_first, grad_gain_second])
    grads = (
        grad_in_weight,
        grad_out_weight,
        grad_up,
        grad_down,
        grad_shifts,
        grad_up_shift,
        grad_gain_rows,
        grad_table,
    )
    return (grad_inputs, grads)


MESH = pl.DeviceIdType.MESH
CHUNK_TILES = 1


def add_rows(target, other):
    target[...] = (target[...].astype(jnp.float32) + other[...].astype(jnp.float32)).astype(
        jnp.bfloat16
    )


def reduce_kernel(
    high, count, grads, out, own, core_in, x_in, y_in, z_in, full, load_sem, core_sem,
    x_sem, y_sem, z_sem, zg_sem, yg_sem, sent, out_sem,
):
    dp = lax.axis_index("dp")
    shard = lax.axis_index("fsdp")
    y_at, z_at = lax.rem(dp, 2), lax.div(dp, 2)
    x_at, core = lax.div(shard, 2), lax.rem(shard, 2)
    core_peer = (dp, x_at * 2 + 1 - core)
    x_peer = (dp, (1 - x_at) * 2 + core)
    y_peer = (z_at * 2 + 1 - y_at, shard)
    z_of = [lax.rem(z_at + step, high) for step in range(high)]
    z_from = [lax.rem(z_at + high - step, high) for step in range(high)]
    z_peers = [(z_of[step] * 2 + y_at, shard) for step in range(high)]
    chunk = own.shape[2]
    half = chunk // 2
    piece = half // high

    barrier = pltpu.get_barrier_semaphore()
    peers = [core_peer, x_peer, y_peer] + z_peers[1:]
    for peer in peers:
        pl.semaphore_signal(barrier, inc=1, device_id=peer, device_id_type=MESH)
    pl.semaphore_wait(barrier, len(peers))

    def remote(source, target, send_at, receive, peer):
        return pltpu.make_async_remote_copy(
            src_ref=source, dst_ref=target, send_sem=sent.at[send_at], recv_sem=receive,
            device_id=peer, device_id_type=MESH,
        )

    def rows_of(k, wanted):
        return grads.at[wanted, pl.ds(pl.multiple_of(k * chunk, chunk), chunk), :]

    def load(k, j):
        wanted = (x_at if j == 0 else 1 - x_at) * 2 + core
        return pltpu.make_async_copy(rows_of(k, wanted), own.at[k, j], load_sem.at[k, j])

    def core_send(k, j):
        wanted = (x_at if j == 0 else 1 - x_at) * 2 + 1 - core
        return remote(rows_of(k, wanted), core_in.at[k, j], 0, core_sem.at[k, j], core_peer)

    def x_send(k):
        return remote(own.at[k, 1], x_in.at[k], 1, x_sem.at[k], x_peer)

    def y_rows(side):
        return pl.ds(pl.multiple_of(side * half, half), half)

    def y_send(k):
        return remote(own.at[k, 0, y_rows(1 - y_at)], y_in.at[k], 2, y_sem.at[k], y_peer)

    def z_rows(at):
        return pl.ds(pl.multiple_of(y_at * half + at * piece, piece), piece)

    def z_send(k, step):
        return remote(
            own.at[k, 0, z_rows(z_of[step])], z_in.at[k, step - 1], 3,
            z_sem.at[k, step - 1], z_peers[step],
        )

    def zg_send(k, step):
        mine = full.at[k, z_rows(z_at)]
        return remote(mine, mine, 4, zg_sem.at[k, step - 1], z_peers[step])

    def zg_arrival(k, step):
        theirs = full.at[k, z_rows(z_from[step])]
        return remote(theirs, theirs, 4, zg_sem.at[k, step - 1], z_peers[step])

    def yg_send(k):
        mine = full.at[k, y_rows(y_at)]
        return remote(mine, mine, 5, yg_sem.at[k], y_peer)

    def store(k):
        return pltpu.make_async_copy(
            full.at[k], out.at[pl.ds(pl.multiple_of(k * chunk, chunk), chunk), :], out_sem.at[k]
        )

    @pl.loop(0, count)
    def _(k):
        for j in (1, 0):
            core_send(k, j).start()
            load(k, j).start()

    def stage_core(k):
        for j in (1, 0):
            load(k, j).wait()
            core_send(k, j).wait_recv()
            add_rows(own.at[k, j], core_in.at[k, j])
            if j == 1:
                x_send(k).start()

    def stage_x(k):
        x_send(k).wait_recv()
        add_rows(own.at[k, 0], x_in.at[k])
        y_send(k).start()

    def stage_y(k):
        y_send(k).wait_recv()
        add_rows(own.at[k, 0, y_rows(y_at)], y_in.at[k])
        for step in range(1, high):
            z_send(k, step).start()

    def stage_z(k):
        total = own[k, 0, z_rows(z_at), :].astype(jnp.float32)
        for step in range(1, high):
            z_send(k, step).wait_recv()
            total = total + z_in[k, step - 1].astype(jnp.float32)
        full[k, z_rows(z_at), :] = total.astype(jnp.bfloat16)
        for step in range(1, high):
            zg_send(k, step).start()

    def stage_spread(k):
        for step in range(1, high):
            zg_arrival(k, step).wait_recv()
        yg_send(k).start()

    def stage_store(k):
        yg_send(k).wait_recv()
        store(k).start()

    stages = (stage_core, stage_x, stage_y, stage_z, stage_spread, stage_store)
    lags = (0, LAG, 2 * LAG, 3 * LAG, 4 * LAG, 5 * LAG)

    @pl.loop(0, count + lags[-1])
    def _(t):
        for stage, lag in zip(stages, lags):
            k = t - lag

            @pl.when((k >= 0) & (k < count))
            def _():
                stage(k)

    def all_sent(source, target, send_at, peer):
        remote(source, target, send_at, x_sem.at[0], peer).wait_send()

    all_sent(own, core_in, 0, core_peer)
    all_sent(x_in, x_in, 1, x_peer)
    all_sent(y_in, y_in, 2, y_peer)
    all_sent(z_in, z_in, 3, z_peers[1])
    all_sent(z_in, z_in, 4, z_peers[1])
    all_sent(y_in, y_in, 5, y_peer)

    @pl.loop(0, count)
    def _(k):
        store(k).wait()


def reduce_gradients(grads, group):
    shards, rows, width = grads.shape
    high = group // 2
    chunk = chunk_rows(group)
    count = rows // chunk
    piece = chunk // group
    buffers = [
        (count, 2, chunk, width),
        (count, 2, chunk, width),
        (count, chunk, width),
        (count, chunk // 2, width),
        (count, high - 1, piece, width),
        (count, chunk, width),
    ]
    semaphores = [(count, 2), (count, 2), (count,), (count,), (count, high - 1),
                  (count, high - 1), (count,), (6,), (count,)]
    return pl.pallas_call(
        functools.partial(reduce_kernel, high, count),
        out_shape=jax.ShapeDtypeStruct((rows, width), jnp.bfloat16),
        in_specs=[pl.BlockSpec(memory_space=pltpu.MemorySpace.HBM)],
        out_specs=pl.BlockSpec(memory_space=pltpu.MemorySpace.HBM),
        scratch_shapes=[pltpu.VMEM(shape, jnp.bfloat16) for shape in buffers]
        + [pltpu.SemaphoreType.DMA(shape) for shape in semaphores],
        compiler_params=pltpu.CompilerParams(
            collective_id=1, has_side_effects=True, vmem_limit_bytes=64 * 1024 * 1024 - 65536
        ),
    )(grads)


def chunk_rows(group):
    return 16 * CHUNK_TILES * group


def pack_gradients(grad_list, shards, group):
    blocks, smalls = [], []
    for grads in grad_list:
        w_in, w_out, w_up, w_down, shifts, up_shift, gain_rows, bias_table = grads
        width = w_out.shape[1]
        for member in (w_in, w_out, w_up, w_down):
            member = member.astype(jnp.bfloat16)
            depth = member.shape[0] // shards
            member = member.reshape(shards, depth, member.shape[1] // width, width)
            blocks.append(jnp.swapaxes(member, 1, 2).reshape(shards, -1, width))
        smalls.append(jnp.swapaxes(shifts.reshape(6, shards, -1), 0, 1).reshape(shards, -1))
        smalls.append(up_shift.reshape(shards, -1))
        smalls.append(jnp.swapaxes(gain_rows.reshape(2, shards, -1), 0, 1).reshape(shards, -1))
        smalls.append(jnp.swapaxes(bias_table.reshape(3, shards, -1), 0, 1).reshape(shards, -1))
    small = jnp.concatenate(smalls, axis=1)
    rows = sum(block.shape[1] for block in blocks)
    chunk = chunk_rows(group)
    total = -(-(rows + -(-small.shape[1] // width)) // chunk) * chunk
    small = jnp.pad(small, ((0, 0), (0, (total - rows) * width - small.shape[1])))
    blocks.append(small.reshape(shards, total - rows, width).astype(jnp.bfloat16))
    return jnp.concatenate(blocks, axis=1), (len(grad_list), rows, shards)


def unpack_gradients(reduced, shapes):
    layers, rows, shards = shapes
    width = reduced.shape[1]
    per_layer = rows // layers
    depth = width // shards
    body = reduced[:rows].astype(jnp.float32).reshape(layers, per_layer, width)
    spans = []
    start = 0
    for blocks in (3, 1, 4):
        part = body[:, start : start + blocks * depth].reshape(layers, blocks, depth, width)
        spans.append(jnp.swapaxes(part, 1, 2).reshape(layers, depth, blocks * width))
        start += blocks * depth
    spans.append(body[:, start:])
    small = reduced[rows:].astype(jnp.float32).reshape(-1)
    sizes = (6 * depth, width, 2 * depth, 3 * (NB // shards) * H)
    small = small[: layers * sum(sizes)].reshape(layers, -1)
    forms = ((6, depth), (width,), (2, depth), (3, NB // shards, H))
    start = 0
    for size, form in zip(sizes, forms):
        spans.append(small[:, start : start + size].reshape((layers,) + form))
        start += size
    return tuple(spans)


def local(
    tokens,
    out_grad,
    mlm_mask,
    live_mask,
    doc_lengths,
    layout_buckets,
    attn_in,
    attn_out,
    ffn_in,
    ffn_out,
    biases,
    ffn_in_bias,
    gains,
    tables,
):
    pair_mask, linear, across = geometry(doc_lengths, live_mask, layout_buckets)
    layer_total = attn_in.shape[0]
    current = tokens
    layer_inputs = []
    kept_list = []
    fetched_list = []
    outputs = []
    for layer_index in range(layer_total):
        fetched = fetch_forward(
            attn_in[layer_index],
            attn_out[layer_index],
            ffn_in[layer_index],
            ffn_out[layer_index],
            biases[layer_index],
            ffn_in_bias[layer_index],
            gains[layer_index],
            tables[layer_index],
        )
        result, kept = layer_forward(current, fetched, pair_mask, linear, across)
        layer_inputs.append(current)
        kept_list.append(kept)
        fetched_list.append(fetched)
        current = result.astype(jnp.bfloat16)
        outputs.append(current)
    grad_inputs = out_grad.astype(jnp.float32) * mlm_mask.astype(jnp.float32)[:, None]
    shard_list = []
    for layer_index in reversed(range(layer_total)):
        grad_inputs, grads = layer_backward(
            grad_inputs,
            layer_inputs[layer_index],
            fetched_list[layer_index],
            kept_list[layer_index],
            pair_mask,
            linear,
            across,
        )
        shard_list.insert(0, grads)
    packed, shapes = pack_gradients(shard_list, lax.axis_size("fsdp"), lax.axis_size("dp"))
    reduced = reduce_gradients(packed, lax.axis_size("dp"))
    return (jnp.stack(outputs), grad_inputs) + unpack_gradients(reduced, shapes)


def solution(mesh):
    return jax.shard_map(
        local,
        mesh=mesh,
        in_specs=(
            P(("dp", "fsdp"), None),
            P(("dp", "fsdp"), None),
            P(("dp", "fsdp")),
            P(("dp", "fsdp")),
            P(("dp", "fsdp"), None),
            P(None, ("dp", "fsdp"), None),
            P(None, "fsdp", None),
            P(None, "fsdp", None),
            P(None, "fsdp", None),
            P(None, "fsdp", None),
            P(None, None, "fsdp"),
            P(None, "fsdp"),
            P(None, None, "fsdp"),
            P(None, None, "fsdp", None),
        ),
        out_specs=(
            P(None, ("dp", "fsdp"), None),
            P(("dp", "fsdp"), None),
            P(None, "fsdp", None),
            P(None, "fsdp", None),
            P(None, "fsdp", None),
            P(None, "fsdp", None),
            P(None, None, "fsdp"),
            P(None, "fsdp"),
            P(None, None, "fsdp"),
            P(None, None, "fsdp", None),
        ),
        check_vma=False,
    )
```

```python
import functools
from typing import NamedTuple

import jax
import jax.numpy as jnp
from jax import lax
from jax.experimental import pallas as pl
from jax.experimental.pallas import tpu as pltpu
from jax.sharding import PartitionSpec as P

H = 12
DH = 64
NB = 32
WIN = 128


EPSILON = 1e-05
LAG = 2


def exact_gelu(values):
    return jax.nn.gelu(values, approximate=False)


def norm_forward(values, gain_row, shift_row):
    centre = values - jnp.mean(values, axis=-1, keepdims=True)
    spread = jnp.mean(centre * centre, axis=-1, keepdims=True)
    inverse = lax.rsqrt(spread + EPSILON)
    normed = centre * inverse
    return (normed * gain_row + shift_row, normed, inverse)


def norm_backward(incoming, normed, inverse, gain_row):
    scaled = incoming * gain_row
    centred = (
        scaled
        - jnp.mean(scaled, axis=-1, keepdims=True)
        - normed * jnp.mean(scaled * normed, axis=-1, keepdims=True)
    )
    return (centred * inverse, jnp.sum(incoming * normed, axis=0), jnp.sum(incoming, axis=0))


def geometry(doc_lengths, live_mask, layout_buckets):
    windows = doc_lengths.shape[0]
    positions = jnp.arange(WIN, dtype=jnp.int32)
    doc_ends = jnp.cumsum(doc_lengths, axis=1)
    document = jnp.sum((positions[None, :, None] >= doc_ends[:, None, :]).astype(jnp.int32), axis=2)
    live_rows = live_mask.reshape(windows, WIN) == 1
    diagonal = positions[:, None] == positions[None, :]
    pair_mask = (document[:, :, None] == document[:, None, :]) & (
        live_rows[:, None, :] | diagonal[None]
    )
    offset = jnp.clip(positions[None, :] - positions[:, None], -(NB // 2), NB // 2 - 1) + NB // 2
    buckets = jnp.arange(NB, dtype=jnp.int32)
    linear = (offset[None] == buckets[:, None, None]).astype(jnp.bfloat16)
    layout_rows = layout_buckets.reshape(2, windows, WIN, WIN)
    across = (layout_rows[:, :, None] == buckets[None, None, :, None, None]).astype(jnp.bfloat16)
    return (pair_mask, linear, across)


def pair_terms_of(bias_table, linear, across):
    terms = jnp.einsum("bij,bh->hij", linear, bias_table[0], preferred_element_type=jnp.float32)[
        None
    ]
    terms = terms + jnp.einsum(
        "wbij,bh->whij", across[0], bias_table[1], preferred_element_type=jnp.float32
    )
    return terms + jnp.einsum(
        "wbij,bh->whij", across[1], bias_table[2], preferred_element_type=jnp.float32
    )


def masked_scores(query_rows, key_rows, pair_terms, pair_mask):
    scores = (
        jnp.einsum("wihd,wjhd->whij", query_rows, key_rows, preferred_element_type=jnp.float32)
        + pair_terms
    )
    return jnp.where(pair_mask[:, None], scores, -1e30)


def layer_forward(inputs, weights, pair_mask, linear, across):
    w_in, w_out, w_up, w_down, shifts, up_shift, gain_rows, bias_table = weights
    shifts = shifts.astype(jnp.float32)
    gain_rows = gain_rows.astype(jnp.float32)
    rows = inputs.shape[0]
    windows = rows // WIN
    width = w_out.shape[0]
    scaling = DH ** (-0.5)
    projected = jnp.dot(inputs, w_in, preferred_element_type=jnp.float32)
    query_rows = (
        ((projected[:, :width] + shifts[0]) * scaling)
        .astype(jnp.bfloat16)
        .reshape(windows, WIN, H, DH)
    )
    key_rows = projected[:, width : 2 * width].astype(jnp.bfloat16).reshape(windows, WIN, H, DH)
    value_rows = (
        (projected[:, 2 * width :] + shifts[1]).astype(jnp.bfloat16).reshape(windows, WIN, H, DH)
    )
    pair_terms = pair_terms_of(bias_table, linear, across)
    scores = masked_scores(query_rows, key_rows, pair_terms, pair_mask)
    highest = jnp.max(scores, axis=-1, keepdims=True)
    exponent = jnp.exp(scores - highest)
    denominator = jnp.sum(exponent, axis=-1, keepdims=True)
    probs = exponent / denominator
    log_total = highest + jnp.log(denominator)
    mixed_rows = jnp.einsum(
        "whij,wjhd->wihd",
        probs.astype(jnp.bfloat16),
        value_rows,
        preferred_element_type=jnp.float32,
    )
    mixed_rows = mixed_rows.reshape(rows, width).astype(jnp.bfloat16)
    attended = jnp.dot(mixed_rows, w_out, preferred_element_type=jnp.float32) + shifts[2]
    first_norm, normed_first, inverse_first = norm_forward(
        inputs.astype(jnp.float32) + attended, gain_rows[0], shifts[3]
    )
    first_low = first_norm.astype(jnp.bfloat16)
    hidden = jnp.dot(first_low, w_up, preferred_element_type=jnp.float32) + up_shift.astype(
        jnp.float32
    )
    active = exact_gelu(hidden).astype(jnp.bfloat16)
    branch = jnp.dot(active, w_down, preferred_element_type=jnp.float32) + shifts[4]
    result, normed_second, inverse_second = norm_forward(
        first_norm + branch, gain_rows[1], shifts[5]
    )
    kept = (
        query_rows,
        key_rows,
        value_rows,
        pair_terms,
        log_total,
        mixed_rows,
        normed_first,
        inverse_first,
        first_low,
        hidden,
        active,
        normed_second,
        inverse_second,
    )
    return (result, kept)


def layer_backward(incoming, inputs, weights, kept, pair_mask, linear, across):
    w_in, w_out, w_up, w_down, shifts, up_shift, gain_rows, bias_table = weights
    gain_rows = gain_rows.astype(jnp.float32)
    (
        query_rows,
        key_rows,
        value_rows,
        pair_terms,
        log_total,
        mixed_rows,
        normed_first,
        inverse_first,
        first_low,
        hidden,
        active,
        normed_second,
        inverse_second,
    ) = kept
    rows = inputs.shape[0]
    width = w_out.shape[0]
    windows = rows // WIN
    scaling = DH ** (-0.5)
    grad_second, grad_gain_second, grad_shift_second = norm_backward(
        incoming, normed_second, inverse_second, gain_rows[1]
    )
    branch_low = grad_second.astype(jnp.bfloat16)
    grad_down = jnp.einsum("nf,nd->fd", active, branch_low, preferred_element_type=jnp.float32)
    grad_branch_shift = jnp.sum(branch_low.astype(jnp.float32), axis=0)
    grad_active = jnp.einsum("nd,fd->nf", branch_low, w_down, preferred_element_type=jnp.float32)
    hidden_low = jax.vjp(exact_gelu, hidden)[1](grad_active)[0].astype(jnp.bfloat16)
    grad_up = jnp.einsum("nd,nf->df", first_low, hidden_low, preferred_element_type=jnp.float32)
    grad_up_shift = jnp.sum(hidden_low.astype(jnp.float32), axis=0)
    grad_first = grad_second + jnp.einsum(
        "nf,df->nd", hidden_low, w_up, preferred_element_type=jnp.float32
    )
    grad_attended, grad_gain_first, grad_shift_first = norm_backward(
        grad_first, normed_first, inverse_first, gain_rows[0]
    )
    attended_low = grad_attended.astype(jnp.bfloat16)
    grad_out_weight = jnp.einsum(
        "nd,ne->de", mixed_rows, attended_low, preferred_element_type=jnp.float32
    )
    grad_attended_shift = jnp.sum(attended_low.astype(jnp.float32), axis=0)
    grad_mixed = jnp.einsum("ne,de->nd", attended_low, w_out, preferred_element_type=jnp.float32)
    grad_mixed = grad_mixed.astype(jnp.bfloat16).reshape(windows, WIN, H, DH)
    scores = masked_scores(query_rows, key_rows, pair_terms, pair_mask)
    probs = jnp.exp(scores - log_total)
    grad_probs = jnp.einsum(
        "wihd,wjhd->whij", grad_mixed, value_rows, preferred_element_type=jnp.float32
    )
    grad_value = jnp.einsum(
        "whij,wihd->wjhd",
        probs.astype(jnp.bfloat16),
        grad_mixed,
        preferred_element_type=jnp.float32,
    ).astype(jnp.bfloat16)
    grad_scores = (
        probs * (grad_probs - jnp.sum(probs * grad_probs, axis=-1, keepdims=True))
    ).astype(jnp.bfloat16)
    grad_query = (
        jnp.einsum(
            "whij,wjhd->wihd", grad_scores, key_rows, preferred_element_type=jnp.float32
        ).astype(jnp.bfloat16)
        * scaling
    )
    grad_key = jnp.einsum(
        "whij,wihd->wjhd", grad_scores, query_rows, preferred_element_type=jnp.float32
    ).astype(jnp.bfloat16)
    grad_qkv = jnp.concatenate(
        [
            grad_query.reshape(rows, width),
            grad_key.reshape(rows, width),
            grad_value.reshape(rows, width),
        ],
        axis=1,
    )
    grad_in_weight = jnp.einsum("nd,ne->de", inputs, grad_qkv, preferred_element_type=jnp.float32)
    grad_linear = jnp.einsum(
        "bij,whij->bh", linear, grad_scores, preferred_element_type=jnp.float32
    )
    grad_across_x = jnp.einsum(
        "wbij,whij->bh", across[0], grad_scores, preferred_element_type=jnp.float32
    )
    grad_across_y = jnp.einsum(
        "wbij,whij->bh", across[1], grad_scores, preferred_element_type=jnp.float32
    )
    grad_table = jnp.stack([grad_linear, grad_across_x, grad_across_y])
    grad_inputs = grad_attended + jnp.einsum(
        "ne,de->nd", grad_qkv, w_in, preferred_element_type=jnp.float32
    )
    grad_query_shift = jnp.sum(grad_query.reshape(rows, width).astype(jnp.float32), axis=0)
    grad_value_shift = jnp.sum(grad_value.reshape(rows, width).astype(jnp.float32), axis=0)
    grad_shifts = jnp.stack(
        [
            grad_query_shift,
            grad_value_shift,
            grad_attended_shift,
            grad_shift_first,
            grad_branch_shift,
            grad_shift_second,
        ]
    )
    grad_gain_rows = jnp.stack([grad_gain_first, grad_gain_second])
    grads = (
        grad_in_weight,
        grad_out_weight,
        grad_up,
        grad_down,
        grad_shifts,
        grad_up_shift,
        grad_gain_rows,
        grad_table,
    )
    return (grad_inputs, grads)


MESH = pl.DeviceIdType.MESH
CHUNK_TILES = 1


def add_rows(target, other):
    target[...] = (target[...].astype(jnp.float32) + other[...].astype(jnp.float32)).astype(
        jnp.bfloat16
    )


def reduce_kernel(high, count, segments, members, *refs):
    sources, targets = refs[:members], refs[members : 2 * members]
    (own, core_in, x_in, y_in, z_in, full, load_sem, core_sem, x_sem, y_sem, z_sem, zg_sem,
     yg_sem, sent, out_sem) = refs[2 * members :]
    dp = lax.axis_index("dp")
    shard = lax.axis_index("fsdp")
    y_at, z_at = lax.rem(dp, 2), lax.div(dp, 2)
    x_at, core = lax.div(shard, 2), lax.rem(shard, 2)
    core_peer = (dp, x_at * 2 + 1 - core)
    x_peer = (dp, (1 - x_at) * 2 + core)
    y_peer = (z_at * 2 + 1 - y_at, shard)
    z_of = [lax.rem(z_at + step, high) for step in range(high)]
    z_from = [lax.rem(z_at + high - step, high) for step in range(high)]
    z_peers = [(z_of[step] * 2 + y_at, shard) for step in range(high)]
    chunk = own.shape[2]
    half = chunk // 2
    piece = half // high

    barrier = pltpu.get_barrier_semaphore()
    peers = [core_peer, x_peer, y_peer] + z_peers[1:]
    for peer in peers:
        pl.semaphore_signal(barrier, inc=1, device_id=peer, device_id_type=MESH)
    pl.semaphore_wait(barrier, len(peers))

    def remote(source, target, send_at, receive, peer):
        return pltpu.make_async_remote_copy(
            src_ref=source, dst_ref=target, send_sem=sent.at[send_at], recv_sem=receive,
            device_id=peer, device_id_type=MESH,
        )

    def source_of(segment, wanted):
        ref = sources[segment.member]
        start = pl.multiple_of(wanted * segment.depth + segment.row, 16)
        return ref.at[pl.ds(start, segment.rows), pl.ds(segment.column, own.shape[3])]

    def slot_of(buffer, k, j, segment):
        return buffer.at[k, j, pl.ds(segment.at, segment.rows)]

    def load_arrival(k, j):
        slot = own.at[k, j]
        return pltpu.make_async_copy(slot, slot, load_sem.at[k, j])

    def core_arrival(k, j):
        return remote(core_in.at[k, j], core_in.at[k, j], 0, core_sem.at[k, j], core_peer)

    def x_send(k):
        return remote(own.at[k, 1], x_in.at[k], 1, x_sem.at[k], x_peer)

    def y_rows(side):
        return pl.ds(pl.multiple_of(side * half, half), half)

    def y_send(k):
        return remote(own.at[k, 0, y_rows(1 - y_at)], y_in.at[k], 2, y_sem.at[k], y_peer)

    def z_rows(at):
        return pl.ds(pl.multiple_of(y_at * half + at * piece, piece), piece)

    def z_send(k, step):
        return remote(
            own.at[k, 0, z_rows(z_of[step])], z_in.at[k, step - 1], 3,
            z_sem.at[k, step - 1], z_peers[step],
        )

    def zg_send(k, step):
        mine = full.at[k, z_rows(z_at)]
        return remote(mine, mine, 4, zg_sem.at[k, step - 1], z_peers[step])

    def zg_arrival(k, step):
        theirs = full.at[k, z_rows(z_from[step])]
        return remote(theirs, theirs, 4, zg_sem.at[k, step - 1], z_peers[step])

    def yg_send(k):
        mine = full.at[k, y_rows(y_at)]
        return remote(mine, mine, 5, yg_sem.at[k], y_peer)

    def store_end(k):
        return pltpu.make_async_copy(full.at[k], full.at[k], out_sem.at[k])

    for segment in segments:
        k = segment.chunk
        for j in (1, 0):
            x_wanted = x_at if j == 0 else 1 - x_at
            remote(
                source_of(segment, x_wanted * 2 + 1 - core), slot_of(core_in, k, j, segment),
                0, core_sem.at[k, j], core_peer,
            ).start()
            pltpu.make_async_copy(
                source_of(segment, x_wanted * 2 + core), slot_of(own, k, j, segment),
                load_sem.at[k, j],
            ).start()

    def stage_core(k):
        for j in (1, 0):
            load_arrival(k, j).wait()
            core_arrival(k, j).wait_recv()
            add_rows(own.at[k, j], core_in.at[k, j])
            if j == 1:
                x_send(k).start()

    def stage_x(k):
        x_send(k).wait_recv()
        add_rows(own.at[k, 0], x_in.at[k])
        y_send(k).start()

    def stage_y(k):
        y_send(k).wait_recv()
        add_rows(own.at[k, 0, y_rows(y_at)], y_in.at[k])
        for step in range(1, high):
            z_send(k, step).start()

    def stage_z(k):
        total = own[k, 0, z_rows(z_at), :].astype(jnp.float32)
        for step in range(1, high):
            z_send(k, step).wait_recv()
            total = total + z_in[k, step - 1].astype(jnp.float32)
        full[k, z_rows(z_at), :] = total.astype(jnp.bfloat16)
        for step in range(1, high):
            zg_send(k, step).start()

    def stage_spread(k):
        for step in range(1, high):
            zg_arrival(k, step).wait_recv()
        yg_send(k).start()

    def stage_store(k):
        yg_send(k).wait_recv()
        for segment in segments:

            @pl.when(k == segment.chunk)
            def _(segment=segment):
                target = targets[segment.member].at[
                    pl.ds(segment.row, segment.rows), pl.ds(segment.column, own.shape[3])
                ]
                pltpu.make_async_copy(
                    full.at[segment.chunk, pl.ds(segment.at, segment.rows)], target,
                    out_sem.at[segment.chunk],
                ).start()

    stages = (stage_core, stage_x, stage_y, stage_z, stage_spread, stage_store)
    lags = (0, LAG, 2 * LAG, 3 * LAG, 4 * LAG, 5 * LAG)

    @pl.loop(0, count + lags[-1])
    def _(t):
        for stage, lag in zip(stages, lags):
            k = t - lag

            @pl.when((k >= 0) & (k < count))
            def _():
                stage(k)

    def all_sent(source, target, send_at, peer):
        remote(source, target, send_at, x_sem.at[0], peer).wait_send()

    all_sent(own, core_in, 0, core_peer)
    all_sent(x_in, x_in, 1, x_peer)
    all_sent(y_in, y_in, 2, y_peer)
    all_sent(z_in, z_in, 3, z_peers[1])
    all_sent(z_in, z_in, 4, z_peers[1])
    all_sent(y_in, y_in, 5, y_peer)

    @pl.loop(0, count)
    def _(k):
        store_end(k).wait()


class Segment(NamedTuple):
    member: int
    depth: int
    row: int
    column: int
    rows: int
    chunk: int
    at: int


def plan_segments(members, shards, width, chunk):
    segments, place = [], 0
    for member, array in enumerate(members):
        depth = array.shape[0] // shards
        for column in range(0, array.shape[1], width):
            row = 0
            while row < depth:
                rows = min(depth - row, chunk - place % chunk)
                segments.append(
                    Segment(member, depth, row, column, rows, place // chunk, place % chunk)
                )
                row, place = row + rows, place + rows
    return tuple(segments), place


def reduce_gradients(members, shards, group, width):
    high = group // 2
    chunk = chunk_rows(group)
    segments, rows = plan_segments(members, shards, width, chunk)
    count = rows // chunk
    piece = chunk // group
    buffers = [
        (count, 2, chunk, width),
        (count, 2, chunk, width),
        (count, chunk, width),
        (count, chunk // 2, width),
        (count, high - 1, piece, width),
        (count, chunk, width),
    ]
    semaphores = [(count, 2), (count, 2), (count,), (count,), (count, high - 1),
                  (count, high - 1), (count,), (6,), (count,)]
    hbm = pl.BlockSpec(memory_space=pltpu.MemorySpace.HBM)
    return pl.pallas_call(
        functools.partial(reduce_kernel, high, count, segments, len(members)),
        out_shape=[
            jax.ShapeDtypeStruct((array.shape[0] // shards, array.shape[1]), jnp.bfloat16)
            for array in members
        ],
        in_specs=[hbm] * len(members),
        out_specs=[hbm] * len(members),
        scratch_shapes=[pltpu.VMEM(shape, jnp.bfloat16) for shape in buffers]
        + [pltpu.SemaphoreType.DMA(shape) for shape in semaphores],
        compiler_params=pltpu.CompilerParams(
            collective_id=1, has_side_effects=True, vmem_limit_bytes=64 * 1024 * 1024 - 65536
        ),
    )(*members)


def chunk_rows(group):
    return 16 * CHUNK_TILES * group


def sum_gradients(grad_list, shards, group):
    members, smalls = [], []
    for grads in grad_list:
        w_in, w_out, w_up, w_down, shifts, up_shift, gain_rows, bias_table = grads
        width = w_out.shape[1]
        members += [member.astype(jnp.bfloat16) for member in (w_in, w_out, w_up, w_down)]
        smalls.append(jnp.swapaxes(shifts.reshape(6, shards, -1), 0, 1).reshape(shards, -1))
        smalls.append(up_shift.reshape(shards, -1))
        smalls.append(jnp.swapaxes(gain_rows.reshape(2, shards, -1), 0, 1).reshape(shards, -1))
        smalls.append(jnp.swapaxes(bias_table.reshape(3, shards, -1), 0, 1).reshape(shards, -1))
    small = jnp.concatenate(smalls, axis=1).astype(jnp.bfloat16)
    layers = len(grad_list)
    rows = sum(member.size // (shards * width) for member in members)
    chunk = chunk_rows(group)
    total = -(-(rows + -(-small.shape[1] // width)) // chunk) * chunk
    small = jnp.pad(small, ((0, 0), (0, (total - rows) * width - small.shape[1])))
    members.append(small.reshape(shards * (total - rows), width))
    reduced = reduce_gradients(members, shards, group, width)
    spans = [
        jnp.stack([reduced[4 * layer + member] for layer in range(layers)]).astype(jnp.float32)
        for member in range(4)
    ]
    depth = width // shards
    sizes = (6 * depth, width, 2 * depth, 3 * (NB // shards) * H)
    used = layers * sum(sizes)
    small = reduced[-1][: -(-used // width)].astype(jnp.float32).reshape(-1)
    small = small[:used].reshape(layers, -1)
    forms = ((6, depth), (width,), (2, depth), (3, NB // shards, H))
    start = 0
    for size, form in zip(sizes, forms):
        spans.append(small[:, start : start + size].reshape((layers,) + form))
        start += size
    return tuple(spans)


def gather_kernel(items, *refs):
    total = len(items)
    sources, targets = refs[:5], refs[5 : 5 + total]
    stages = refs[5 + total : 5 + 2 * total]
    load_sem, store_sem, send_sem, arrive = refs[5 + 2 * total :]
    dp = lax.axis_index("dp")
    shard = lax.axis_index("fsdp")
    x_at, core = lax.div(shard, 2), lax.rem(shard, 2)
    bits = (lax.rem(dp, 2), lax.rem(lax.div(dp, 2), 2))
    core_peer = (dp, x_at * 2 + 1 - core)
    other = (1 - x_at) * 2 + core
    x_peer = (dp, other)
    dp_peers = [
        (dp + 1 - 2 * bits[0], shard),
        (dp + 2 - 4 * bits[1], shard),
    ]
    barrier = pltpu.get_barrier_semaphore()
    for peer in [core_peer, x_peer] + dp_peers:
        pl.semaphore_signal(barrier, inc=1, device_id=peer, device_id_type=MESH)
    pl.semaphore_wait(barrier, 4)

    def copy(source, target, item, kind, peer):
        return pltpu.make_async_remote_copy(
            src_ref=source, dst_ref=target, send_sem=send_sem.at[item, kind],
            recv_sem=arrive.at[item, kind], device_id=peer, device_id_type=MESH,
        )

    def shard_of(i):
        member, layer = items[i]
        return sources[member] if layer is None else sources[member].at[layer]

    def depth_of(i):
        return stages[i].shape[0]

    def parts_of(i):
        return 4 if depth_of(i) % 64 == 0 else 1

    def mine_out(i):
        n = depth_of(i)
        return targets[i].at[pl.ds(pl.multiple_of(shard * n, 16), n)]

    def other_out(i, quarter):
        n = depth_of(i)
        part = n // parts_of(i)
        return targets[i].at[pl.ds(pl.multiple_of(other * n + quarter * part, 16), part)]

    def other_whole(i):
        n = depth_of(i)
        return targets[i].at[pl.ds(pl.multiple_of(other * n, 16), n)]

    def order_of(i):
        return (0, 1) if i % 2 == 0 else (1, 0)

    def quarter_of(i, flips):
        if parts_of(i) == 1:
            return 0
        now = [bits[axis] if axis not in flips else 1 - bits[axis] for axis in (0, 1)]
        return now[1] * 2 + now[0]

    def x_send(i):
        n = depth_of(i)
        part = n // parts_of(i)
        start = pl.multiple_of(quarter_of(i, ()) * part, 16)
        rows = pl.ds(start, part)
        landing = targets[i].at[pl.ds(pl.multiple_of(shard * n + start, 16), part)]
        return copy(shard_of(i).at[rows], landing, i, 0, x_peer)

    def first_send(i):
        mine = other_out(i, quarter_of(i, ()))
        return copy(mine, mine, i, 1, dp_peers[order_of(i)[0]])

    def second_send(i):
        mine = other_out(i, quarter_of(i, ()))
        return copy(mine, mine, i, 2, dp_peers[order_of(i)[1]])

    def relay_send(i):
        mine = other_out(i, quarter_of(i, (order_of(i)[0],)))
        return copy(mine, mine, i, 3, dp_peers[order_of(i)[1]])

    def own_share(i):
        return copy(shard_of(i), mine_out(i), i, 4, core_peer)

    def far_share(i):
        return copy(other_whole(i), other_whole(i), i, 5, core_peer)

    def load(i):
        return pltpu.make_async_copy(shard_of(i), stages[i], load_sem.at[i])

    def store(i):
        return pltpu.make_async_copy(stages[i], mine_out(i), store_sem.at[i])

    for i in range(total):
        x_send(i).start()
    for i in range(total):
        own_share(i).start()
        load(i).start()

    def spread(i):
        x_send(i).wait_recv()
        if parts_of(i) == 4:
            first_send(i).start()
            second_send(i).start()
        load(i).wait()
        store(i).start()

    def relay(i):
        if parts_of(i) == 4:
            first_send(i).wait_recv()
            relay_send(i).start()

    def share(i):
        if parts_of(i) == 4:
            second_send(i).wait_recv()
            relay_send(i).wait_recv()
        far_share(i).start()

    for step in range(total + 4):
        if step < total:
            spread(step)
        if 0 <= step - 1 < total:
            relay(step - 1)
        if 0 <= step - 3 < total:
            share(step - 3)
    for i in range(total):
        own_share(i).wait()
        far_share(i).wait()
        x_send(i).wait_send()
        if parts_of(i) == 4:
            first_send(i).wait_send()
            second_send(i).wait_send()
            relay_send(i).wait_send()
        store(i).wait()


def gather_weights(sources, small, shards):
    layers = sources[0].shape[0]
    items = [(4, None)]
    forms = [small.shape]
    for layer in range(layers):
        for member in range(4):
            items.append((member, layer))
            forms.append(sources[member].shape[1:])
    hbm = pl.BlockSpec(memory_space=pltpu.MemorySpace.HBM)
    total = len(items)
    return pl.pallas_call(
        functools.partial(gather_kernel, tuple(items)),
        out_shape=[
            jax.ShapeDtypeStruct((form[0] * shards, form[1]), jnp.bfloat16) for form in forms
        ],
        in_specs=[hbm] * 5,
        out_specs=[hbm] * total,
        scratch_shapes=[pltpu.VMEM(form, jnp.bfloat16) for form in forms]
        + [
            pltpu.SemaphoreType.DMA((total,)),
            pltpu.SemaphoreType.DMA((total,)),
            pltpu.SemaphoreType.DMA((total, 6)),
            pltpu.SemaphoreType.DMA((total, 6)),
        ],
        compiler_params=pltpu.CompilerParams(collective_id=0, has_side_effects=True),
    )(*sources, small)


def fetch_all(attn_in, attn_out, ffn_in, ffn_out, biases, ffn_in_bias, gains, tables, shards):
    layers, depth = attn_in.shape[0], attn_in.shape[1]
    width = depth * shards
    flat = jnp.concatenate(
        [member.reshape(-1) for member in (biases, ffn_in_bias, gains, tables)]
    )
    rows = -(-flat.shape[0] // (16 * width)) * 16
    small = jnp.pad(flat, (0, rows * width - flat.shape[0])).reshape(rows, width)
    gathered = gather_weights((attn_in, attn_out, ffn_in, ffn_out), small, shards)
    small = gathered[0].reshape(shards, -1)
    pieces = []
    start = 0
    for member, axis in ((biases, 2), (ffn_in_bias, 1), (gains, 2), (tables, 2)):
        piece = small[:, start : start + member.size].reshape((shards,) + member.shape)
        start += member.size
        piece = jnp.moveaxis(piece, 0, axis)
        pieces.append(
            piece.reshape(member.shape[:axis] + (-1,) + member.shape[axis + 1 :])
        )
    return [
        tuple(gathered[1 + 4 * layer : 5 + 4 * layer]) + tuple(piece[layer] for piece in pieces)
        for layer in range(layers)
    ]


def local(
    tokens,
    out_grad,
    mlm_mask,
    live_mask,
    doc_lengths,
    layout_buckets,
    attn_in,
    attn_out,
    ffn_in,
    ffn_out,
    biases,
    ffn_in_bias,
    gains,
    tables,
):
    pair_mask, linear, across = geometry(doc_lengths, live_mask, layout_buckets)
    layer_total = attn_in.shape[0]
    current = tokens
    layer_inputs = []
    kept_list = []
    shards = lax.axis_size("fsdp")
    fetched_list = fetch_all(
        attn_in, attn_out, ffn_in, ffn_out, biases, ffn_in_bias, gains, tables, shards
    )
    outputs = []
    for layer_index in range(layer_total):
        fetched = fetched_list[layer_index]
        result, kept = layer_forward(current, fetched, pair_mask, linear, across)
        layer_inputs.append(current)
        kept_list.append(kept)
        current = result.astype(jnp.bfloat16)
        outputs.append(current)
    grad_inputs = out_grad.astype(jnp.float32) * mlm_mask.astype(jnp.float32)[:, None]
    shard_list = []
    for layer_index in reversed(range(layer_total)):
        grad_inputs, grads = layer_backward(
            grad_inputs,
            layer_inputs[layer_index],
            fetched_list[layer_index],
            kept_list[layer_index],
            pair_mask,
            linear,
            across,
        )
        shard_list.insert(0, grads)
    summed = sum_gradients(shard_list, shards, lax.axis_size("dp"))
    return (jnp.stack(outputs), grad_inputs) + summed


def solution(mesh):
    return jax.shard_map(
        local,
        mesh=mesh,
        in_specs=(
            P(("dp", "fsdp"), None),
            P(("dp", "fsdp"), None),
            P(("dp", "fsdp")),
            P(("dp", "fsdp")),
            P(("dp", "fsdp"), None),
            P(None, ("dp", "fsdp"), None),
            P(None, "fsdp", None),
            P(None, "fsdp", None),
            P(None, "fsdp", None),
            P(None, "fsdp", None),
            P(None, None, "fsdp"),
            P(None, "fsdp"),
            P(None, None, "fsdp"),
            P(None, None, "fsdp", None),
        ),
        out_specs=(
            P(None, ("dp", "fsdp"), None),
            P(("dp", "fsdp"), None),
            P(None, "fsdp", None),
            P(None, "fsdp", None),
            P(None, "fsdp", None),
            P(None, "fsdp", None),
            P(None, None, "fsdp"),
            P(None, "fsdp"),
            P(None, None, "fsdp"),
            P(None, None, "fsdp", None),
        ),
        check_vma=False,
    )
```

```python
import functools
import math
from typing import NamedTuple

import jax
import jax.numpy as jnp
from jax import lax
from jax.experimental import pallas as pl
from jax.experimental.pallas import tpu as pltpu
from jax.sharding import PartitionSpec as P

H = 12
DH = 64
NB = 32
WIN = 128


EPSILON = 1e-05
LAG = 2


def norm_forward(values, gain_row, shift_row):
    centre = values - jnp.mean(values, axis=-1, keepdims=True)
    spread = jnp.mean(centre * centre, axis=-1, keepdims=True)
    inverse = lax.rsqrt(spread + EPSILON)
    normed = centre * inverse
    return (normed * gain_row + shift_row, normed, inverse)


MESH = pl.DeviceIdType.MESH
CHUNK_TILES = 1


def add_rows(target, other):
    target[...] = (target[...].astype(jnp.float32) + other[...].astype(jnp.float32)).astype(
        jnp.bfloat16
    )


def reduce_kernel(high, count, segments, members, *refs):
    sources, targets = refs[:members], refs[members : 2 * members]
    (own, core_in, x_in, y_in, z_in, full, load_sem, core_sem, x_sem, y_sem, z_sem, zg_sem,
     yg_sem, sent, out_sem) = refs[2 * members :]
    dp = lax.axis_index("dp")
    shard = lax.axis_index("fsdp")
    y_at, z_at = lax.rem(dp, 2), lax.div(dp, 2)
    x_at, core = lax.div(shard, 2), lax.rem(shard, 2)
    core_peer = (dp, x_at * 2 + 1 - core)
    x_peer = (dp, (1 - x_at) * 2 + core)
    y_peer = (z_at * 2 + 1 - y_at, shard)
    z_of = [lax.rem(z_at + step, high) for step in range(high)]
    z_from = [lax.rem(z_at + high - step, high) for step in range(high)]
    z_peers = [(z_of[step] * 2 + y_at, shard) for step in range(high)]
    chunk = own.shape[2]
    half = chunk // 2
    piece = half // high

    barrier = pltpu.get_barrier_semaphore()
    peers = [core_peer, x_peer, y_peer] + z_peers[1:]
    for peer in peers:
        pl.semaphore_signal(barrier, inc=1, device_id=peer, device_id_type=MESH)
    pl.semaphore_wait(barrier, len(peers))

    def remote(source, target, send_at, receive, peer):
        return pltpu.make_async_remote_copy(
            src_ref=source, dst_ref=target, send_sem=sent.at[send_at], recv_sem=receive,
            device_id=peer, device_id_type=MESH,
        )

    def source_of(segment, wanted):
        ref = sources[segment.member]
        start = pl.multiple_of(wanted * segment.depth + segment.row, 16)
        return ref.at[pl.ds(start, segment.rows), pl.ds(segment.column, own.shape[3])]

    def slot_of(buffer, k, j, segment):
        return buffer.at[k, j, pl.ds(segment.at, segment.rows)]

    def load_arrival(k, j):
        slot = own.at[k, j]
        return pltpu.make_async_copy(slot, slot, load_sem.at[k, j])

    def core_arrival(k, j):
        return remote(core_in.at[k, j], core_in.at[k, j], 0, core_sem.at[k, j], core_peer)

    def x_send(k):
        return remote(own.at[k, 1], x_in.at[k], 1, x_sem.at[k], x_peer)

    def y_rows(side):
        return pl.ds(pl.multiple_of(side * half, half), half)

    def y_send(k):
        return remote(own.at[k, 0, y_rows(1 - y_at)], y_in.at[k], 2, y_sem.at[k], y_peer)

    def z_rows(at):
        return pl.ds(pl.multiple_of(y_at * half + at * piece, piece), piece)

    def z_send(k, step):
        return remote(
            own.at[k, 0, z_rows(z_of[step])], z_in.at[k, step - 1], 3,
            z_sem.at[k, step - 1], z_peers[step],
        )

    def zg_send(k, step):
        mine = full.at[k, z_rows(z_at)]
        return remote(mine, mine, 4, zg_sem.at[k, step - 1], z_peers[step])

    def zg_arrival(k, step):
        theirs = full.at[k, z_rows(z_from[step])]
        return remote(theirs, theirs, 4, zg_sem.at[k, step - 1], z_peers[step])

    def yg_send(k):
        mine = full.at[k, y_rows(y_at)]
        return remote(mine, mine, 5, yg_sem.at[k], y_peer)

    def store_end(k):
        return pltpu.make_async_copy(full.at[k], full.at[k], out_sem.at[k])

    for segment in segments:
        k = segment.chunk
        for j in (1, 0):
            x_wanted = x_at if j == 0 else 1 - x_at
            remote(
                source_of(segment, x_wanted * 2 + 1 - core), slot_of(core_in, k, j, segment),
                0, core_sem.at[k, j], core_peer,
            ).start()
            pltpu.make_async_copy(
                source_of(segment, x_wanted * 2 + core), slot_of(own, k, j, segment),
                load_sem.at[k, j],
            ).start()

    def stage_core(k):
        for j in (1, 0):
            load_arrival(k, j).wait()
            core_arrival(k, j).wait_recv()
            add_rows(own.at[k, j], core_in.at[k, j])
            if j == 1:
                x_send(k).start()

    def stage_x(k):
        x_send(k).wait_recv()
        add_rows(own.at[k, 0], x_in.at[k])
        y_send(k).start()

    def stage_y(k):
        y_send(k).wait_recv()
        add_rows(own.at[k, 0, y_rows(y_at)], y_in.at[k])
        for step in range(1, high):
            z_send(k, step).start()

    def stage_z(k):
        total = own[k, 0, z_rows(z_at), :].astype(jnp.float32)
        for step in range(1, high):
            z_send(k, step).wait_recv()
            total = total + z_in[k, step - 1].astype(jnp.float32)
        full[k, z_rows(z_at), :] = total.astype(jnp.bfloat16)
        for step in range(1, high):
            zg_send(k, step).start()

    def stage_spread(k):
        for step in range(1, high):
            zg_arrival(k, step).wait_recv()
        yg_send(k).start()

    def stage_store(k):
        yg_send(k).wait_recv()
        for segment in segments:

            @pl.when(k == segment.chunk)
            def _(segment=segment):
                target = targets[segment.member].at[
                    pl.ds(segment.row, segment.rows), pl.ds(segment.column, own.shape[3])
                ]
                pltpu.make_async_copy(
                    full.at[segment.chunk, pl.ds(segment.at, segment.rows)], target,
                    out_sem.at[segment.chunk],
                ).start()

    stages = (stage_core, stage_x, stage_y, stage_z, stage_spread, stage_store)
    lags = (0, LAG, 2 * LAG, 3 * LAG, 4 * LAG, 5 * LAG)

    @pl.loop(0, count + lags[-1])
    def _(t):
        for stage, lag in zip(stages, lags):
            k = t - lag

            @pl.when((k >= 0) & (k < count))
            def _():
                stage(k)

    def all_sent(source, target, send_at, peer):
        remote(source, target, send_at, x_sem.at[0], peer).wait_send()

    all_sent(own, core_in, 0, core_peer)
    all_sent(x_in, x_in, 1, x_peer)
    all_sent(y_in, y_in, 2, y_peer)
    all_sent(z_in, z_in, 3, z_peers[1])
    all_sent(z_in, z_in, 4, z_peers[1])
    all_sent(y_in, y_in, 5, y_peer)

    @pl.loop(0, count)
    def _(k):
        store_end(k).wait()


class Segment(NamedTuple):
    member: int
    depth: int
    row: int
    column: int
    rows: int
    chunk: int
    at: int


def plan_segments(members, depths, strides, width, chunk):
    segments, place = [], 0
    for member, array in enumerate(members):
        depth = depths[member]
        for column in range(0, array.shape[1], width):
            row = 0
            while row < depth:
                rows = min(depth - row, chunk - place % chunk)
                segments.append(
                    Segment(
                        member, strides[member], row, column, rows, place // chunk, place % chunk
                    )
                )
                row, place = row + rows, place + rows
    return tuple(segments), place


def reduce_gradients(members, smalls, shards, group, width):
    high = group // 2
    chunk = chunk_rows(group)
    depths = [array.shape[0] // shards for array in members]
    strides = depths + [0] * len(smalls)
    depths += [array.shape[0] for array in smalls]
    filled = sum(
        array.shape[1] // width * depth for array, depth in zip(members + smalls, depths)
    )
    rest = -filled % chunk
    members = members + smalls
    if rest:
        members = members + [jnp.zeros((rest, width), jnp.bfloat16)]
        depths.append(rest)
        strides.append(0)
    segments, rows = plan_segments(members, depths, strides, width, chunk)
    count = rows // chunk
    piece = chunk // group
    buffers = [
        (count, 2, chunk, width),
        (count, 2, chunk, width),
        (count, chunk, width),
        (count, chunk // 2, width),
        (count, high - 1, piece, width),
        (count, chunk, width),
    ]
    semaphores = [(count, 2), (count, 2), (count,), (count,), (count, high - 1),
                  (count, high - 1), (count,), (6,), (count,)]
    hbm = pl.BlockSpec(memory_space=pltpu.MemorySpace.HBM)
    return pl.pallas_call(
        functools.partial(reduce_kernel, high, count, segments, len(members)),
        out_shape=[
            jax.ShapeDtypeStruct((depth, array.shape[1]), jnp.bfloat16)
            for array, depth in zip(members, depths)
        ],
        in_specs=[hbm] * len(members),
        out_specs=[hbm] * len(members),
        scratch_shapes=[pltpu.VMEM(shape, jnp.bfloat16) for shape in buffers]
        + [pltpu.SemaphoreType.DMA(shape) for shape in semaphores],
        compiler_params=pltpu.CompilerParams(
            collective_id=1, has_side_effects=True, vmem_limit_bytes=64 * 1024 * 1024 - 65536
        ),
    )(*members)


def chunk_rows(group):
    return 16 * CHUNK_TILES * group


def sum_gradients(members, smalls, shards, group):
    width = smalls[0].shape[1]
    layers = len(smalls)
    reduced = reduce_gradients(members, smalls, shards, group, width)
    spans = [
        jnp.stack([reduced[4 * layer + member] for layer in range(layers)]).astype(jnp.float32)
        for member in range(4)
    ]
    small = jnp.stack(reduced[4 * layers : 5 * layers]).astype(jnp.float32)
    depth = width // shards
    shard = lax.axis_index("fsdp")
    rows = lax.dynamic_slice_in_dim(small[:, :8], shard * depth, depth, axis=2)
    up_shift = lax.dynamic_slice_in_dim(small, 8 + shard, 1, axis=1)[:, 0]
    table = small[:, 16 : 16 + H, : 3 * NB].reshape(layers, H, 3, NB)
    table = lax.dynamic_slice_in_dim(table, shard * (NB // shards), NB // shards, axis=3)
    return tuple(spans) + (
        rows[:, :6], up_shift, rows[:, 6:], jnp.transpose(table, (0, 2, 3, 1)),
    )


def gather_kernel(items, *refs):
    total = len(items)
    sources, targets = refs[:5], refs[5 : 5 + total]
    stages = refs[5 + total : 5 + 2 * total]
    load_sem, store_sem, send_sem, arrive = refs[5 + 2 * total :]
    dp = lax.axis_index("dp")
    shard = lax.axis_index("fsdp")
    x_at, core = lax.div(shard, 2), lax.rem(shard, 2)
    bits = (lax.rem(dp, 2), lax.rem(lax.div(dp, 2), 2))
    core_peer = (dp, x_at * 2 + 1 - core)
    other = (1 - x_at) * 2 + core
    x_peer = (dp, other)
    dp_peers = [
        (dp + 1 - 2 * bits[0], shard),
        (dp + 2 - 4 * bits[1], shard),
    ]
    barrier = pltpu.get_barrier_semaphore()
    for peer in [core_peer, x_peer] + dp_peers:
        pl.semaphore_signal(barrier, inc=1, device_id=peer, device_id_type=MESH)
    pl.semaphore_wait(barrier, 4)

    def copy(source, target, item, kind, peer):
        return pltpu.make_async_remote_copy(
            src_ref=source, dst_ref=target, send_sem=send_sem.at[item, kind],
            recv_sem=arrive.at[item, kind], device_id=peer, device_id_type=MESH,
        )

    def shard_of(i):
        member, layer = items[i]
        return sources[member] if layer is None else sources[member].at[layer]

    def depth_of(i):
        return stages[i].shape[0]

    def parts_of(i):
        return 4 if depth_of(i) % 64 == 0 else 1

    def mine_out(i):
        n = depth_of(i)
        return targets[i].at[pl.ds(pl.multiple_of(shard * n, 16), n)]

    def other_out(i, quarter):
        n = depth_of(i)
        part = n // parts_of(i)
        return targets[i].at[pl.ds(pl.multiple_of(other * n + quarter * part, 16), part)]

    def other_whole(i):
        n = depth_of(i)
        return targets[i].at[pl.ds(pl.multiple_of(other * n, 16), n)]

    def order_of(i):
        return (0, 1) if i % 2 == 0 else (1, 0)

    def quarter_of(i, flips):
        if parts_of(i) == 1:
            return 0
        now = [bits[axis] if axis not in flips else 1 - bits[axis] for axis in (0, 1)]
        return now[1] * 2 + now[0]

    def x_send(i):
        n = depth_of(i)
        part = n // parts_of(i)
        start = pl.multiple_of(quarter_of(i, ()) * part, 16)
        rows = pl.ds(start, part)
        landing = targets[i].at[pl.ds(pl.multiple_of(shard * n + start, 16), part)]
        return copy(shard_of(i).at[rows], landing, i, 0, x_peer)

    def first_send(i):
        mine = other_out(i, quarter_of(i, ()))
        return copy(mine, mine, i, 1, dp_peers[order_of(i)[0]])

    def second_send(i):
        mine = other_out(i, quarter_of(i, ()))
        return copy(mine, mine, i, 2, dp_peers[order_of(i)[1]])

    def relay_send(i):
        mine = other_out(i, quarter_of(i, (order_of(i)[0],)))
        return copy(mine, mine, i, 3, dp_peers[order_of(i)[1]])

    def own_share(i):
        return copy(shard_of(i), mine_out(i), i, 4, core_peer)

    def far_share(i):
        return copy(other_whole(i), other_whole(i), i, 5, core_peer)

    def load(i):
        return pltpu.make_async_copy(shard_of(i), stages[i], load_sem.at[i])

    def store(i):
        return pltpu.make_async_copy(stages[i], mine_out(i), store_sem.at[i])

    for i in range(total):
        x_send(i).start()
    for i in range(total):
        own_share(i).start()
        load(i).start()

    def spread(i):
        x_send(i).wait_recv()
        if parts_of(i) == 4:
            first_send(i).start()
            second_send(i).start()
        load(i).wait()
        store(i).start()

    def relay(i):
        if parts_of(i) == 4:
            first_send(i).wait_recv()
            relay_send(i).start()

    def share(i):
        if parts_of(i) == 4:
            second_send(i).wait_recv()
            relay_send(i).wait_recv()
        far_share(i).start()

    for step in range(total + 4):
        if step < total:
            spread(step)
        if 0 <= step - 1 < total:
            relay(step - 1)
        if 0 <= step - 3 < total:
            share(step - 3)
    for i in range(total):
        own_share(i).wait()
        far_share(i).wait()
        x_send(i).wait_send()
        if parts_of(i) == 4:
            first_send(i).wait_send()
            second_send(i).wait_send()
            relay_send(i).wait_send()
        store(i).wait()


def gather_weights(sources, small, shards):
    layers = sources[0].shape[0]
    items = [(4, None)]
    forms = [small.shape]
    for layer in range(layers):
        for member in range(4):
            items.append((member, layer))
            forms.append(sources[member].shape[1:])
    hbm = pl.BlockSpec(memory_space=pltpu.MemorySpace.HBM)
    total = len(items)
    return pl.pallas_call(
        functools.partial(gather_kernel, tuple(items)),
        out_shape=[
            jax.ShapeDtypeStruct((form[0] * shards, form[1]), jnp.bfloat16) for form in forms
        ],
        in_specs=[hbm] * 5,
        out_specs=[hbm] * total,
        scratch_shapes=[pltpu.VMEM(form, jnp.bfloat16) for form in forms]
        + [
            pltpu.SemaphoreType.DMA((total,)),
            pltpu.SemaphoreType.DMA((total,)),
            pltpu.SemaphoreType.DMA((total, 6)),
            pltpu.SemaphoreType.DMA((total, 6)),
        ],
        compiler_params=pltpu.CompilerParams(collective_id=0, has_side_effects=True),
    )(*sources, small)


def fetch_all(attn_in, attn_out, ffn_in, ffn_out, biases, ffn_in_bias, gains, tables, shards):
    layers, depth = attn_in.shape[0], attn_in.shape[1]
    width = depth * shards
    flat = jnp.concatenate(
        [member.reshape(-1) for member in (biases, ffn_in_bias, gains, tables)]
    )
    rows = -(-flat.shape[0] // (16 * width)) * 16
    small = jnp.pad(flat, (0, rows * width - flat.shape[0])).reshape(rows, width)
    gathered = gather_weights((attn_in, attn_out, ffn_in, ffn_out), small, shards)
    small = gathered[0].reshape(shards, -1)
    pieces = []
    start = 0
    for member, axis in ((biases, 2), (ffn_in_bias, 1), (gains, 2), (tables, 2)):
        piece = small[:, start : start + member.size].reshape((shards,) + member.shape)
        start += member.size
        piece = jnp.moveaxis(piece, 0, axis)
        pieces.append(
            piece.reshape(member.shape[:axis] + (-1,) + member.shape[axis + 1 :])
        )
    shifts, up_shift, gain_rows, table = [piece.astype(jnp.float32) for piece in pieces]
    vectors = jnp.concatenate([shifts, gain_rows], axis=1)
    table = jnp.pad(
        jnp.swapaxes(table, 2, 3), ((0, 0), (0, 0), (0, 16 - H), (0, WIN - NB))
    )
    return [
        tuple(gathered[1 + 4 * layer : 5 + 4 * layer])
        + (vectors[layer], up_shift[layer : layer + 1], table[layer])
        for layer in range(layers)
    ]


def contract(left, right, left_axis, right_axis):
    return lax.dot_general(
        left, right, (((left_axis,), (right_axis,)), ((), ())),
        preferred_element_type=jnp.float32,
    )


def positions_of(axis):
    return lax.broadcasted_iota(jnp.int32, (WIN, WIN), axis)


def linear_bucket(offset):
    return jnp.clip(offset, -(NB // 2), NB // 2 - 1) + NB // 2


def lane_halves():
    lane = lax.broadcasted_iota(jnp.int32, (1, 2 * DH), 1)
    first = (lane < DH).astype(jnp.float32)
    return first.astype(jnp.bfloat16), (1.0 - first).astype(jnp.bfloat16)


def forward_kernel(
    x_ref, buckets, live, lengths, vectors, up_shift, table, w_in_hbm, w_out_hbm, w_up_hbm,
    w_down_hbm, out_ref, q_ref, k_ref, v_ref, o_ref, p_ref, low_ref, n1_ref, r1_ref, slope_ref,
    g_ref, n2_ref, r2_ref, w_in, w_out, w_up, w_down, allowed, y1, total, sem,
):
    loads = [
        pltpu.make_async_copy(source, target, sem.at[at])
        for at, (source, target) in enumerate(
            ((w_in_hbm, w_in), (w_out_hbm, w_out), (w_up_hbm, w_up), (w_down_hbm, w_down))
        )
    ]
    for load in loads:
        load.start()
    rows, width = x_ref.shape
    windows = rows // WIN
    row, column = positions_of(0), positions_of(1)
    offset = linear_bucket(column - row)
    first, second = lane_halves()
    for w in range(windows):
        row_doc, column_doc = jnp.zeros_like(row), jnp.zeros_like(column)
        end = 0
        for k in range(lengths.shape[1]):
            end = end + lengths[w, k]
            row_doc = row_doc + (row >= end).astype(jnp.int32)
            column_doc = column_doc + (column >= end).astype(jnp.int32)
        alive = jnp.broadcast_to(live[w : w + 1, :], (WIN, WIN))
        seen = (row_doc == column_doc) & ((alive == 1) | (row == column))
        allowed[w] = seen.astype(jnp.int32)

    loads[0].wait()
    inputs = x_ref[...]
    q_ref[...] = (
        (jnp.dot(inputs, w_in[:, :width], preferred_element_type=jnp.float32) + vectors[0:1, :])
        * DH ** (-0.5)
    ).astype(jnp.bfloat16)
    k_ref[...] = jnp.dot(
        inputs, w_in[:, width : 2 * width], preferred_element_type=jnp.float32
    ).astype(jnp.bfloat16)
    v_ref[...] = (
        jnp.dot(inputs, w_in[:, 2 * width :], preferred_element_type=jnp.float32)
        + vectors[1:2, :]
    ).astype(jnp.bfloat16)

    def attend(w, pair):
        span = pl.ds(w * WIN, WIN)
        lanes = pl.ds(pl.multiple_of(pair * 2 * DH, 2 * DH), 2 * DH)
        queries, keys, values = q_ref[span, lanes], k_ref[span, lanes], v_ref[span, lanes]
        mixed = []
        for side, half in enumerate((first, second)):
            head = pair * 2 + side
            scores = contract(queries * half, keys, 1, 1)
            bias = 0.0
            for kind, index in enumerate((offset, buckets[0, span, :], buckets[1, span, :])):
                entries = jnp.broadcast_to(table[kind, pl.ds(head, 1), :], (WIN, WIN))
                bias = bias + jnp.take_along_axis(
                    entries, index, axis=1, mode="promise_in_bounds"
                )
            scores = jnp.where(allowed[w] == 1, scores + bias, -1e30)
            exponent = jnp.exp(scores - jnp.max(scores, axis=-1, keepdims=True))
            probs = exponent / jnp.sum(exponent, axis=-1, keepdims=True)
            p_ref[w * H + head] = probs
            mixed.append(
                jnp.dot(
                    probs.astype(jnp.bfloat16), values * half, preferred_element_type=jnp.float32
                )
            )
        o_ref[span, lanes] = (mixed[0] + mixed[1]).astype(jnp.bfloat16)

    for w in range(windows):

        @pl.loop(0, H // 4)
        def _(quad, w=w):
            attend(w, quad * 2)
            attend(w, quad * 2 + 1)

    loads[1].wait()
    attended = (
        jnp.dot(o_ref[...], w_out[...], preferred_element_type=jnp.float32) + vectors[2:3, :]
    )
    first_norm, normed, inverse = norm_forward(
        inputs.astype(jnp.float32) + attended, vectors[6:7, :], vectors[3:4, :]
    )
    n1_ref[...] = normed
    r1_ref[...] = jnp.broadcast_to(inverse, r1_ref.shape)
    y1[...] = first_norm
    low_ref[...] = first_norm.astype(jnp.bfloat16)
    total[...] = jnp.zeros_like(total)
    loads[2].wait()
    loads[3].wait()

    @pl.loop(0, w_up.shape[1] // width)
    def _(at):
        lanes = pl.ds(pl.multiple_of(at * width, width), width)
        hidden = (
            jnp.dot(low_ref[...], w_up[:, lanes], preferred_element_type=jnp.float32)
            + up_shift[:, lanes]
        )
        mass = 0.5 + 0.5 * lax.erf(hidden * 0.5**0.5)
        slope_ref[:, lanes] = mass + hidden * jnp.exp(-0.5 * hidden * hidden) * (
            0.5 / math.pi
        ) ** 0.5
        active = (hidden * mass).astype(jnp.bfloat16)
        g_ref[:, lanes] = active
        total[...] += jnp.dot(active, w_down[lanes, :], preferred_element_type=jnp.float32)

    result, normed, inverse = norm_forward(
        y1[...] + (total[...] + vectors[4:5, :]), vectors[7:8, :], vectors[5:6, :]
    )
    n2_ref[...] = normed
    r2_ref[...] = jnp.broadcast_to(inverse, r2_ref.shape)
    out_ref[...] = result.astype(jnp.bfloat16)


def forward_layer(inputs, weights, buckets, live, lengths):
    w_in, w_out, w_up, w_down, vectors, up_shift, table = weights
    rows, width = inputs.shape
    hidden = w_up.shape[1]
    low, full = jnp.bfloat16, jnp.float32
    narrow = jax.ShapeDtypeStruct((rows, width), low)
    wide = jax.ShapeDtypeStruct((rows, width), full)
    column = jax.ShapeDtypeStruct((rows, WIN), full)
    vmem = pl.BlockSpec(memory_space=pltpu.MemorySpace.VMEM)
    hbm = pl.BlockSpec(memory_space=pltpu.MemorySpace.HBM)
    smem = pl.BlockSpec(memory_space=pltpu.MemorySpace.SMEM)
    return pl.pallas_call(
        forward_kernel,
        out_shape=[
            narrow, narrow, narrow, narrow, narrow,
            jax.ShapeDtypeStruct((rows // WIN * H, WIN, WIN), full),
            narrow, wide, column,
            jax.ShapeDtypeStruct((rows, hidden), full),
            jax.ShapeDtypeStruct((rows, hidden), low),
            wide, column,
        ],
        in_specs=[vmem, vmem, vmem, smem, vmem, vmem, vmem, hbm, hbm, hbm, hbm],
        out_specs=[vmem] * 13,
        scratch_shapes=[
            pltpu.VMEM(w_in.shape, low), pltpu.VMEM(w_out.shape, low),
            pltpu.VMEM(w_up.shape, low), pltpu.VMEM(w_down.shape, low),
            pltpu.VMEM((rows // WIN, WIN, WIN), jnp.int32),
            pltpu.VMEM((rows, width), full), pltpu.VMEM((rows, width), full),
            pltpu.SemaphoreType.DMA((4,)),
        ],
        compiler_params=pltpu.CompilerParams(vmem_limit_bytes=56 * 1024 * 1024),
    )(inputs, buckets, live, lengths, vectors, up_shift, table, w_in, w_out, w_up, w_down)


def backward_kernel(
    dz_ref, n2_ref, r2_ref, slope_ref, n1_ref, r1_ref, p_ref, q_ref, k_ref, v_ref, buckets,
    vectors, w_down_hbm, w_up_hbm, w_out_hbm, w_in_hbm, dx_ref, df_ref, du_ref, da_ref, dqkv_ref,
    small_ref, w_down, w_up, w_out, w_in, small, grad, mixed, spread, sem,
):
    loads = [
        pltpu.make_async_copy(source, target, sem.at[at])
        for at, (source, target) in enumerate(
            ((w_down_hbm, w_down), (w_up_hbm, w_up), (w_out_hbm, w_out), (w_in_hbm, w_in))
        )
    ]
    for load in loads:
        load.start()
    rows, width = dz_ref.shape
    windows = rows // WIN
    first, second = lane_halves()
    small[...] = jnp.zeros_like(small)
    spread[...] = jnp.zeros_like(spread)

    def add_row(at, values):
        small[pl.ds(at, 1), :] = jnp.sum(values, axis=0, keepdims=True)

    def norm_back(incoming, normed, inverse, gain_row):
        scaled = incoming * gain_row
        centred = (
            scaled
            - jnp.mean(scaled, axis=-1, keepdims=True)
            - normed * jnp.mean(scaled * normed, axis=-1, keepdims=True)
        )
        return centred * inverse

    incoming, normed = dz_ref[...], n2_ref[...]
    add_row(7, incoming * normed)
    add_row(5, incoming)
    grad_second = norm_back(incoming, normed, r2_ref[:, 0:1], vectors[7:8, :])
    grad[...] = grad_second
    branch_low = grad_second.astype(jnp.bfloat16)
    df_ref[...] = branch_low
    add_row(4, branch_low.astype(jnp.float32))
    loads[0].wait()
    loads[1].wait()

    @pl.loop(0, w_up.shape[1] // width)
    def _(at):
        lanes = pl.ds(pl.multiple_of(at * width, width), width)
        grad_active = contract(df_ref[...], w_down[lanes, :], 1, 1)
        hidden_low = (grad_active * slope_ref[:, lanes]).astype(jnp.bfloat16)
        du_ref[:, lanes] = hidden_low
        add_row(8 + at, hidden_low.astype(jnp.float32))
        grad[...] += contract(hidden_low, w_up[:, lanes], 1, 1)

    incoming, normed = grad[...], n1_ref[...]
    add_row(6, incoming * normed)
    add_row(3, incoming)
    grad_attended = norm_back(incoming, normed, r1_ref[:, 0:1], vectors[6:7, :])
    grad[...] = grad_attended
    attended_low = grad_attended.astype(jnp.bfloat16)
    da_ref[...] = attended_low
    add_row(2, attended_low.astype(jnp.float32))
    loads[2].wait()
    mixed[...] = contract(attended_low, w_out[...], 1, 1).astype(jnp.bfloat16)

    def attend(w, pair):
        span = pl.ds(w * WIN, WIN)
        start = pl.multiple_of(pair * 2 * DH, 2 * DH)
        lanes = pl.ds(start, 2 * DH)
        queries, keys, values = q_ref[span, lanes], k_ref[span, lanes], v_ref[span, lanes]
        outgoing = mixed[span, lanes]
        sums = [0.0, 0.0, 0.0]
        for side, half in enumerate((first, second)):
            head = pair * 2 + side
            probs = p_ref[w * H + head]
            own = outgoing * half
            grad_probs = contract(own, values, 1, 1)
            centred = grad_probs - jnp.sum(probs * grad_probs, axis=-1, keepdims=True)
            grad_scores = (probs * centred).astype(jnp.bfloat16)
            spread[pl.ds(head, WIN, stride=16), :] = grad_scores.astype(jnp.float32)
            sums[0] += jnp.dot(grad_scores, keys * half, preferred_element_type=jnp.float32)
            sums[1] += contract(grad_scores, queries * half, 0, 0)
            sums[2] += contract(probs.astype(jnp.bfloat16), own, 0, 0)
        scaled = sums[0].astype(jnp.bfloat16).astype(jnp.float32) * DH ** (-0.5)
        dqkv_ref[span, lanes] = scaled.astype(jnp.bfloat16)
        dqkv_ref[span, pl.ds(pl.multiple_of(start + width, 2 * DH), 2 * DH)] = sums[1].astype(
            jnp.bfloat16
        )
        dqkv_ref[span, pl.ds(pl.multiple_of(start + 2 * width, 2 * DH), 2 * DH)] = sums[2].astype(
            jnp.bfloat16
        )

    bucket = lax.broadcasted_iota(jnp.int32, (NB, WIN), 0)
    column = lax.broadcasted_iota(jnp.int32, (1, WIN), 1)
    group = 8
    for w in range(windows):

        @pl.loop(0, H // 4)
        def _(quad, w=w):
            attend(w, quad * 2)
            attend(w, quad * 2 + 1)

        def count_group(at, w=w):
            hits, terms = [], []
            for step in range(group):
                i = at * group + step
                indices = (
                    linear_bucket(column - i),
                    buckets[0, pl.ds(w * WIN + i, 1), :],
                    buckets[1, pl.ds(w * WIN + i, 1), :],
                )
                hits.append(
                    jnp.concatenate(
                        [(index == bucket).astype(jnp.float32) for index in indices], axis=0
                    ).astype(jnp.bfloat16)
                )
                terms.append(
                    spread[pl.ds(pl.multiple_of(i * 16, 16), 16), :].astype(jnp.bfloat16)
                )
            return contract(jnp.concatenate(terms, axis=1), jnp.concatenate(hits, axis=1), 1, 1)

        @pl.loop(0, WIN // group)
        def _(at):
            small[16:32, 0 : 3 * NB] += count_group(at)

    loads[3].wait()
    add_row(0, dqkv_ref[:, :width].astype(jnp.float32))
    add_row(1, dqkv_ref[:, 2 * width :].astype(jnp.float32))
    dx_ref[...] = grad[...] + contract(dqkv_ref[...], w_in[...], 1, 1)
    small_ref[...] = small[...].astype(jnp.bfloat16)


def backward_layer(incoming, weights, kept, buckets):
    w_in, w_out, w_up, w_down, vectors, _, _ = weights
    rows, width = incoming.shape
    hidden = w_up.shape[1]
    low, full = jnp.bfloat16, jnp.float32
    narrow = jax.ShapeDtypeStruct((rows, width), low)
    vmem = pl.BlockSpec(memory_space=pltpu.MemorySpace.VMEM)
    hbm = pl.BlockSpec(memory_space=pltpu.MemorySpace.HBM)
    q, k, v, _, p, _, n1, r1, slope, _, n2, r2 = kept
    return pl.pallas_call(
        backward_kernel,
        out_shape=[
            jax.ShapeDtypeStruct((rows, width), full),
            narrow,
            jax.ShapeDtypeStruct((rows, hidden), low),
            narrow,
            jax.ShapeDtypeStruct((rows, 3 * width), low),
            jax.ShapeDtypeStruct((64, width), low),
        ],
        in_specs=[vmem] * 12 + [hbm] * 4,
        out_specs=[vmem] * 6,
        scratch_shapes=[
            pltpu.VMEM(w_down.shape, low), pltpu.VMEM(w_up.shape, low),
            pltpu.VMEM(w_out.shape, low), pltpu.VMEM(w_in.shape, low),
            pltpu.VMEM((64, width), full), pltpu.VMEM((rows, width), full),
            pltpu.VMEM((rows, width), low), pltpu.VMEM((WIN * 16, WIN), full),
            pltpu.SemaphoreType.DMA((4,)),
        ],
        compiler_params=pltpu.CompilerParams(vmem_limit_bytes=56 * 1024 * 1024),
    )(incoming, n2, r2, slope, n1, r1, p, q, k, v, buckets, vectors, w_down, w_up, w_out, w_in)


def local(
    tokens,
    out_grad,
    mlm_mask,
    live_mask,
    doc_lengths,
    layout_buckets,
    attn_in,
    attn_out,
    ffn_in,
    ffn_out,
    biases,
    ffn_in_bias,
    gains,
    tables,
):
    shards = lax.axis_size("fsdp")
    weights_list = fetch_all(
        attn_in, attn_out, ffn_in, ffn_out, biases, ffn_in_bias, gains, tables, shards
    )
    live = live_mask.reshape(-1, WIN)
    current = tokens
    layer_inputs, kept_list, outputs = [], [], []
    for weights in weights_list:
        layer_inputs.append(current)
        current, *kept = forward_layer(current, weights, layout_buckets, live, doc_lengths)
        kept_list.append(kept)
        outputs.append(current)
    incoming = out_grad.astype(jnp.float32) * mlm_mask.astype(jnp.float32)[:, None]
    members, smalls = [], []
    for layer in reversed(range(len(weights_list))):
        kept = kept_list[layer]
        incoming, df, du, da, dqkv, small = backward_layer(
            incoming, weights_list[layer], kept, layout_buckets
        )
        pairs = ((layer_inputs[layer], dqkv), (kept[3], da), (kept[5], du), (kept[9], df))
        members = [
            jnp.einsum("nd,ne->de", left, right, preferred_element_type=jnp.float32).astype(
                jnp.bfloat16
            )
            for left, right in pairs
        ] + members
        smalls = [small] + smalls
    summed = sum_gradients(members, smalls, shards, lax.axis_size("dp"))
    return (jnp.stack(outputs), incoming) + summed


def solution(mesh):
    return jax.shard_map(
        local,
        mesh=mesh,
        in_specs=(
            P(("dp", "fsdp"), None),
            P(("dp", "fsdp"), None),
            P(("dp", "fsdp")),
            P(("dp", "fsdp")),
            P(("dp", "fsdp"), None),
            P(None, ("dp", "fsdp"), None),
            P(None, "fsdp", None),
            P(None, "fsdp", None),
            P(None, "fsdp", None),
            P(None, "fsdp", None),
            P(None, None, "fsdp"),
            P(None, "fsdp"),
            P(None, None, "fsdp"),
            P(None, None, "fsdp", None),
        ),
        out_specs=(
            P(None, ("dp", "fsdp"), None),
            P(("dp", "fsdp"), None),
            P(None, "fsdp", None),
            P(None, "fsdp", None),
            P(None, "fsdp", None),
            P(None, "fsdp", None),
            P(None, None, "fsdp"),
            P(None, "fsdp"),
            P(None, None, "fsdp"),
            P(None, None, "fsdp", None),
        ),
        check_vma=False,
    )
```

```python
import functools
import math
from typing import NamedTuple

import jax
import jax.numpy as jnp
from jax import lax
from jax.experimental import pallas as pl
from jax.experimental.pallas import tpu as pltpu
from jax.sharding import PartitionSpec as P

H = 12
DH = 64
NB = 32
WIN = 128


EPSILON = 1e-05
LAG = 1


def norm_forward(values, gain_row, shift_row):
    centre = values - jnp.mean(values, axis=-1, keepdims=True)
    spread = jnp.mean(centre * centre, axis=-1, keepdims=True)
    inverse = lax.rsqrt(spread + EPSILON)
    normed = centre * inverse
    return (normed * gain_row + shift_row, normed, inverse)


MESH = pl.DeviceIdType.MESH
CHUNK_TILES = 1


def add_rows(target, other):
    target[...] = (target[...].astype(jnp.float32) + other[...].astype(jnp.float32)).astype(
        jnp.bfloat16
    )


def reduce_kernel(high, count, segments, members, *refs):
    sources, targets = refs[:members], refs[members : 2 * members]
    (own, core_in, x_in, y_in, z_in, full, load_sem, core_sem, x_sem, y_sem, z_sem, zg_sem,
     yg_sem, sent, out_sem) = refs[2 * members :]
    dp = lax.axis_index("dp")
    shard = lax.axis_index("fsdp")
    y_at, z_at = lax.rem(dp, 2), lax.div(dp, 2)
    x_at, core = lax.div(shard, 2), lax.rem(shard, 2)
    core_peer = (dp, x_at * 2 + 1 - core)
    x_peer = (dp, (1 - x_at) * 2 + core)
    y_peer = (z_at * 2 + 1 - y_at, shard)
    z_of = [lax.rem(z_at + step, high) for step in range(high)]
    z_from = [lax.rem(z_at + high - step, high) for step in range(high)]
    z_peers = [(z_of[step] * 2 + y_at, shard) for step in range(high)]
    chunk = own.shape[2]
    half = chunk // 2
    piece = half // high

    barrier = pltpu.get_barrier_semaphore()
    peers = [core_peer, x_peer, y_peer] + z_peers[1:]
    for peer in peers:
        pl.semaphore_signal(barrier, inc=1, device_id=peer, device_id_type=MESH)
    pl.semaphore_wait(barrier, len(peers))

    def remote(source, target, send_at, receive, peer):
        return pltpu.make_async_remote_copy(
            src_ref=source, dst_ref=target, send_sem=sent.at[send_at], recv_sem=receive,
            device_id=peer, device_id_type=MESH,
        )

    def source_of(segment, wanted):
        ref = sources[segment.member]
        start = pl.multiple_of(wanted * segment.depth + segment.row, 16)
        return ref.at[pl.ds(start, segment.rows), pl.ds(segment.column, own.shape[3])]

    def slot_of(buffer, k, j, segment):
        return buffer.at[k, j, pl.ds(segment.at, segment.rows)]

    def load_arrival(k, j):
        slot = own.at[k, j]
        return pltpu.make_async_copy(slot, slot, load_sem.at[k, j])

    def core_arrival(k, j):
        return remote(core_in.at[k, j], core_in.at[k, j], 0, core_sem.at[k, j], core_peer)

    def x_send(k):
        return remote(own.at[k, 1], x_in.at[k], 1, x_sem.at[k], x_peer)

    def y_rows(side):
        return pl.ds(pl.multiple_of(side * half, half), half)

    def y_send(k):
        return remote(own.at[k, 0, y_rows(1 - y_at)], y_in.at[k], 2, y_sem.at[k], y_peer)

    def z_rows(at):
        return pl.ds(pl.multiple_of(y_at * half + at * piece, piece), piece)

    def z_send(k, step):
        return remote(
            own.at[k, 0, z_rows(z_of[step])], z_in.at[k, step - 1], 3,
            z_sem.at[k, step - 1], z_peers[step],
        )

    def zg_send(k, step):
        mine = full.at[k, z_rows(z_at)]
        return remote(mine, mine, 4, zg_sem.at[k, step - 1], z_peers[step])

    def zg_arrival(k, step):
        theirs = full.at[k, z_rows(z_from[step])]
        return remote(theirs, theirs, 4, zg_sem.at[k, step - 1], z_peers[step])

    def yg_send(k):
        mine = full.at[k, y_rows(y_at)]
        return remote(mine, mine, 5, yg_sem.at[k], y_peer)

    def store_end(k):
        return pltpu.make_async_copy(full.at[k], full.at[k], out_sem.at[k])

    for segment in segments:
        k = segment.chunk
        for j in (1, 0):
            x_wanted = x_at if j == 0 else 1 - x_at
            remote(
                source_of(segment, x_wanted * 2 + 1 - core), slot_of(core_in, k, j, segment),
                0, core_sem.at[k, j], core_peer,
            ).start()
            pltpu.make_async_copy(
                source_of(segment, x_wanted * 2 + core), slot_of(own, k, j, segment),
                load_sem.at[k, j],
            ).start()

    def stage_core(k):
        for j in (1, 0):
            load_arrival(k, j).wait()
            core_arrival(k, j).wait_recv()
            add_rows(own.at[k, j], core_in.at[k, j])
            if j == 1:
                x_send(k).start()

    def stage_x(k):
        x_send(k).wait_recv()
        add_rows(own.at[k, 0], x_in.at[k])
        y_send(k).start()

    def stage_y(k):
        y_send(k).wait_recv()
        add_rows(own.at[k, 0, y_rows(y_at)], y_in.at[k])
        for step in range(1, high):
            z_send(k, step).start()

    def stage_z(k):
        total = own[k, 0, z_rows(z_at), :].astype(jnp.float32)
        for step in range(1, high):
            z_send(k, step).wait_recv()
            total = total + z_in[k, step - 1].astype(jnp.float32)
        full[k, z_rows(z_at), :] = total.astype(jnp.bfloat16)
        for step in range(1, high):
            zg_send(k, step).start()

    def stage_spread(k):
        for step in range(1, high):
            zg_arrival(k, step).wait_recv()
        yg_send(k).start()

    def stage_store(k):
        yg_send(k).wait_recv()
        for segment in segments:

            @pl.when(k == segment.chunk)
            def _(segment=segment):
                target = targets[segment.member].at[
                    pl.ds(segment.row, segment.rows), pl.ds(segment.column, own.shape[3])
                ]
                pltpu.make_async_copy(
                    full.at[segment.chunk, pl.ds(segment.at, segment.rows)], target,
                    out_sem.at[segment.chunk],
                ).start()

    stages = (stage_core, stage_x, stage_y, stage_z, stage_spread, stage_store)
    lags = (0, LAG, 2 * LAG, 3 * LAG, 4 * LAG, 5 * LAG)

    @pl.loop(0, count + lags[-1])
    def _(t):
        for stage, lag in zip(stages, lags):
            k = t - lag

            @pl.when((k >= 0) & (k < count))
            def _():
                stage(k)

    def all_sent(source, target, send_at, peer):
        remote(source, target, send_at, x_sem.at[0], peer).wait_send()

    all_sent(own, core_in, 0, core_peer)
    all_sent(x_in, x_in, 1, x_peer)
    all_sent(y_in, y_in, 2, y_peer)
    all_sent(z_in, z_in, 3, z_peers[1])
    all_sent(z_in, z_in, 4, z_peers[1])
    all_sent(y_in, y_in, 5, y_peer)

    @pl.loop(0, count)
    def _(k):
        store_end(k).wait()


class Segment(NamedTuple):
    member: int
    depth: int
    row: int
    column: int
    rows: int
    chunk: int
    at: int


def plan_segments(members, depths, strides, width, chunk):
    segments, place = [], 0
    for member, array in enumerate(members):
        depth = depths[member]
        for column in range(0, array.shape[1], width):
            row = 0
            while row < depth:
                rows = min(depth - row, chunk - place % chunk)
                segments.append(
                    Segment(
                        member, strides[member], row, column, rows, place // chunk, place % chunk
                    )
                )
                row, place = row + rows, place + rows
    return tuple(segments), place


def reduce_gradients(members, smalls, shards, group, width):
    high = group // 2
    chunk = chunk_rows(group)
    depths = [array.shape[0] // shards for array in members]
    strides = depths + [0] * len(smalls)
    depths += [array.shape[0] for array in smalls]
    filled = sum(
        array.shape[1] // width * depth for array, depth in zip(members + smalls, depths)
    )
    rest = -filled % chunk
    members = members + smalls
    if rest:
        members = members + [jnp.zeros((rest, width), jnp.bfloat16)]
        depths.append(rest)
        strides.append(0)
    segments, rows = plan_segments(members, depths, strides, width, chunk)
    count = rows // chunk
    piece = chunk // group
    buffers = [
        (count, 2, chunk, width),
        (count, 2, chunk, width),
        (count, chunk, width),
        (count, chunk // 2, width),
        (count, high - 1, piece, width),
        (count, chunk, width),
    ]
    semaphores = [(count, 2), (count, 2), (count,), (count,), (count, high - 1),
                  (count, high - 1), (count,), (6,), (count,)]
    hbm = pl.BlockSpec(memory_space=pltpu.MemorySpace.HBM)
    return pl.pallas_call(
        functools.partial(reduce_kernel, high, count, segments, len(members)),
        out_shape=[
            jax.ShapeDtypeStruct((depth, array.shape[1]), jnp.bfloat16)
            for array, depth in zip(members, depths)
        ],
        in_specs=[hbm] * len(members),
        out_specs=[hbm] * len(members),
        scratch_shapes=[pltpu.VMEM(shape, jnp.bfloat16) for shape in buffers]
        + [pltpu.SemaphoreType.DMA(shape) for shape in semaphores],
        compiler_params=pltpu.CompilerParams(
            collective_id=1, has_side_effects=True, vmem_limit_bytes=64 * 1024 * 1024 - 65536
        ),
    )(*members)


def chunk_rows(group):
    return 16 * CHUNK_TILES * group


def sum_gradients(members, smalls, shards, group):
    width = smalls[0].shape[1]
    layers = len(smalls)
    reduced = reduce_gradients(members, smalls, shards, group, width)
    spans = [
        jnp.stack([reduced[4 * layer + member] for layer in range(layers)]).astype(jnp.float32)
        for member in range(4)
    ]
    small = jnp.stack(reduced[4 * layers : 5 * layers]).astype(jnp.float32)
    depth = width // shards
    shard = lax.axis_index("fsdp")
    rows = lax.dynamic_slice_in_dim(small[:, :8], shard * depth, depth, axis=2)
    up_shift = lax.dynamic_slice_in_dim(small, 8 + shard, 1, axis=1)[:, 0]
    table = small[:, 16 : 16 + H, : 3 * NB].reshape(layers, H, 3, NB)
    table = lax.dynamic_slice_in_dim(table, shard * (NB // shards), NB // shards, axis=3)
    return tuple(spans) + (
        rows[:, :6], up_shift, rows[:, 6:], jnp.transpose(table, (0, 2, 3, 1)),
    )


def opening_kernel(items, *refs):
    total = len(items)
    ready = 1 + 4
    sources, forward_in = refs[:5], refs[5:9]
    outs = refs[9 : 9 + total - 1 + 3 + 13]
    vectors, up_shifts, table = outs[total - 1 : total + 2]
    forward_out = outs[total + 2 :]
    rest = refs[9 + len(outs) :]
    stages, rest = rest[:total], rest[total:]
    landing_small, load_sem, store_sem, send_sem, arrive = rest[:5]
    forward_scratch = rest[5:]
    targets = (landing_small,) + tuple(outs[: total - 1])
    dp = lax.axis_index("dp")
    shard = lax.axis_index("fsdp")
    x_at, core = lax.div(shard, 2), lax.rem(shard, 2)
    bits = (lax.rem(dp, 2), lax.rem(lax.div(dp, 2), 2))
    core_peer = (dp, x_at * 2 + 1 - core)
    other = (1 - x_at) * 2 + core
    x_peer = (dp, other)
    dp_peers = [
        (dp + 1 - 2 * bits[0], shard),
        (dp + 2 - 4 * bits[1], shard),
    ]
    barrier = pltpu.get_barrier_semaphore()
    for peer in [core_peer, x_peer] + dp_peers:
        pl.semaphore_signal(barrier, inc=1, device_id=peer, device_id_type=MESH)
    pl.semaphore_wait(barrier, 4)

    def copy(source, target, item, kind, peer):
        return pltpu.make_async_remote_copy(
            src_ref=source, dst_ref=target, send_sem=send_sem.at[item, kind],
            recv_sem=arrive.at[item, kind], device_id=peer, device_id_type=MESH,
        )

    def shard_of(i):
        member, layer = items[i]
        return sources[member] if layer is None else sources[member].at[layer]

    def depth_of(i):
        return stages[i].shape[0]

    def parts_of(i):
        return 1 if i == 0 else 4

    def small_lanes(at):
        size = stages[0].shape[1]
        return landing_small.at[:, pl.ds(pl.multiple_of(at * size, size), size)]

    def mine_out(i):
        if i == 0:
            return small_lanes(shard)
        n = depth_of(i)
        return targets[i].at[pl.ds(pl.multiple_of(shard * n, 16), n)]

    def other_out(i, quarter):
        n = depth_of(i)
        part = n // parts_of(i)
        return targets[i].at[pl.ds(pl.multiple_of(other * n + quarter * part, 16), part)]

    def other_whole(i):
        if i == 0:
            return small_lanes(other)
        n = depth_of(i)
        return targets[i].at[pl.ds(pl.multiple_of(other * n, 16), n)]

    def order_of(i):
        return (0, 1) if i % 2 == 0 else (1, 0)

    def quarter_of(i, flips):
        if parts_of(i) == 1:
            return 0
        now = [bits[axis] if axis not in flips else 1 - bits[axis] for axis in (0, 1)]
        return now[1] * 2 + now[0]

    def x_send(i):
        if i == 0:
            return copy(shard_of(i), small_lanes(shard), i, 0, x_peer)
        n = depth_of(i)
        part = n // parts_of(i)
        start = pl.multiple_of(quarter_of(i, ()) * part, 16)
        rows = pl.ds(start, part)
        landing = targets[i].at[pl.ds(pl.multiple_of(shard * n + start, 16), part)]
        return copy(shard_of(i).at[rows], landing, i, 0, x_peer)

    def first_send(i):
        mine = other_out(i, quarter_of(i, ()))
        return copy(mine, mine, i, 1, dp_peers[order_of(i)[0]])

    def second_send(i):
        mine = other_out(i, quarter_of(i, ()))
        return copy(mine, mine, i, 2, dp_peers[order_of(i)[1]])

    def relay_send(i):
        mine = other_out(i, quarter_of(i, (order_of(i)[0],)))
        return copy(mine, mine, i, 3, dp_peers[order_of(i)[1]])

    def own_share(i):
        return copy(shard_of(i), mine_out(i), i, 4, core_peer)

    def far_share(i):
        return copy(other_whole(i), other_whole(i), i, 5, core_peer)

    def load(i):
        return pltpu.make_async_copy(shard_of(i), stages[i], load_sem.at[i])

    def store(i):
        return pltpu.make_async_copy(stages[i], mine_out(i), store_sem.at[i])

    for i in range(total):
        x_send(i).start()
    for i in range(total):
        own_share(i).start()
        load(i).start()

    def spread(i):
        x_send(i).wait_recv()
        if parts_of(i) == 4:
            first_send(i).start()
            second_send(i).start()
        load(i).wait()
        store(i).start()

    def relay(i):
        if parts_of(i) == 4:
            first_send(i).wait_recv()
            relay_send(i).start()

    def share(i):
        if parts_of(i) == 4:
            second_send(i).wait_recv()
            relay_send(i).wait_recv()
        far_share(i).start()

    def arrived(i):
        own_share(i).wait_recv()
        far_share(i).wait_recv()
        store(i).wait()

    for step in range(ready + 3):
        if step < ready:
            spread(step)
        elif step < total:
            spread(step)
        if 0 <= step - 1 < ready:
            relay(step - 1)
        if 0 <= step - 3 < ready:
            share(step - 3)
    for i in range(ready):
        arrived(i)
    place_small(landing_small, vectors, up_shifts, table)

    waiting = [functools.partial(spread, i) for i in range(ready + 3, total)]
    waiting += [functools.partial(relay, i) for i in range(ready, total)]
    waiting += [functools.partial(share, i) for i in range(ready, total)]
    points = 4
    per_point = -(-len(waiting) // points)

    def service(point):
        for act in waiting[point * per_point : (point + 1) * per_point]:
            act()

    forward_core(
        0, service, *forward_in, vectors, up_shifts, table, *targets[1:5], *forward_out,
        *forward_scratch,
    )
    for i in range(ready, total):
        arrived(i)
    for i in range(total):
        own_share(i).wait_send()
        far_share(i).wait_send()
        x_send(i).wait_send()
        if parts_of(i) == 4:
            first_send(i).wait_send()
            second_send(i).wait_send()
            relay_send(i).wait_send()


def place_small(landing, vectors, up_shifts, table):
    lanes = landing.shape[1]
    each = 2 * WIN
    shards = lanes // each

    def selected(rows, own, width):
        source = lax.broadcasted_iota(jnp.int32, (lanes, width), 0)
        target = lax.broadcasted_iota(jnp.int32, (lanes, width), 1)
        within = source % each
        picked = (within < own) & (target == source // each * own + within)
        return jnp.dot(
            landing[rows, :], picked.astype(jnp.float32).astype(jnp.bfloat16),
            preferred_element_type=jnp.float32,
        )

    layers = up_shifts.shape[0]
    width = vectors.shape[1]
    vectors[...] = selected(pl.ds(0, 16), width // shards, width)
    shift_rows = landing[16:32, :].astype(jnp.float32)
    runs = width // each
    for layer in range(layers):
        for shard in range(shards):
            for run in range(runs):
                start = shard * width + run * each
                up_shifts[layer : layer + 1, start : start + each] = shift_rows[
                    layer * runs + run : layer * runs + run + 1,
                    shard * each : (shard + 1) * each,
                ]
    table[...] = selected(pl.ds(32, table.shape[0]), NB // shards, WIN)


def small_rows(biases, ffn_in_bias, gains, tables):
    layers = biases.shape[0]
    each = 2 * WIN
    vectors = jnp.concatenate([biases, gains], axis=1).reshape(layers * 8, -1)
    vectors = jnp.pad(vectors, ((0, 16 - 8 * layers), (0, each - vectors.shape[1])))
    shifts = ffn_in_bias.reshape(-1, each)
    shifts = jnp.pad(shifts, ((0, 16 - shifts.shape[0]), (0, 0)))
    entries = jnp.swapaxes(tables, 2, 3)
    entries = jnp.pad(
        entries, ((0, 0), (0, 0), (0, 16 - H), (0, each - entries.shape[3]))
    ).reshape(layers * 48, each)
    return jnp.concatenate([vectors, shifts, entries], axis=0)


def open_layers(sources, small, shards, inputs, buckets, live, lengths):
    layers = sources[0].shape[0]
    rows, width = inputs.shape
    items = [(4, None)] + [(member, layer) for layer in range(layers) for member in range(4)]
    forms = [small.shape] + [sources[member].shape[1:] for member, _ in items[1:]]
    total = len(items)
    hidden = sources[2].shape[2]
    outs, scratch = forward_forms(rows, width, hidden)
    vmem, hbm, smem = memory_specs()
    shared = [
        jax.ShapeDtypeStruct((16, width), jnp.float32),
        jax.ShapeDtypeStruct((layers, hidden), jnp.float32),
        jax.ShapeDtypeStruct((layers * 48, WIN), jnp.float32),
    ]
    results = pl.pallas_call(
        functools.partial(opening_kernel, tuple(items)),
        out_shape=[
            jax.ShapeDtypeStruct((form[0] * shards, form[1]), jnp.bfloat16) for form in forms[1:]
        ]
        + shared
        + outs,
        in_specs=[hbm] * 5 + [vmem, vmem, vmem, smem],
        out_specs=[hbm] * (total - 1) + [vmem] * (3 + len(outs)),
        scratch_shapes=[pltpu.VMEM(form, jnp.bfloat16) for form in forms]
        + [
            pltpu.VMEM((small.shape[0], small.shape[1] * shards), jnp.bfloat16),
            pltpu.SemaphoreType.DMA((total,)),
            pltpu.SemaphoreType.DMA((total,)),
            pltpu.SemaphoreType.DMA((total, 6)),
            pltpu.SemaphoreType.DMA((total, 6)),
        ]
        + scratch,
        compiler_params=pltpu.CompilerParams(
            collective_id=0, has_side_effects=True, vmem_limit_bytes=58 * 1024 * 1024
        ),
    )(*sources, small, inputs, buckets, live, lengths)
    weights = [results[4 * layer : 4 * layer + 4] for layer in range(layers)]
    return weights, results[total - 1 : total + 2], results[total + 2 :]


def contract(left, right, left_axis, right_axis):
    return lax.dot_general(
        left, right, (((left_axis,), (right_axis,)), ((), ())),
        preferred_element_type=jnp.float32,
    )


def positions_of(axis):
    return lax.broadcasted_iota(jnp.int32, (WIN, WIN), axis)


def linear_bucket(offset):
    return jnp.clip(offset, -(NB // 2), NB // 2 - 1) + NB // 2


def lane_halves():
    lane = lax.broadcasted_iota(jnp.int32, (1, 2 * DH), 1)
    first = (lane < DH).astype(jnp.float32)
    return first.astype(jnp.bfloat16), (1.0 - first).astype(jnp.bfloat16)


def forward_kernel(layer, *refs):
    forward_core(layer, lambda point: None, *refs)


def forward_core(
    layer, service, x_ref, buckets, live, lengths, all_vectors, up_shifts, table, w_in_hbm,
    w_out_hbm, w_up_hbm, w_down_hbm, out_ref, q_ref, k_ref, v_ref, o_ref, p_ref, low_ref, n1_ref, r1_ref, slope_ref,
    g_ref, n2_ref, r2_ref, w_in, w_out, w_up, w_down, allowed, y1, total, sem,
):
    loads = [
        pltpu.make_async_copy(source, target, sem.at[at])
        for at, (source, target) in enumerate(
            ((w_in_hbm, w_in), (w_out_hbm, w_out), (w_up_hbm, w_up), (w_down_hbm, w_down))
        )
    ]
    for load in loads:
        load.start()
    vectors = all_vectors.at[pl.ds(8 * layer, 8)]
    up_shift = up_shifts.at[pl.ds(layer, 1)]
    rows, width = x_ref.shape
    windows = rows // WIN
    row, column = positions_of(0), positions_of(1)
    offset = linear_bucket(column - row)
    first, second = lane_halves()
    for w in range(windows):
        row_doc, column_doc = jnp.zeros_like(row), jnp.zeros_like(column)
        end = 0
        for k in range(lengths.shape[1]):
            end = end + lengths[w, k]
            row_doc = row_doc + (row >= end).astype(jnp.int32)
            column_doc = column_doc + (column >= end).astype(jnp.int32)
        alive = jnp.broadcast_to(live[w : w + 1, :], (WIN, WIN))
        seen = (row_doc == column_doc) & ((alive == 1) | (row == column))
        allowed[w] = seen.astype(jnp.int32)

    loads[0].wait()
    inputs = x_ref[...]
    q_ref[...] = (
        (jnp.dot(inputs, w_in[:, :width], preferred_element_type=jnp.float32) + vectors[0:1, :])
        * DH ** (-0.5)
    ).astype(jnp.bfloat16)
    k_ref[...] = jnp.dot(
        inputs, w_in[:, width : 2 * width], preferred_element_type=jnp.float32
    ).astype(jnp.bfloat16)
    v_ref[...] = (
        jnp.dot(inputs, w_in[:, 2 * width :], preferred_element_type=jnp.float32)
        + vectors[1:2, :]
    ).astype(jnp.bfloat16)
    service(0)

    def attend(w, pair):
        span = pl.ds(w * WIN, WIN)
        lanes = pl.ds(pl.multiple_of(pair * 2 * DH, 2 * DH), 2 * DH)
        queries, keys, values = q_ref[span, lanes], k_ref[span, lanes], v_ref[span, lanes]
        mixed = []
        for side, half in enumerate((first, second)):
            head = pair * 2 + side
            scores = contract(queries * half, keys, 1, 1)
            bias = 0.0
            for kind, index in enumerate((offset, buckets[0, span, :], buckets[1, span, :])):
                entry = table[pl.ds(48 * layer + 16 * kind + head, 1), :]
                entries = jnp.broadcast_to(entry, (WIN, WIN))
                bias = bias + jnp.take_along_axis(
                    entries, index, axis=1, mode="promise_in_bounds"
                )
            scores = jnp.where(allowed[w] == 1, scores + bias, -1e30)
            exponent = jnp.exp(scores - jnp.max(scores, axis=-1, keepdims=True))
            probs = exponent / jnp.sum(exponent, axis=-1, keepdims=True)
            p_ref[w * H + head] = probs
            mixed.append(
                jnp.dot(
                    probs.astype(jnp.bfloat16), values * half, preferred_element_type=jnp.float32
                )
            )
        o_ref[span, lanes] = (mixed[0] + mixed[1]).astype(jnp.bfloat16)

    for w in range(windows):

        @pl.loop(0, H // 4)
        def _(quad, w=w):
            attend(w, quad * 2)
            attend(w, quad * 2 + 1)

        service(1 + w)

    loads[1].wait()
    attended = (
        jnp.dot(o_ref[...], w_out[...], preferred_element_type=jnp.float32) + vectors[2:3, :]
    )
    first_norm, normed, inverse = norm_forward(
        inputs.astype(jnp.float32) + attended, vectors[6:7, :], vectors[3:4, :]
    )
    n1_ref[...] = normed
    r1_ref[...] = jnp.broadcast_to(inverse, r1_ref.shape)
    y1[...] = first_norm
    low_ref[...] = first_norm.astype(jnp.bfloat16)
    total[...] = jnp.zeros_like(total)
    service(1 + windows)
    loads[2].wait()
    loads[3].wait()

    @pl.loop(0, w_up.shape[1] // width)
    def _(at):
        lanes = pl.ds(pl.multiple_of(at * width, width), width)
        hidden = (
            jnp.dot(low_ref[...], w_up[:, lanes], preferred_element_type=jnp.float32)
            + up_shift[:, lanes]
        )
        mass = 0.5 + 0.5 * lax.erf(hidden * 0.5**0.5)
        slope_ref[:, lanes] = mass + hidden * jnp.exp(-0.5 * hidden * hidden) * (
            0.5 / math.pi
        ) ** 0.5
        active = (hidden * mass).astype(jnp.bfloat16)
        g_ref[:, lanes] = active
        total[...] += jnp.dot(active, w_down[lanes, :], preferred_element_type=jnp.float32)

    result, normed, inverse = norm_forward(
        y1[...] + (total[...] + vectors[4:5, :]), vectors[7:8, :], vectors[5:6, :]
    )
    n2_ref[...] = normed
    r2_ref[...] = jnp.broadcast_to(inverse, r2_ref.shape)
    out_ref[...] = result.astype(jnp.bfloat16)


def forward_forms(rows, width, hidden):
    low, full = jnp.bfloat16, jnp.float32
    narrow = jax.ShapeDtypeStruct((rows, width), low)
    wide = jax.ShapeDtypeStruct((rows, width), full)
    column = jax.ShapeDtypeStruct((rows, WIN), full)
    outs = [
        narrow, narrow, narrow, narrow, narrow,
        jax.ShapeDtypeStruct((rows // WIN * H, WIN, WIN), full),
        narrow, wide, column,
        jax.ShapeDtypeStruct((rows, hidden), full),
        jax.ShapeDtypeStruct((rows, hidden), low),
        wide, column,
    ]
    scratch = [
        pltpu.VMEM((width, 3 * width), low), pltpu.VMEM((width, width), low),
        pltpu.VMEM((width, hidden), low), pltpu.VMEM((hidden, width), low),
        pltpu.VMEM((rows // WIN, WIN, WIN), jnp.int32),
        pltpu.VMEM((rows, width), full), pltpu.VMEM((rows, width), full),
        pltpu.SemaphoreType.DMA((4,)),
    ]
    return outs, scratch


def memory_specs():
    return [
        pl.BlockSpec(memory_space=space)
        for space in (
            pltpu.MemorySpace.VMEM, pltpu.MemorySpace.HBM, pltpu.MemorySpace.SMEM
        )
    ]


def forward_layer(layer, inputs, weights, shared, buckets, live, lengths):
    rows, width = inputs.shape
    outs, scratch = forward_forms(rows, width, weights[2].shape[1])
    vmem, hbm, smem = memory_specs()
    return pl.pallas_call(
        functools.partial(forward_kernel, layer),
        out_shape=outs,
        in_specs=[vmem, vmem, vmem, smem, vmem, vmem, vmem, hbm, hbm, hbm, hbm],
        out_specs=[vmem] * len(outs),
        scratch_shapes=scratch,
        compiler_params=pltpu.CompilerParams(vmem_limit_bytes=56 * 1024 * 1024),
    )(inputs, buckets, live, lengths, *shared, *weights)


def backward_kernel(
    layer, dz_ref, n2_ref, r2_ref, slope_ref, n1_ref, r1_ref, p_ref, q_ref, k_ref, v_ref, buckets,
    all_vectors, w_down_hbm, w_up_hbm, w_out_hbm, w_in_hbm, dx_ref, df_ref, du_ref, da_ref, dqkv_ref,
    small_ref, w_down, w_up, w_out, w_in, small, grad, mixed, spread, sem,
):
    loads = [
        pltpu.make_async_copy(source, target, sem.at[at])
        for at, (source, target) in enumerate(
            ((w_down_hbm, w_down), (w_up_hbm, w_up), (w_out_hbm, w_out), (w_in_hbm, w_in))
        )
    ]
    for load in loads:
        load.start()
    vectors = all_vectors.at[pl.ds(8 * layer, 8)]
    rows, width = dz_ref.shape
    windows = rows // WIN
    first, second = lane_halves()
    small[...] = jnp.zeros_like(small)
    spread[...] = jnp.zeros_like(spread)

    def add_row(at, values):
        small[pl.ds(at, 1), :] = jnp.sum(values, axis=0, keepdims=True)

    def norm_back(incoming, normed, inverse, gain_row):
        scaled = incoming * gain_row
        centred = (
            scaled
            - jnp.mean(scaled, axis=-1, keepdims=True)
            - normed * jnp.mean(scaled * normed, axis=-1, keepdims=True)
        )
        return centred * inverse

    incoming, normed = dz_ref[...], n2_ref[...]
    add_row(7, incoming * normed)
    add_row(5, incoming)
    grad_second = norm_back(incoming, normed, r2_ref[:, 0:1], vectors[7:8, :])
    grad[...] = grad_second
    branch_low = grad_second.astype(jnp.bfloat16)
    df_ref[...] = branch_low
    add_row(4, branch_low.astype(jnp.float32))
    loads[0].wait()
    loads[1].wait()

    @pl.loop(0, w_up.shape[1] // width)
    def _(at):
        lanes = pl.ds(pl.multiple_of(at * width, width), width)
        grad_active = contract(df_ref[...], w_down[lanes, :], 1, 1)
        hidden_low = (grad_active * slope_ref[:, lanes]).astype(jnp.bfloat16)
        du_ref[:, lanes] = hidden_low
        add_row(8 + at, hidden_low.astype(jnp.float32))
        grad[...] += contract(hidden_low, w_up[:, lanes], 1, 1)

    incoming, normed = grad[...], n1_ref[...]
    add_row(6, incoming * normed)
    add_row(3, incoming)
    grad_attended = norm_back(incoming, normed, r1_ref[:, 0:1], vectors[6:7, :])
    grad[...] = grad_attended
    attended_low = grad_attended.astype(jnp.bfloat16)
    da_ref[...] = attended_low
    add_row(2, attended_low.astype(jnp.float32))
    loads[2].wait()
    mixed[...] = contract(attended_low, w_out[...], 1, 1).astype(jnp.bfloat16)

    def attend(w, pair):
        span = pl.ds(w * WIN, WIN)
        start = pl.multiple_of(pair * 2 * DH, 2 * DH)
        lanes = pl.ds(start, 2 * DH)
        queries, keys, values = q_ref[span, lanes], k_ref[span, lanes], v_ref[span, lanes]
        outgoing = mixed[span, lanes]
        sums = [0.0, 0.0, 0.0]
        for side, half in enumerate((first, second)):
            head = pair * 2 + side
            probs = p_ref[w * H + head]
            own = outgoing * half
            grad_probs = contract(own, values, 1, 1)
            centred = grad_probs - jnp.sum(probs * grad_probs, axis=-1, keepdims=True)
            grad_scores = (probs * centred).astype(jnp.bfloat16)
            spread[pl.ds(head, WIN, stride=16), :] = grad_scores.astype(jnp.float32)
            sums[0] += jnp.dot(grad_scores, keys * half, preferred_element_type=jnp.float32)
            sums[1] += contract(grad_scores, queries * half, 0, 0)
            sums[2] += contract(probs.astype(jnp.bfloat16), own, 0, 0)
        scaled = sums[0].astype(jnp.bfloat16).astype(jnp.float32) * DH ** (-0.5)
        dqkv_ref[span, lanes] = scaled.astype(jnp.bfloat16)
        dqkv_ref[span, pl.ds(pl.multiple_of(start + width, 2 * DH), 2 * DH)] = sums[1].astype(
            jnp.bfloat16
        )
        dqkv_ref[span, pl.ds(pl.multiple_of(start + 2 * width, 2 * DH), 2 * DH)] = sums[2].astype(
            jnp.bfloat16
        )

    bucket = lax.broadcasted_iota(jnp.int32, (NB, WIN), 0)
    column = lax.broadcasted_iota(jnp.int32, (1, WIN), 1)
    group = 8
    for w in range(windows):

        @pl.loop(0, H // 4)
        def _(quad, w=w):
            attend(w, quad * 2)
            attend(w, quad * 2 + 1)

        def count_group(at, w=w):
            hits, terms = [], []
            for step in range(group):
                i = at * group + step
                indices = (
                    linear_bucket(column - i),
                    buckets[0, pl.ds(w * WIN + i, 1), :],
                    buckets[1, pl.ds(w * WIN + i, 1), :],
                )
                hits.append(
                    jnp.concatenate(
                        [(index == bucket).astype(jnp.float32) for index in indices], axis=0
                    ).astype(jnp.bfloat16)
                )
                terms.append(
                    spread[pl.ds(pl.multiple_of(i * 16, 16), 16), :].astype(jnp.bfloat16)
                )
            return contract(jnp.concatenate(terms, axis=1), jnp.concatenate(hits, axis=1), 1, 1)

        @pl.loop(0, WIN // group)
        def _(at):
            small[16:32, 0 : 3 * NB] += count_group(at)

    loads[3].wait()
    add_row(0, dqkv_ref[:, :width].astype(jnp.float32))
    add_row(1, dqkv_ref[:, 2 * width :].astype(jnp.float32))
    dx_ref[...] = grad[...] + contract(dqkv_ref[...], w_in[...], 1, 1)
    small_ref[...] = small[...].astype(jnp.bfloat16)


def backward_layer(layer, incoming, weights, vectors, kept, buckets):
    w_in, w_out, w_up, w_down = weights
    rows, width = incoming.shape
    hidden = w_up.shape[1]
    low, full = jnp.bfloat16, jnp.float32
    narrow = jax.ShapeDtypeStruct((rows, width), low)
    vmem, hbm, _ = memory_specs()
    q, k, v, _, p, _, n1, r1, slope, _, n2, r2 = kept
    return pl.pallas_call(
        functools.partial(backward_kernel, layer),
        out_shape=[
            jax.ShapeDtypeStruct((rows, width), full),
            narrow,
            jax.ShapeDtypeStruct((rows, hidden), low),
            narrow,
            jax.ShapeDtypeStruct((rows, 3 * width), low),
            jax.ShapeDtypeStruct((64, width), low),
        ],
        in_specs=[vmem] * 12 + [hbm] * 4,
        out_specs=[vmem] * 6,
        scratch_shapes=[
            pltpu.VMEM(w_down.shape, low), pltpu.VMEM(w_up.shape, low),
            pltpu.VMEM(w_out.shape, low), pltpu.VMEM(w_in.shape, low),
            pltpu.VMEM((64, width), full), pltpu.VMEM((rows, width), full),
            pltpu.VMEM((rows, width), low), pltpu.VMEM((WIN * 16, WIN), full),
            pltpu.SemaphoreType.DMA((4,)),
        ],
        compiler_params=pltpu.CompilerParams(vmem_limit_bytes=56 * 1024 * 1024),
    )(incoming, n2, r2, slope, n1, r1, p, q, k, v, buckets, vectors, w_down, w_up, w_out, w_in)


def local(
    tokens,
    out_grad,
    mlm_mask,
    live_mask,
    doc_lengths,
    layout_buckets,
    attn_in,
    attn_out,
    ffn_in,
    ffn_out,
    biases,
    ffn_in_bias,
    gains,
    tables,
):
    shards = lax.axis_size("fsdp")
    live = live_mask.reshape(-1, WIN)
    weights_list, shared, first = open_layers(
        (attn_in, attn_out, ffn_in, ffn_out), small_rows(biases, ffn_in_bias, gains, tables),
        shards, tokens, layout_buckets, live, doc_lengths,
    )
    current, *kept = first
    layer_inputs, kept_list, outputs = [tokens], [kept], [current]
    for layer in range(1, len(weights_list)):
        layer_inputs.append(current)
        current, *kept = forward_layer(
            layer, current, weights_list[layer], shared, layout_buckets, live, doc_lengths
        )
        kept_list.append(kept)
        outputs.append(current)
    incoming = out_grad.astype(jnp.float32) * mlm_mask.astype(jnp.float32)[:, None]
    members, smalls = [], []
    for layer in reversed(range(len(weights_list))):
        kept = kept_list[layer]
        incoming, df, du, da, dqkv, small = backward_layer(
            layer, incoming, weights_list[layer], shared[0], kept, layout_buckets
        )
        pairs = ((layer_inputs[layer], dqkv), (kept[3], da), (kept[5], du), (kept[9], df))
        members = [
            jnp.einsum("nd,ne->de", left, right, preferred_element_type=jnp.float32).astype(
                jnp.bfloat16
            )
            for left, right in pairs
        ] + members
        smalls = [small] + smalls
    summed = sum_gradients(members, smalls, shards, lax.axis_size("dp"))
    return (jnp.stack(outputs), incoming) + summed


def solution(mesh):
    return jax.shard_map(
        local,
        mesh=mesh,
        in_specs=(
            P(("dp", "fsdp"), None),
            P(("dp", "fsdp"), None),
            P(("dp", "fsdp")),
            P(("dp", "fsdp")),
            P(("dp", "fsdp"), None),
            P(None, ("dp", "fsdp"), None),
            P(None, "fsdp", None),
            P(None, "fsdp", None),
            P(None, "fsdp", None),
            P(None, "fsdp", None),
            P(None, None, "fsdp"),
            P(None, "fsdp"),
            P(None, None, "fsdp"),
            P(None, None, "fsdp", None),
        ),
        out_specs=(
            P(None, ("dp", "fsdp"), None),
            P(("dp", "fsdp"), None),
            P(None, "fsdp", None),
            P(None, "fsdp", None),
            P(None, "fsdp", None),
            P(None, "fsdp", None),
            P(None, None, "fsdp"),
            P(None, "fsdp"),
            P(None, None, "fsdp"),
            P(None, None, "fsdp", None),
        ),
        check_vma=False,
    )
```

```python
import functools
import math
from typing import NamedTuple

import jax
import jax.numpy as jnp
from jax import lax
from jax.experimental import pallas as pl
from jax.experimental.pallas import tpu as pltpu
from jax.sharding import PartitionSpec as P

H = 12
DH = 64
NB = 32
WIN = 128


EPSILON = 1e-05
LAG = 1
LAG_OWN = 1


def norm_forward(values, gain_row, shift_row):
    centre = values - jnp.mean(values, axis=-1, keepdims=True)
    spread = jnp.mean(centre * centre, axis=-1, keepdims=True)
    inverse = lax.rsqrt(spread + EPSILON)
    normed = centre * inverse
    return (normed * gain_row + shift_row, normed, inverse)


MESH = pl.DeviceIdType.MESH
CHUNK_TILES = 1


def add_rows(target, other):
    target[...] = (target[...].astype(jnp.float32) + other[...].astype(jnp.float32)).astype(
        jnp.bfloat16
    )


RING = 4


def reduce_kernel(high, chunk, segments, shards, layers, *refs):
    each = 4 * layers
    lefts, rights, smalls = refs[:each], refs[each : 2 * each], refs[2 * each : 2 * each + layers]
    refs = refs[2 * each + layers :]
    members = len(refs) - 19
    targets = refs[:members]
    (left, right, ring, total, x_in, y_in, z_in, full, load_sem, ring_sem, core_sem, small_sem,
     x_sem, y_sem, z_sem, zg_sem, yg_sem, sent) = refs[members:][:18]
    out_sem = refs[-1]
    dp = lax.axis_index("dp")
    shard = lax.axis_index("fsdp")
    y_at, z_at = lax.rem(dp, 2), lax.div(dp, 2)
    x_at, core = lax.div(shard, 2), lax.rem(shard, 2)
    core_peer = (dp, x_at * 2 + 1 - core)
    x_peer = (dp, (1 - x_at) * 2 + core)
    y_peer = (z_at * 2 + 1 - y_at, shard)
    z_of = [lax.rem(z_at + step, high) for step in range(high)]
    z_from = [lax.rem(z_at + high - step, high) for step in range(high)]
    z_peers = [(z_of[step] * 2 + y_at, shard) for step in range(high)]
    half = chunk // 2
    piece = half // high
    width = full.shape[2]
    count = full.shape[0]
    depth = width // shards
    down = rights[2].shape[1] // width
    blocks = layers * (8 + down)

    barrier = pltpu.get_barrier_semaphore()
    peers = [core_peer, x_peer, y_peer] + z_peers[1:]
    for peer in peers:
        pl.semaphore_signal(barrier, inc=1, device_id=peer, device_id_type=MESH)
    pl.semaphore_wait(barrier, len(peers))

    def remote(source, target, send_at, receive, peer):
        return pltpu.make_async_remote_copy(
            src_ref=source, dst_ref=target, send_sem=sent.at[send_at], recv_sem=receive,
            device_id=peer, device_id_type=MESH,
        )

    loads, at_left, at_right, first_block = [], 0, 0, []
    for layer in range(layers):
        for kind in range(4):
            member = 4 * layer + kind
            rows = lefts[member].shape[0]
            pairs = [(lefts[member], left.at[pl.ds(at_left, rows)])]
            for column in range(0, rights[member].shape[1], width):
                pairs.append((rights[member].at[:, pl.ds(column, width)], right.at[at_right]))
                at_right += 1
            at_left += rows
            loads.append([
                pltpu.make_async_copy(source, target, load_sem.at[member, at])
                for at, (source, target) in enumerate(pairs)
            ])
            first_block.append(layer * (8 + down) + (0, 3, 4, 4 + down)[kind])
    for load in loads:
        for copy in load:
            copy.start()

    def gradient(block, wanted):
        layer, b = lax.div(block, 8 + down), lax.rem(block, 8 + down)
        deep = b - 4 - down
        start = layer * (at_left // layers) + jnp.where(
            b < 3, 0, jnp.where(b < 4, width, jnp.where(deep < 0, 2 * width, 3 * width))
        )
        start = start + jnp.where(deep < 0, depth * wanted, down * depth * wanted + depth * deep)
        column = layer * (at_right // layers) + jnp.minimum(b, 4 + down)
        return jnp.dot(
            left[pl.ds(pl.multiple_of(start, 64), depth), :], right[column],
            preferred_element_type=jnp.float32,
        )

    def block_rows(block):
        return pl.ds(pl.multiple_of(block * depth, 64), depth)

    def chunk_rows_of(k):
        return pl.ds(pl.multiple_of(k * chunk, chunk), chunk)

    def wanted_of(j, side):
        return (x_at if j == 0 else 1 - x_at) * 2 + side

    def core_send(block, j):
        slot = lax.rem(block, RING)
        return pltpu.make_async_remote_copy(
            src_ref=ring.at[slot, j], dst_ref=total.at[j, block_rows(block)],
            send_sem=ring_sem.at[slot, j], recv_sem=core_sem.at[block, j],
            device_id=core_peer, device_id_type=MESH,
        )

    small_depth = smalls[0].shape[0]

    def small_rows_of(layer):
        return pl.ds(blocks * depth + layer * small_depth, small_depth)

    def small_send(layer, j):
        return pltpu.make_async_remote_copy(
            src_ref=smalls[layer], dst_ref=total.at[j, small_rows_of(layer)],
            send_sem=small_sem.at[0, layer, j], recv_sem=small_sem.at[1, layer, j],
            device_id=core_peer, device_id_type=MESH,
        )

    for layer in range(layers):
        for j in (1, 0):
            small_send(layer, j).start()

    def stage_make(block):
        for member, first in enumerate(first_block):

            @pl.when(block == first)
            def _(member=member):
                for copy in loads[member]:
                    copy.wait()

        for j in (1, 0):

            @pl.when(block >= RING)
            def _(j=j):
                core_send(block, j).wait_send()

            ring[lax.rem(block, RING), j] = gradient(block, wanted_of(j, 1 - core)).astype(
                jnp.bfloat16
            )
            core_send(block, j).start()

    def stage_own(block):
        for j in (1, 0):
            own = gradient(block, wanted_of(j, core))
            core_send(block, j).wait_recv()
            place = total.at[j, block_rows(block)]
            place[...] = (place[...].astype(jnp.float32) + own).astype(jnp.bfloat16)

    def add_smalls():
        for layer in range(layers):
            for j in (1, 0):
                small_send(layer, j).wait_recv()
                add_rows(total.at[j, small_rows_of(layer)], smalls[layer])

    def x_send(k):
        return remote(total.at[1, chunk_rows_of(k)], x_in.at[k], 1, x_sem.at[k], x_peer)

    def y_rows(side):
        return pl.ds(pl.multiple_of(side * half, half), half)

    def y_part(k, side):
        return total.at[0, pl.ds(pl.multiple_of(k * chunk + side * half, half), half)]

    def y_send(k):
        return remote(y_part(k, 1 - y_at), y_in.at[k], 2, y_sem.at[k], y_peer)

    def z_rows(at):
        return pl.ds(pl.multiple_of(y_at * half + at * piece, piece), piece)

    def z_part(k, at):
        start = k * chunk + y_at * half + at * piece
        return total.at[0, pl.ds(pl.multiple_of(start, piece), piece)]

    def z_send(k, step):
        return remote(
            z_part(k, z_of[step]), z_in.at[k, step - 1], 3, z_sem.at[k, step - 1], z_peers[step]
        )

    def zg_send(k, step):
        mine = full.at[k, z_rows(z_at)]
        return remote(mine, mine, 4, zg_sem.at[k, step - 1], z_peers[step])

    def zg_arrival(k, step):
        theirs = full.at[k, z_rows(z_from[step])]
        return remote(theirs, theirs, 4, zg_sem.at[k, step - 1], z_peers[step])

    def yg_send(k):
        mine = full.at[k, y_rows(y_at)]
        return remote(mine, mine, 5, yg_sem.at[k], y_peer)

    def store_end(k):
        return pltpu.make_async_copy(full.at[k], full.at[k], out_sem.at[k])

    def stage_core(k):
        x_send(k).start()

    def stage_x(k):
        x_send(k).wait_recv()
        add_rows(total.at[0, chunk_rows_of(k)], x_in.at[k])
        y_send(k).start()

    def stage_y(k):
        y_send(k).wait_recv()
        add_rows(y_part(k, y_at), y_in.at[k])
        for step in range(1, high):
            z_send(k, step).start()

    def stage_z(k):
        summed = z_part(k, z_at)[...].astype(jnp.float32)
        for step in range(1, high):
            z_send(k, step).wait_recv()
            summed = summed + z_in[k, step - 1].astype(jnp.float32)
        full[k, z_rows(z_at), :] = summed.astype(jnp.bfloat16)
        for step in range(1, high):
            zg_send(k, step).start()

    def stage_spread(k):
        for step in range(1, high):
            zg_arrival(k, step).wait_recv()
        yg_send(k).start()

    def stage_store(k):
        yg_send(k).wait_recv()
        for segment in segments:

            @pl.when(k == segment.chunk)
            def _(segment=segment):
                target = targets[segment.member].at[
                    pl.ds(segment.row, segment.rows), pl.ds(segment.column, width)
                ]
                pltpu.make_async_copy(
                    full.at[segment.chunk, pl.ds(segment.at, segment.rows)], target,
                    out_sem.at[segment.chunk],
                ).start()

    def done(block):
        return jnp.where(
            block >= blocks, count, lax.div(jnp.maximum(block, 0) * depth, chunk)
        )

    stages = (stage_core, stage_x, stage_y, stage_z, stage_spread, stage_store)

    @pl.loop(0, blocks + LAG_OWN + 5 * LAG)
    def _(t):
        pl.when(t < blocks)(lambda: stage_make(t))
        own_at = t - LAG_OWN
        pl.when((own_at >= 0) & (own_at < blocks))(lambda: stage_own(own_at))
        pl.when(own_at == blocks - 1)(add_smalls)
        for at, stage in enumerate(stages):
            last = own_at - at * LAG + 1

            @pl.loop(done(last - 1), done(last))
            def _(k, stage=stage):
                stage(k)

    for block in range(max(0, blocks - RING), blocks):
        for j in (1, 0):
            core_send(block, j).wait_send()
    for layer in range(layers):
        for j in (1, 0):
            small_send(layer, j).wait_send()

    def all_sent(source, target, send_at, peer):
        remote(source, target, send_at, x_sem.at[0], peer).wait_send()

    all_sent(x_in, x_in, 1, x_peer)
    all_sent(y_in, y_in, 2, y_peer)
    all_sent(z_in, z_in, 3, z_peers[1])
    all_sent(z_in, z_in, 4, z_peers[1])
    all_sent(y_in, y_in, 5, y_peer)

    @pl.loop(0, count)
    def _(k):
        store_end(k).wait()


class Segment(NamedTuple):
    member: int
    row: int
    column: int
    rows: int
    chunk: int
    at: int


def plan_segments(forms, width, chunk):
    segments, place = [], 0
    for member, (depth, columns) in enumerate(forms):
        for column in range(0, columns, width):
            row = 0
            while row < depth:
                rows = min(depth - row, chunk - place % chunk)
                segments.append(
                    Segment(member, row, column, rows, place // chunk, place % chunk)
                )
                row, place = row + rows, place + rows
    return tuple(segments), place


def reduce_gradients(lefts, rights, smalls, shards, group, width):
    high = group // 2
    chunk = chunk_rows(group)
    layers = len(smalls)
    forms = [
        (left.shape[0] // shards, right.shape[1]) for left, right in zip(lefts, rights)
    ] + [small.shape for small in smalls]
    segments, used = plan_segments(forms, width, chunk)
    count = -(-used // chunk)
    piece = chunk // group
    depth = width // shards
    blocks = sum(rows * columns for rows, columns in forms[: 4 * layers]) // (depth * width)
    tokens = rights[0].shape[0]
    buffers = [
        (sum(left.shape[0] for left in lefts), tokens),
        (sum(right.shape[1] for right in rights) // width, tokens, width),
        (RING, 2, depth, width),
        (2, count * chunk, width),
        (count, chunk, width),
        (count, chunk // 2, width),
        (count, high - 1, piece, width),
        (count, chunk, width),
    ]
    semaphores = [(4 * layers, 1 + rights[2].shape[1] // width), (RING, 2), (blocks, 2),
                  (2, layers, 2), (count,), (count,), (count, high - 1), (count, high - 1),
                  (count,), (6,), (count,)]
    vmem, hbm, _ = memory_specs()
    return pl.pallas_call(
        functools.partial(reduce_kernel, high, chunk, segments, shards, layers),
        out_shape=[jax.ShapeDtypeStruct(form, jnp.bfloat16) for form in forms],
        in_specs=[hbm] * (8 * layers) + [vmem] * layers,
        out_specs=[hbm] * len(forms),
        scratch_shapes=[pltpu.VMEM(shape, jnp.bfloat16) for shape in buffers]
        + [pltpu.SemaphoreType.DMA(shape) for shape in semaphores],
        compiler_params=pltpu.CompilerParams(
            collective_id=1, has_side_effects=True, vmem_limit_bytes=64 * 1024 * 1024 - 65536
        ),
    )(*lefts, *rights, *smalls)


def chunk_rows(group):
    return 16 * CHUNK_TILES * group


def sum_gradients(lefts, rights, smalls, shards, group):
    width = smalls[0].shape[1]
    layers = len(smalls)
    reduced = reduce_gradients(lefts, rights, smalls, shards, group, width)
    spans = [
        jnp.stack([reduced[4 * layer + member] for layer in range(layers)]).astype(jnp.float32)
        for member in range(4)
    ]
    small = jnp.stack(reduced[4 * layers : 5 * layers]).astype(jnp.float32)
    depth = width // shards
    shard = lax.axis_index("fsdp")
    rows = lax.dynamic_slice_in_dim(small[:, :8], shard * depth, depth, axis=2)
    up_shift = lax.dynamic_slice_in_dim(small, 8 + shard, 1, axis=1)[:, 0]
    table = small[:, 16 : 16 + H, : 3 * NB].reshape(layers, H, 3, NB)
    table = lax.dynamic_slice_in_dim(table, shard * (NB // shards), NB // shards, axis=3)
    return tuple(spans) + (
        rows[:, :6], up_shift, rows[:, 6:], jnp.transpose(table, (0, 2, 3, 1)),
    )


def opening_kernel(items, *refs):
    total = len(items)
    ready = 1 + 4
    sources, forward_in = refs[:5], refs[5:9]
    outs = refs[9 : 9 + total - 1 + 3 + 14]
    vectors, up_shifts, table = outs[total - 1 : total + 2]
    forward_out = outs[total + 2 :]
    rest = refs[9 + len(outs) :]
    stages, rest = rest[:total], rest[total:]
    landing_small, load_sem, store_sem, send_sem, arrive = rest[:5]
    forward_scratch = rest[5:]
    targets = (landing_small,) + tuple(outs[: total - 1])
    dp = lax.axis_index("dp")
    shard = lax.axis_index("fsdp")
    x_at, core = lax.div(shard, 2), lax.rem(shard, 2)
    bits = (lax.rem(dp, 2), lax.rem(lax.div(dp, 2), 2))
    core_peer = (dp, x_at * 2 + 1 - core)
    other = (1 - x_at) * 2 + core
    x_peer = (dp, other)
    dp_peers = [
        (dp + 1 - 2 * bits[0], shard),
        (dp + 2 - 4 * bits[1], shard),
    ]
    barrier = pltpu.get_barrier_semaphore()
    for peer in [core_peer, x_peer] + dp_peers:
        pl.semaphore_signal(barrier, inc=1, device_id=peer, device_id_type=MESH)
    pl.semaphore_wait(barrier, 4)

    def copy(source, target, item, kind, peer):
        return pltpu.make_async_remote_copy(
            src_ref=source, dst_ref=target, send_sem=send_sem.at[item, kind],
            recv_sem=arrive.at[item, kind], device_id=peer, device_id_type=MESH,
        )

    def shard_of(i):
        member, layer = items[i]
        return sources[member] if layer is None else sources[member].at[layer]

    def depth_of(i):
        return stages[i].shape[0]

    def parts_of(i):
        return 1 if i == 0 else 4

    def small_lanes(at):
        size = stages[0].shape[1]
        return landing_small.at[:, pl.ds(pl.multiple_of(at * size, size), size)]

    def mine_out(i):
        if i == 0:
            return small_lanes(shard)
        n = depth_of(i)
        return targets[i].at[pl.ds(pl.multiple_of(shard * n, 16), n)]

    def other_out(i, quarter):
        n = depth_of(i)
        part = n // parts_of(i)
        return targets[i].at[pl.ds(pl.multiple_of(other * n + quarter * part, 16), part)]

    def other_whole(i):
        if i == 0:
            return small_lanes(other)
        n = depth_of(i)
        return targets[i].at[pl.ds(pl.multiple_of(other * n, 16), n)]

    def order_of(i):
        return (0, 1) if i % 2 == 0 else (1, 0)

    def quarter_of(i, flips):
        if parts_of(i) == 1:
            return 0
        now = [bits[axis] if axis not in flips else 1 - bits[axis] for axis in (0, 1)]
        return now[1] * 2 + now[0]

    def x_send(i):
        if i == 0:
            return copy(shard_of(i), small_lanes(shard), i, 0, x_peer)
        n = depth_of(i)
        part = n // parts_of(i)
        start = pl.multiple_of(quarter_of(i, ()) * part, 16)
        rows = pl.ds(start, part)
        landing = targets[i].at[pl.ds(pl.multiple_of(shard * n + start, 16), part)]
        return copy(shard_of(i).at[rows], landing, i, 0, x_peer)

    def first_send(i):
        mine = other_out(i, quarter_of(i, ()))
        return copy(mine, mine, i, 1, dp_peers[order_of(i)[0]])

    def second_send(i):
        mine = other_out(i, quarter_of(i, ()))
        return copy(mine, mine, i, 2, dp_peers[order_of(i)[1]])

    def relay_send(i):
        mine = other_out(i, quarter_of(i, (order_of(i)[0],)))
        return copy(mine, mine, i, 3, dp_peers[order_of(i)[1]])

    def own_share(i):
        return copy(shard_of(i), mine_out(i), i, 4, core_peer)

    def far_share(i):
        return copy(other_whole(i), other_whole(i), i, 5, core_peer)

    def load(i):
        return pltpu.make_async_copy(shard_of(i), stages[i], load_sem.at[i])

    def store(i):
        return pltpu.make_async_copy(stages[i], mine_out(i), store_sem.at[i])

    for i in range(total):
        x_send(i).start()
    for i in range(total):
        own_share(i).start()
        load(i).start()

    def spread(i):
        x_send(i).wait_recv()
        if parts_of(i) == 4:
            first_send(i).start()
            second_send(i).start()
        load(i).wait()
        store(i).start()

    def relay(i):
        if parts_of(i) == 4:
            first_send(i).wait_recv()
            relay_send(i).start()

    def share(i):
        if parts_of(i) == 4:
            second_send(i).wait_recv()
            relay_send(i).wait_recv()
        far_share(i).start()

    def arrived(i):
        own_share(i).wait_recv()
        far_share(i).wait_recv()
        store(i).wait()

    for step in range(ready + 3):
        if step < ready:
            spread(step)
        elif step < total:
            spread(step)
        if 0 <= step - 1 < ready:
            relay(step - 1)
        if 0 <= step - 3 < ready:
            share(step - 3)
    for i in range(ready):
        arrived(i)
    place_small(landing_small, vectors, up_shifts, table)

    waiting = [functools.partial(spread, i) for i in range(ready + 3, total)]
    waiting += [functools.partial(relay, i) for i in range(ready, total)]
    waiting += [functools.partial(share, i) for i in range(ready, total)]
    points = 4
    per_point = -(-len(waiting) // points)

    def service(point):
        for act in waiting[point * per_point : (point + 1) * per_point]:
            act()

    forward_core(
        0, service, *forward_in, vectors, up_shifts, table, *targets[1:5], *forward_out,
        *forward_scratch,
    )
    for i in range(ready, total):
        arrived(i)
    for i in range(total):
        own_share(i).wait_send()
        far_share(i).wait_send()
        x_send(i).wait_send()
        if parts_of(i) == 4:
            first_send(i).wait_send()
            second_send(i).wait_send()
            relay_send(i).wait_send()


def place_small(landing, vectors, up_shifts, table):
    lanes = landing.shape[1]
    each = 2 * WIN
    shards = lanes // each

    def selected(rows, own, width):
        source = lax.broadcasted_iota(jnp.int32, (lanes, width), 0)
        target = lax.broadcasted_iota(jnp.int32, (lanes, width), 1)
        within = source % each
        picked = (within < own) & (target == source // each * own + within)
        return jnp.dot(
            landing[rows, :], picked.astype(jnp.float32).astype(jnp.bfloat16),
            preferred_element_type=jnp.float32,
        )

    layers = up_shifts.shape[0]
    width = vectors.shape[1]
    vectors[...] = selected(pl.ds(0, 16), width // shards, width)
    shift_rows = landing[16:32, :].astype(jnp.float32)
    runs = width // each
    for layer in range(layers):
        for shard in range(shards):
            for run in range(runs):
                start = shard * width + run * each
                up_shifts[layer : layer + 1, start : start + each] = shift_rows[
                    layer * runs + run : layer * runs + run + 1,
                    shard * each : (shard + 1) * each,
                ]
    table[...] = selected(pl.ds(32, table.shape[0]), NB // shards, WIN)


def small_rows(biases, ffn_in_bias, gains, tables):
    layers = biases.shape[0]
    each = 2 * WIN
    vectors = jnp.concatenate([biases, gains], axis=1).reshape(layers * 8, -1)
    vectors = jnp.pad(vectors, ((0, 16 - 8 * layers), (0, each - vectors.shape[1])))
    shifts = ffn_in_bias.reshape(-1, each)
    shifts = jnp.pad(shifts, ((0, 16 - shifts.shape[0]), (0, 0)))
    entries = jnp.swapaxes(tables, 2, 3)
    entries = jnp.pad(
        entries, ((0, 0), (0, 0), (0, 16 - H), (0, each - entries.shape[3]))
    ).reshape(layers * 48, each)
    return jnp.concatenate([vectors, shifts, entries], axis=0)


def open_layers(sources, small, shards, inputs, buckets, live, lengths):
    layers = sources[0].shape[0]
    rows, width = inputs.shape
    items = [(4, None)] + [(member, layer) for layer in range(layers) for member in range(4)]
    forms = [small.shape] + [sources[member].shape[1:] for member, _ in items[1:]]
    total = len(items)
    hidden = sources[2].shape[2]
    outs, scratch = forward_forms(rows, width, hidden)
    vmem, hbm, smem = memory_specs()
    shared = [
        jax.ShapeDtypeStruct((16, width), jnp.float32),
        jax.ShapeDtypeStruct((layers, hidden), jnp.float32),
        jax.ShapeDtypeStruct((layers * 48, WIN), jnp.float32),
    ]
    results = pl.pallas_call(
        functools.partial(opening_kernel, tuple(items)),
        out_shape=[
            jax.ShapeDtypeStruct((form[0] * shards, form[1]), jnp.bfloat16) for form in forms[1:]
        ]
        + shared
        + outs,
        in_specs=[hbm] * 5 + [vmem, vmem, vmem, smem],
        out_specs=[hbm] * (total - 1) + [vmem] * (3 + len(outs)),
        scratch_shapes=[pltpu.VMEM(form, jnp.bfloat16) for form in forms]
        + [
            pltpu.VMEM((small.shape[0], small.shape[1] * shards), jnp.bfloat16),
            pltpu.SemaphoreType.DMA((total,)),
            pltpu.SemaphoreType.DMA((total,)),
            pltpu.SemaphoreType.DMA((total, 6)),
            pltpu.SemaphoreType.DMA((total, 6)),
        ]
        + scratch,
        compiler_params=pltpu.CompilerParams(
            collective_id=0, has_side_effects=True, vmem_limit_bytes=58 * 1024 * 1024
        ),
    )(*sources, small, inputs, buckets, live, lengths)
    weights = [results[4 * layer : 4 * layer + 4] for layer in range(layers)]
    return weights, results[total - 1 : total + 2], results[total + 2 :]


def contract(left, right, left_axis, right_axis):
    return lax.dot_general(
        left, right, (((left_axis,), (right_axis,)), ((), ())),
        preferred_element_type=jnp.float32,
    )


def positions_of(axis):
    return lax.broadcasted_iota(jnp.int32, (WIN, WIN), axis)


def linear_bucket(offset):
    return jnp.clip(offset, -(NB // 2), NB // 2 - 1) + NB // 2


def lane_halves():
    lane = lax.broadcasted_iota(jnp.int32, (1, 2 * DH), 1)
    first = (lane < DH).astype(jnp.float32)
    return first.astype(jnp.bfloat16), (1.0 - first).astype(jnp.bfloat16)


def forward_kernel(layer, *refs):
    forward_core(layer, lambda point: None, *refs)


def forward_core(
    layer, service, x_ref, buckets, live, lengths, all_vectors, up_shifts, table, w_in_hbm,
    w_out_hbm, w_up_hbm, w_down_hbm, out_ref, q_ref, k_ref, v_ref, o_turned, p_ref, low_turned, n1_ref, r1_ref,
    slope_ref, g_turned, n2_ref, r2_ref, x_turned, w_in, w_out, w_up, w_down, allowed, y1, total,
    o_ref, low_ref, sem,
):
    loads = [
        pltpu.make_async_copy(source, target, sem.at[at])
        for at, (source, target) in enumerate(
            ((w_in_hbm, w_in), (w_out_hbm, w_out), (w_up_hbm, w_up), (w_down_hbm, w_down))
        )
    ]
    for load in loads:
        load.start()
    vectors = all_vectors.at[pl.ds(8 * layer, 8)]
    up_shift = up_shifts.at[pl.ds(layer, 1)]
    rows, width = x_ref.shape
    windows = rows // WIN
    row, column = positions_of(0), positions_of(1)
    offset = linear_bucket(column - row)
    first, second = lane_halves()
    for w in range(windows):
        row_doc, column_doc = jnp.zeros_like(row), jnp.zeros_like(column)
        end = 0
        for k in range(lengths.shape[1]):
            end = end + lengths[w, k]
            row_doc = row_doc + (row >= end).astype(jnp.int32)
            column_doc = column_doc + (column >= end).astype(jnp.int32)
        alive = jnp.broadcast_to(live[w : w + 1, :], (WIN, WIN))
        seen = (row_doc == column_doc) & ((alive == 1) | (row == column))
        allowed[w] = seen.astype(jnp.int32)

    loads[0].wait()
    inputs = x_ref[...]
    q_ref[...] = (
        (jnp.dot(inputs, w_in[:, :width], preferred_element_type=jnp.float32) + vectors[0:1, :])
        * DH ** (-0.5)
    ).astype(jnp.bfloat16)
    k_ref[...] = jnp.dot(
        inputs, w_in[:, width : 2 * width], preferred_element_type=jnp.float32
    ).astype(jnp.bfloat16)
    v_ref[...] = (
        jnp.dot(inputs, w_in[:, 2 * width :], preferred_element_type=jnp.float32)
        + vectors[1:2, :]
    ).astype(jnp.bfloat16)
    service(0)

    def attend(w, pair):
        span = pl.ds(w * WIN, WIN)
        lanes = pl.ds(pl.multiple_of(pair * 2 * DH, 2 * DH), 2 * DH)
        queries, keys, values = q_ref[span, lanes], k_ref[span, lanes], v_ref[span, lanes]
        mixed = []
        for side, half in enumerate((first, second)):
            head = pair * 2 + side
            scores = contract(queries * half, keys, 1, 1)
            bias = 0.0
            for kind, index in enumerate((offset, buckets[0, span, :], buckets[1, span, :])):
                entry = table[pl.ds(48 * layer + 16 * kind + head, 1), :]
                entries = jnp.broadcast_to(entry, (WIN, WIN))
                bias = bias + jnp.take_along_axis(
                    entries, index, axis=1, mode="promise_in_bounds"
                )
            scores = jnp.where(allowed[w] == 1, scores + bias, -1e30)
            exponent = jnp.exp(scores - jnp.max(scores, axis=-1, keepdims=True))
            probs = exponent / jnp.sum(exponent, axis=-1, keepdims=True)
            p_ref[w * H + head] = probs
            mixed.append(
                jnp.dot(
                    probs.astype(jnp.bfloat16), values * half, preferred_element_type=jnp.float32
                )
            )
        o_ref[span, lanes] = (mixed[0] + mixed[1]).astype(jnp.bfloat16)

    for w in range(windows):

        @pl.loop(0, H // 4)
        def _(quad, w=w):
            attend(w, quad * 2)
            attend(w, quad * 2 + 1)

        service(1 + w)

    x_turned[...] = jnp.transpose(inputs)
    o_turned[...] = jnp.transpose(o_ref[...])
    loads[1].wait()
    attended = (
        jnp.dot(o_ref[...], w_out[...], preferred_element_type=jnp.float32) + vectors[2:3, :]
    )
    first_norm, normed, inverse = norm_forward(
        inputs.astype(jnp.float32) + attended, vectors[6:7, :], vectors[3:4, :]
    )
    n1_ref[...] = normed
    r1_ref[...] = jnp.broadcast_to(inverse, r1_ref.shape)
    y1[...] = first_norm
    low = first_norm.astype(jnp.bfloat16)
    low_ref[...] = low
    low_turned[...] = jnp.transpose(low)
    total[...] = jnp.zeros_like(total)
    service(1 + windows)
    loads[2].wait()
    loads[3].wait()

    @pl.loop(0, w_up.shape[1] // width)
    def _(at):
        lanes = pl.ds(pl.multiple_of(at * width, width), width)
        hidden = (
            jnp.dot(low_ref[...], w_up[:, lanes], preferred_element_type=jnp.float32)
            + up_shift[:, lanes]
        )
        mass = 0.5 + 0.5 * lax.erf(hidden * 0.5**0.5)
        slope_ref[:, lanes] = mass + hidden * jnp.exp(-0.5 * hidden * hidden) * (
            0.5 / math.pi
        ) ** 0.5
        active = (hidden * mass).astype(jnp.bfloat16)
        g_turned[lanes, :] = jnp.transpose(active)
        total[...] += jnp.dot(active, w_down[lanes, :], preferred_element_type=jnp.float32)

    result, normed, inverse = norm_forward(
        y1[...] + (total[...] + vectors[4:5, :]), vectors[7:8, :], vectors[5:6, :]
    )
    n2_ref[...] = normed
    r2_ref[...] = jnp.broadcast_to(inverse, r2_ref.shape)
    out_ref[...] = result.astype(jnp.bfloat16)


def forward_forms(rows, width, hidden):
    low, full = jnp.bfloat16, jnp.float32
    narrow = jax.ShapeDtypeStruct((rows, width), low)
    wide = jax.ShapeDtypeStruct((rows, width), full)
    column = jax.ShapeDtypeStruct((rows, WIN), full)
    turned = jax.ShapeDtypeStruct((width, rows), low)
    outs = [
        narrow, narrow, narrow, narrow, turned,
        jax.ShapeDtypeStruct((rows // WIN * H, WIN, WIN), full),
        turned, wide, column,
        jax.ShapeDtypeStruct((rows, hidden), full),
        jax.ShapeDtypeStruct((hidden, rows), low),
        wide, column, turned,
    ]
    scratch = [
        pltpu.VMEM((width, 3 * width), low), pltpu.VMEM((width, width), low),
        pltpu.VMEM((width, hidden), low), pltpu.VMEM((hidden, width), low),
        pltpu.VMEM((rows // WIN, WIN, WIN), jnp.int32),
        pltpu.VMEM((rows, width), full), pltpu.VMEM((rows, width), full),
        pltpu.VMEM((rows, width), low), pltpu.VMEM((rows, width), low),
        pltpu.SemaphoreType.DMA((4,)),
    ]
    return outs, scratch


def memory_specs():
    return [
        pl.BlockSpec(memory_space=space)
        for space in (
            pltpu.MemorySpace.VMEM, pltpu.MemorySpace.HBM, pltpu.MemorySpace.SMEM
        )
    ]


def forward_layer(layer, inputs, weights, shared, buckets, live, lengths):
    rows, width = inputs.shape
    outs, scratch = forward_forms(rows, width, weights[2].shape[1])
    vmem, hbm, smem = memory_specs()
    return pl.pallas_call(
        functools.partial(forward_kernel, layer),
        out_shape=outs,
        in_specs=[vmem, vmem, vmem, smem, vmem, vmem, vmem, hbm, hbm, hbm, hbm],
        out_specs=[vmem] * len(outs),
        scratch_shapes=scratch,
        compiler_params=pltpu.CompilerParams(vmem_limit_bytes=56 * 1024 * 1024),
    )(inputs, buckets, live, lengths, *shared, *weights)


def backward_kernel(
    layer, dz_ref, n2_ref, r2_ref, slope_ref, n1_ref, r1_ref, p_ref, q_ref, k_ref, v_ref, buckets,
    all_vectors, w_down_hbm, w_up_hbm, w_out_hbm, w_in_hbm, dx_ref, df_ref, du_ref, da_ref, dqkv_ref,
    small_ref, w_down, w_up, w_out, w_in, small, grad, mixed, spread, sem,
):
    loads = [
        pltpu.make_async_copy(source, target, sem.at[at])
        for at, (source, target) in enumerate(
            ((w_down_hbm, w_down), (w_up_hbm, w_up), (w_out_hbm, w_out), (w_in_hbm, w_in))
        )
    ]
    for load in loads:
        load.start()
    vectors = all_vectors.at[pl.ds(8 * layer, 8)]
    rows, width = dz_ref.shape
    windows = rows // WIN
    first, second = lane_halves()
    small[...] = jnp.zeros_like(small)
    spread[...] = jnp.zeros_like(spread)

    def add_row(at, values):
        small[pl.ds(at, 1), :] = jnp.sum(values, axis=0, keepdims=True)

    def norm_back(incoming, normed, inverse, gain_row):
        scaled = incoming * gain_row
        centred = (
            scaled
            - jnp.mean(scaled, axis=-1, keepdims=True)
            - normed * jnp.mean(scaled * normed, axis=-1, keepdims=True)
        )
        return centred * inverse

    incoming, normed = dz_ref[...], n2_ref[...]
    add_row(7, incoming * normed)
    add_row(5, incoming)
    grad_second = norm_back(incoming, normed, r2_ref[:, 0:1], vectors[7:8, :])
    grad[...] = grad_second
    branch_low = grad_second.astype(jnp.bfloat16)
    df_ref[...] = branch_low
    add_row(4, branch_low.astype(jnp.float32))
    loads[0].wait()
    loads[1].wait()

    @pl.loop(0, w_up.shape[1] // width)
    def _(at):
        lanes = pl.ds(pl.multiple_of(at * width, width), width)
        grad_active = contract(df_ref[...], w_down[lanes, :], 1, 1)
        hidden_low = (grad_active * slope_ref[:, lanes]).astype(jnp.bfloat16)
        du_ref[:, lanes] = hidden_low
        add_row(8 + at, hidden_low.astype(jnp.float32))
        grad[...] += contract(hidden_low, w_up[:, lanes], 1, 1)

    incoming, normed = grad[...], n1_ref[...]
    add_row(6, incoming * normed)
    add_row(3, incoming)
    grad_attended = norm_back(incoming, normed, r1_ref[:, 0:1], vectors[6:7, :])
    grad[...] = grad_attended
    attended_low = grad_attended.astype(jnp.bfloat16)
    da_ref[...] = attended_low
    add_row(2, attended_low.astype(jnp.float32))
    loads[2].wait()
    mixed[...] = contract(attended_low, w_out[...], 1, 1).astype(jnp.bfloat16)

    def attend(w, pair):
        span = pl.ds(w * WIN, WIN)
        start = pl.multiple_of(pair * 2 * DH, 2 * DH)
        lanes = pl.ds(start, 2 * DH)
        queries, keys, values = q_ref[span, lanes], k_ref[span, lanes], v_ref[span, lanes]
        outgoing = mixed[span, lanes]
        sums = [0.0, 0.0, 0.0]
        for side, half in enumerate((first, second)):
            head = pair * 2 + side
            probs = p_ref[w * H + head]
            own = outgoing * half
            grad_probs = contract(own, values, 1, 1)
            centred = grad_probs - jnp.sum(probs * grad_probs, axis=-1, keepdims=True)
            grad_scores = (probs * centred).astype(jnp.bfloat16)
            spread[pl.ds(head, WIN, stride=16), :] = grad_scores.astype(jnp.float32)
            sums[0] += jnp.dot(grad_scores, keys * half, preferred_element_type=jnp.float32)
            sums[1] += contract(grad_scores, queries * half, 0, 0)
            sums[2] += contract(probs.astype(jnp.bfloat16), own, 0, 0)
        scaled = sums[0].astype(jnp.bfloat16).astype(jnp.float32) * DH ** (-0.5)
        dqkv_ref[span, lanes] = scaled.astype(jnp.bfloat16)
        dqkv_ref[span, pl.ds(pl.multiple_of(start + width, 2 * DH), 2 * DH)] = sums[1].astype(
            jnp.bfloat16
        )
        dqkv_ref[span, pl.ds(pl.multiple_of(start + 2 * width, 2 * DH), 2 * DH)] = sums[2].astype(
            jnp.bfloat16
        )

    bucket = lax.broadcasted_iota(jnp.int32, (NB, WIN), 0)
    column = lax.broadcasted_iota(jnp.int32, (1, WIN), 1)
    group = 8
    for w in range(windows):

        @pl.loop(0, H // 4)
        def _(quad, w=w):
            attend(w, quad * 2)
            attend(w, quad * 2 + 1)

        def count_group(at, w=w):
            hits, terms = [], []
            for step in range(group):
                i = at * group + step
                indices = (
                    linear_bucket(column - i),
                    buckets[0, pl.ds(w * WIN + i, 1), :],
                    buckets[1, pl.ds(w * WIN + i, 1), :],
                )
                hits.append(
                    jnp.concatenate(
                        [(index == bucket).astype(jnp.float32) for index in indices], axis=0
                    ).astype(jnp.bfloat16)
                )
                terms.append(
                    spread[pl.ds(pl.multiple_of(i * 16, 16), 16), :].astype(jnp.bfloat16)
                )
            return contract(jnp.concatenate(terms, axis=1), jnp.concatenate(hits, axis=1), 1, 1)

        @pl.loop(0, WIN // group)
        def _(at):
            small[16:32, 0 : 3 * NB] += count_group(at)

    loads[3].wait()
    add_row(0, dqkv_ref[:, :width].astype(jnp.float32))
    add_row(1, dqkv_ref[:, 2 * width :].astype(jnp.float32))
    dx_ref[...] = grad[...] + contract(dqkv_ref[...], w_in[...], 1, 1)
    small_ref[...] = small[...].astype(jnp.bfloat16)


def backward_layer(layer, incoming, weights, vectors, kept, buckets):
    w_in, w_out, w_up, w_down = weights
    rows, width = incoming.shape
    hidden = w_up.shape[1]
    low, full = jnp.bfloat16, jnp.float32
    narrow = jax.ShapeDtypeStruct((rows, width), low)
    vmem, hbm, _ = memory_specs()
    q, k, v, _, p, _, n1, r1, slope, _, n2, r2, _ = kept
    return pl.pallas_call(
        functools.partial(backward_kernel, layer),
        out_shape=[
            jax.ShapeDtypeStruct((rows, width), full),
            narrow,
            jax.ShapeDtypeStruct((rows, hidden), low),
            narrow,
            jax.ShapeDtypeStruct((rows, 3 * width), low),
            jax.ShapeDtypeStruct((64, width), low),
        ],
        in_specs=[vmem] * 12 + [hbm] * 4,
        out_specs=[vmem] * 6,
        scratch_shapes=[
            pltpu.VMEM(w_down.shape, low), pltpu.VMEM(w_up.shape, low),
            pltpu.VMEM(w_out.shape, low), pltpu.VMEM(w_in.shape, low),
            pltpu.VMEM((64, width), full), pltpu.VMEM((rows, width), full),
            pltpu.VMEM((rows, width), low), pltpu.VMEM((WIN * 16, WIN), full),
            pltpu.SemaphoreType.DMA((4,)),
        ],
        compiler_params=pltpu.CompilerParams(vmem_limit_bytes=56 * 1024 * 1024),
    )(incoming, n2, r2, slope, n1, r1, p, q, k, v, buckets, vectors, w_down, w_up, w_out, w_in)


def local(
    tokens,
    out_grad,
    mlm_mask,
    live_mask,
    doc_lengths,
    layout_buckets,
    attn_in,
    attn_out,
    ffn_in,
    ffn_out,
    biases,
    ffn_in_bias,
    gains,
    tables,
):
    shards = lax.axis_size("fsdp")
    live = live_mask.reshape(-1, WIN)
    weights_list, shared, first = open_layers(
        (attn_in, attn_out, ffn_in, ffn_out), small_rows(biases, ffn_in_bias, gains, tables),
        shards, tokens, layout_buckets, live, doc_lengths,
    )
    current, *kept = first
    kept_list, outputs = [kept], [current]
    for layer in range(1, len(weights_list)):
        current, *kept = forward_layer(
            layer, current, weights_list[layer], shared, layout_buckets, live, doc_lengths
        )
        kept_list.append(kept)
        outputs.append(current)
    incoming = out_grad.astype(jnp.float32) * mlm_mask.astype(jnp.float32)[:, None]
    lefts, rights, smalls = [], [], []
    for layer in reversed(range(len(weights_list))):
        kept = kept_list[layer]
        incoming, df, du, da, dqkv, small = backward_layer(
            layer, incoming, weights_list[layer], shared[0], kept, layout_buckets
        )
        lefts = [kept[12], kept[3], kept[5], kept[9]] + lefts
        rights = [dqkv, da, du, df] + rights
        smalls = [small] + smalls
    summed = sum_gradients(lefts, rights, smalls, shards, lax.axis_size("dp"))
    return (jnp.stack(outputs), incoming) + summed


def solution(mesh):
    return jax.shard_map(
        local,
        mesh=mesh,
        in_specs=(
            P(("dp", "fsdp"), None),
            P(("dp", "fsdp"), None),
            P(("dp", "fsdp")),
            P(("dp", "fsdp")),
            P(("dp", "fsdp"), None),
            P(None, ("dp", "fsdp"), None),
            P(None, "fsdp", None),
            P(None, "fsdp", None),
            P(None, "fsdp", None),
            P(None, "fsdp", None),
            P(None, None, "fsdp"),
            P(None, "fsdp"),
            P(None, None, "fsdp"),
            P(None, None, "fsdp", None),
        ),
        out_specs=(
            P(None, ("dp", "fsdp"), None),
            P(("dp", "fsdp"), None),
            P(None, "fsdp", None),
            P(None, "fsdp", None),
            P(None, "fsdp", None),
            P(None, "fsdp", None),
            P(None, None, "fsdp"),
            P(None, "fsdp"),
            P(None, None, "fsdp"),
            P(None, None, "fsdp", None),
        ),
        check_vma=False,
    )
```

```python
import functools
import math
from typing import NamedTuple

import jax
import jax.numpy as jnp
from jax import lax
from jax.experimental import pallas as pl
from jax.experimental.pallas import tpu as pltpu
from jax.sharding import PartitionSpec as P

H = 12
DH = 64
NB = 32
WIN = 128


EPSILON = 1e-05
LAG = 1
LAG_OWN = 2


def norm_forward(values, gain_row, shift_row):
    centre = values - jnp.mean(values, axis=-1, keepdims=True)
    spread = jnp.mean(centre * centre, axis=-1, keepdims=True)
    inverse = lax.rsqrt(spread + EPSILON)
    normed = centre * inverse
    return (normed * gain_row + shift_row, normed, inverse)


MESH = pl.DeviceIdType.MESH
CHUNK_TILES = 1


def add_rows(target, other):
    target[...] = (target[...].astype(jnp.float32) + other[...].astype(jnp.float32)).astype(
        jnp.bfloat16
    )


RING = 4


def reduce_kernel(high, chunk, segments, shards, layers, *refs):
    each = 4 * layers
    lefts, rights, smalls = refs[:each], refs[each : 2 * each], refs[2 * each : 2 * each + layers]
    refs = refs[2 * each + layers :]
    members = len(refs) - 19
    targets = [
        refs[kind].at[layer] for layer in range(layers) for kind in range(4)
    ] + [refs[4].at[layer] for layer in range(layers)]
    (left, right, ring, total, x_in, y_in, z_in, full, load_sem, ring_sem, core_sem, small_sem,
     x_sem, y_sem, z_sem, zg_sem, yg_sem, sent) = refs[members:][:18]
    out_sem = refs[-1]
    dp = lax.axis_index("dp")
    shard = lax.axis_index("fsdp")
    y_at, z_at = lax.rem(dp, 2), lax.div(dp, 2)
    x_at, core = lax.div(shard, 2), lax.rem(shard, 2)
    core_peer = (dp, x_at * 2 + 1 - core)
    x_peer = (dp, (1 - x_at) * 2 + core)
    y_peer = (z_at * 2 + 1 - y_at, shard)
    z_of = [lax.rem(z_at + step, high) for step in range(high)]
    z_from = [lax.rem(z_at + high - step, high) for step in range(high)]
    z_peers = [(z_of[step] * 2 + y_at, shard) for step in range(high)]
    half = chunk // 2
    piece = half // high
    width = full.shape[2]
    count = full.shape[0]
    depth = width // shards
    down = rights[2].shape[1] // width
    blocks = layers * (8 + down)

    barrier = pltpu.get_barrier_semaphore()
    peers = [core_peer, x_peer, y_peer] + z_peers[1:]
    for peer in peers:
        pl.semaphore_signal(barrier, inc=1, device_id=peer, device_id_type=MESH)
    pl.semaphore_wait(barrier, len(peers))

    def remote(source, target, send_at, receive, peer):
        return pltpu.make_async_remote_copy(
            src_ref=source, dst_ref=target, send_sem=sent.at[send_at], recv_sem=receive,
            device_id=peer, device_id_type=MESH,
        )

    loads, at_left, at_right, first_block = [], 0, 0, []
    for layer in range(layers):
        for kind in range(4):
            member = 4 * layer + kind
            rows = lefts[member].shape[0]
            pairs = [(lefts[member], left.at[pl.ds(at_left, rows)])]
            for column in range(0, rights[member].shape[1], width):
                pairs.append((rights[member].at[:, pl.ds(column, width)], right.at[at_right]))
                at_right += 1
            at_left += rows
            loads.append([
                pltpu.make_async_copy(source, target, load_sem.at[member, at])
                for at, (source, target) in enumerate(pairs)
            ])
            first_block.append(layer * (8 + down) + (0, 3, 4, 4 + down)[kind])
    for load in loads:
        for copy in load:
            copy.start()

    def gradient(block, wanted):
        layer, b = lax.div(block, 8 + down), lax.rem(block, 8 + down)
        deep = b - 4 - down
        start = layer * (at_left // layers) + jnp.where(
            b < 3, 0, jnp.where(b < 4, width, jnp.where(deep < 0, 2 * width, 3 * width))
        )
        start = start + jnp.where(deep < 0, depth * wanted, down * depth * wanted + depth * deep)
        column = layer * (at_right // layers) + jnp.minimum(b, 4 + down)
        return jnp.dot(
            left[pl.ds(pl.multiple_of(start, 64), depth), :], right[column],
            preferred_element_type=jnp.float32,
        )

    def block_rows(block):
        return pl.ds(pl.multiple_of(block * depth, 64), depth)

    def chunk_rows_of(k):
        return pl.ds(pl.multiple_of(k * chunk, chunk), chunk)

    def wanted_of(j, side):
        return (x_at if j == 0 else 1 - x_at) * 2 + side

    def core_send(block, j):
        slot = lax.rem(block, RING)
        return pltpu.make_async_remote_copy(
            src_ref=ring.at[slot, j], dst_ref=total.at[j, block_rows(block)],
            send_sem=ring_sem.at[slot, j], recv_sem=core_sem.at[block, j],
            device_id=core_peer, device_id_type=MESH,
        )

    small_depth = smalls[0].shape[0]

    def small_rows_of(layer):
        return pl.ds(blocks * depth + layer * small_depth, small_depth)

    def small_send(layer, j):
        return pltpu.make_async_remote_copy(
            src_ref=smalls[layer], dst_ref=total.at[j, small_rows_of(layer)],
            send_sem=small_sem.at[0, layer, j], recv_sem=small_sem.at[1, layer, j],
            device_id=core_peer, device_id_type=MESH,
        )

    for layer in range(layers):
        for j in (1, 0):
            small_send(layer, j).start()

    def stage_make(block):
        for member, first in enumerate(first_block):

            @pl.when(block == first)
            def _(member=member):
                for copy in loads[member]:
                    copy.wait()

        for j in (1, 0):

            @pl.when(block >= RING)
            def _(j=j):
                core_send(block, j).wait_send()

            ring[lax.rem(block, RING), j] = gradient(block, wanted_of(j, 1 - core)).astype(
                jnp.bfloat16
            )
            core_send(block, j).start()

    def stage_own(block):
        for j in (1, 0):
            own = gradient(block, wanted_of(j, core))
            core_send(block, j).wait_recv()
            place = total.at[j, block_rows(block)]
            place[...] = (place[...].astype(jnp.float32) + own).astype(jnp.bfloat16)

    def add_smalls():
        for layer in range(layers):
            for j in (1, 0):
                small_send(layer, j).wait_recv()
                add_rows(total.at[j, small_rows_of(layer)], smalls[layer])

    def x_send(k):
        return remote(total.at[1, chunk_rows_of(k)], x_in.at[k], 1, x_sem.at[k], x_peer)

    def y_rows(side):
        return pl.ds(pl.multiple_of(side * half, half), half)

    def y_part(k, side):
        return total.at[0, pl.ds(pl.multiple_of(k * chunk + side * half, half), half)]

    def y_send(k):
        return remote(y_part(k, 1 - y_at), y_in.at[k], 2, y_sem.at[k], y_peer)

    def z_rows(at):
        return pl.ds(pl.multiple_of(y_at * half + at * piece, piece), piece)

    def z_part(k, at):
        start = k * chunk + y_at * half + at * piece
        return total.at[0, pl.ds(pl.multiple_of(start, piece), piece)]

    def z_send(k, step):
        return remote(
            z_part(k, z_of[step]), z_in.at[k, step - 1], 3, z_sem.at[k, step - 1], z_peers[step]
        )

    def zg_send(k, step):
        mine = full.at[k, z_rows(z_at)]
        return remote(mine, mine, 4, zg_sem.at[k, step - 1], z_peers[step])

    def zg_arrival(k, step):
        theirs = full.at[k, z_rows(z_from[step])]
        return remote(theirs, theirs, 4, zg_sem.at[k, step - 1], z_peers[step])

    def yg_send(k):
        mine = full.at[k, y_rows(y_at)]
        return remote(mine, mine, 5, yg_sem.at[k], y_peer)

    def store_end(k):
        return pltpu.make_async_copy(full.at[k], full.at[k], out_sem.at[k])

    def stage_core(k):
        x_send(k).start()

    def stage_x(k):
        x_send(k).wait_recv()
        add_rows(total.at[0, chunk_rows_of(k)], x_in.at[k])
        y_send(k).start()

    def stage_y(k):
        y_send(k).wait_recv()
        add_rows(y_part(k, y_at), y_in.at[k])
        for step in range(1, high):
            z_send(k, step).start()

    def stage_z(k):
        summed = z_part(k, z_at)[...].astype(jnp.float32)
        for step in range(1, high):
            z_send(k, step).wait_recv()
            summed = summed + z_in[k, step - 1].astype(jnp.float32)
        full[k, z_rows(z_at), :] = summed.astype(jnp.bfloat16)
        for step in range(1, high):
            zg_send(k, step).start()

    def stage_spread(k):
        for step in range(1, high):
            zg_arrival(k, step).wait_recv()
        yg_send(k).start()

    def stage_store(k):
        yg_send(k).wait_recv()
        for segment in segments:

            @pl.when(k == segment.chunk)
            def _(segment=segment):
                target = targets[segment.member].at[
                    pl.ds(segment.row, segment.rows), pl.ds(segment.column, width)
                ]
                pltpu.make_async_copy(
                    full.at[segment.chunk, pl.ds(segment.at, segment.rows)], target,
                    out_sem.at[segment.chunk],
                ).start()

    def done(block):
        return jnp.where(
            block >= blocks, count, lax.div(jnp.maximum(block, 0) * depth, chunk)
        )

    stages = (stage_core, stage_x, stage_y, stage_z, stage_spread, stage_store)

    @pl.loop(0, blocks + LAG_OWN + 5 * LAG)
    def _(t):
        pl.when(t < blocks)(lambda: stage_make(t))
        own_at = t - LAG_OWN
        pl.when((own_at >= 0) & (own_at < blocks))(lambda: stage_own(own_at))
        pl.when(own_at == blocks - 1)(add_smalls)
        for at, stage in enumerate(stages):
            last = own_at - at * LAG + 1

            @pl.loop(done(last - 1), done(last))
            def _(k, stage=stage):
                stage(k)

    for block in range(max(0, blocks - RING), blocks):
        for j in (1, 0):
            core_send(block, j).wait_send()
    for layer in range(layers):
        for j in (1, 0):
            small_send(layer, j).wait_send()

    def all_sent(source, target, send_at, peer):
        remote(source, target, send_at, x_sem.at[0], peer).wait_send()

    all_sent(x_in, x_in, 1, x_peer)
    all_sent(y_in, y_in, 2, y_peer)
    all_sent(z_in, z_in, 3, z_peers[1])
    all_sent(z_in, z_in, 4, z_peers[1])
    all_sent(y_in, y_in, 5, y_peer)

    @pl.loop(0, count)
    def _(k):
        store_end(k).wait()


class Segment(NamedTuple):
    member: int
    row: int
    column: int
    rows: int
    chunk: int
    at: int


def plan_segments(forms, width, chunk):
    segments, place = [], 0
    for member, (depth, columns) in enumerate(forms):
        for column in range(0, columns, width):
            row = 0
            while row < depth:
                rows = min(depth - row, chunk - place % chunk)
                segments.append(
                    Segment(member, row, column, rows, place // chunk, place % chunk)
                )
                row, place = row + rows, place + rows
    return tuple(segments), place


def reduce_gradients(lefts, rights, smalls, shards, group, width):
    high = group // 2
    chunk = chunk_rows(group)
    layers = len(smalls)
    forms = [
        (left.shape[0] // shards, right.shape[1]) for left, right in zip(lefts, rights)
    ] + [small.shape for small in smalls]
    segments, used = plan_segments(forms, width, chunk)
    count = -(-used // chunk)
    piece = chunk // group
    depth = width // shards
    blocks = sum(rows * columns for rows, columns in forms[: 4 * layers]) // (depth * width)
    tokens = rights[0].shape[0]
    buffers = [
        (sum(left.shape[0] for left in lefts), tokens),
        (sum(right.shape[1] for right in rights) // width, tokens, width),
        (RING, 2, depth, width),
        (2, count * chunk, width),
        (count, chunk, width),
        (count, chunk // 2, width),
        (count, high - 1, piece, width),
        (count, chunk, width),
    ]
    semaphores = [(4 * layers, 1 + rights[2].shape[1] // width), (RING, 2), (blocks, 2),
                  (2, layers, 2), (count,), (count,), (count, high - 1), (count, high - 1),
                  (count,), (6,), (count,)]
    vmem, hbm, _ = memory_specs()
    return pl.pallas_call(
        functools.partial(reduce_kernel, high, chunk, segments, shards, layers),
        out_shape=[
            jax.ShapeDtypeStruct((layers,) + tuple(form), jnp.bfloat16)
            for form in forms[:4] + forms[-1:]
        ],
        in_specs=[hbm] * (8 * layers) + [vmem] * layers,
        out_specs=[hbm] * 5,
        scratch_shapes=[pltpu.VMEM(shape, jnp.bfloat16) for shape in buffers]
        + [pltpu.SemaphoreType.DMA(shape) for shape in semaphores],
        compiler_params=pltpu.CompilerParams(
            collective_id=1, has_side_effects=True, vmem_limit_bytes=64 * 1024 * 1024 - 65536
        ),
    )(*lefts, *rights, *smalls)


def chunk_rows(group):
    return 16 * CHUNK_TILES * group


def widen_kernel(*refs):
    total = len(refs) // 2
    for source, target in zip(refs[:total], refs[total:]):
        target[...] = source[...].astype(jnp.float32)


def widen(arrays):
    steps = 4
    specs = [
        pl.BlockSpec((1, array.shape[1] // steps, array.shape[2]), lambda i, j: (i, j, 0))
        for array in arrays
    ]
    return pl.pallas_call(
        widen_kernel,
        grid=(arrays[0].shape[0], steps),
        out_shape=[jax.ShapeDtypeStruct(array.shape, jnp.float32) for array in arrays],
        in_specs=specs,
        out_specs=specs,
        compiler_params=pltpu.CompilerParams(vmem_limit_bytes=32 * 1024 * 1024),
    )(*arrays)


def sum_gradients(lefts, rights, smalls, shards, group):
    width = smalls[0].shape[1]
    layers = len(smalls)
    reduced = reduce_gradients(lefts, rights, smalls, shards, group, width)
    spans = widen(reduced[:4])
    small = reduced[4].astype(jnp.float32)
    depth = width // shards
    shard = lax.axis_index("fsdp")
    rows = lax.dynamic_slice_in_dim(small[:, :8], shard * depth, depth, axis=2)
    up_shift = lax.dynamic_slice_in_dim(small, 8 + shard, 1, axis=1)[:, 0]
    table = small[:, 16 : 16 + H, : 3 * NB].reshape(layers, H, 3, NB)
    table = lax.dynamic_slice_in_dim(table, shard * (NB // shards), NB // shards, axis=3)
    return tuple(spans) + (
        rows[:, :6], up_shift, rows[:, 6:], jnp.transpose(table, (0, 2, 3, 1)),
    )


def opening_kernel(items, *refs):
    total = len(items)
    ready = 1 + 4
    sources, forward_in = refs[:5], refs[5:9]
    outs = refs[9 : 9 + total - 1 + 3 + 14]
    vectors, up_shifts, table = outs[total - 1 : total + 2]
    forward_out = outs[total + 2 :]
    rest = refs[9 + len(outs) :]
    stages, rest = rest[:total], rest[total:]
    landing_small, load_sem, store_sem, send_sem, arrive = rest[:5]
    forward_scratch = rest[5:]
    targets = (landing_small,) + tuple(outs[: total - 1])
    dp = lax.axis_index("dp")
    shard = lax.axis_index("fsdp")
    x_at, core = lax.div(shard, 2), lax.rem(shard, 2)
    bits = (lax.rem(dp, 2), lax.rem(lax.div(dp, 2), 2))
    core_peer = (dp, x_at * 2 + 1 - core)
    other = (1 - x_at) * 2 + core
    x_peer = (dp, other)
    dp_peers = [
        (dp + 1 - 2 * bits[0], shard),
        (dp + 2 - 4 * bits[1], shard),
    ]
    barrier = pltpu.get_barrier_semaphore()
    for peer in [core_peer, x_peer] + dp_peers:
        pl.semaphore_signal(barrier, inc=1, device_id=peer, device_id_type=MESH)
    pl.semaphore_wait(barrier, 4)

    def copy(source, target, item, kind, peer):
        return pltpu.make_async_remote_copy(
            src_ref=source, dst_ref=target, send_sem=send_sem.at[item, kind],
            recv_sem=arrive.at[item, kind], device_id=peer, device_id_type=MESH,
        )

    def shard_of(i):
        member, layer = items[i]
        return sources[member] if layer is None else sources[member].at[layer]

    def depth_of(i):
        return stages[i].shape[0]

    def parts_of(i):
        return 1 if i == 0 else 4

    def small_lanes(at):
        size = stages[0].shape[1]
        return landing_small.at[:, pl.ds(pl.multiple_of(at * size, size), size)]

    def mine_out(i):
        if i == 0:
            return small_lanes(shard)
        n = depth_of(i)
        return targets[i].at[pl.ds(pl.multiple_of(shard * n, 16), n)]

    def other_out(i, quarter):
        n = depth_of(i)
        part = n // parts_of(i)
        return targets[i].at[pl.ds(pl.multiple_of(other * n + quarter * part, 16), part)]

    def other_whole(i):
        if i == 0:
            return small_lanes(other)
        n = depth_of(i)
        return targets[i].at[pl.ds(pl.multiple_of(other * n, 16), n)]

    def order_of(i):
        return (0, 1) if i % 2 == 0 else (1, 0)

    def quarter_of(i, flips):
        if parts_of(i) == 1:
            return 0
        now = [bits[axis] if axis not in flips else 1 - bits[axis] for axis in (0, 1)]
        return now[1] * 2 + now[0]

    def x_send(i):
        if i == 0:
            return copy(shard_of(i), small_lanes(shard), i, 0, x_peer)
        n = depth_of(i)
        part = n // parts_of(i)
        start = pl.multiple_of(quarter_of(i, ()) * part, 16)
        rows = pl.ds(start, part)
        landing = targets[i].at[pl.ds(pl.multiple_of(shard * n + start, 16), part)]
        return copy(shard_of(i).at[rows], landing, i, 0, x_peer)

    def first_send(i):
        mine = other_out(i, quarter_of(i, ()))
        return copy(mine, mine, i, 1, dp_peers[order_of(i)[0]])

    def second_send(i):
        mine = other_out(i, quarter_of(i, ()))
        return copy(mine, mine, i, 2, dp_peers[order_of(i)[1]])

    def relay_send(i):
        mine = other_out(i, quarter_of(i, (order_of(i)[0],)))
        return copy(mine, mine, i, 3, dp_peers[order_of(i)[1]])

    def own_share(i):
        return copy(shard_of(i), mine_out(i), i, 4, core_peer)

    def far_share(i):
        return copy(other_whole(i), other_whole(i), i, 5, core_peer)

    def load(i):
        return pltpu.make_async_copy(shard_of(i), stages[i], load_sem.at[i])

    def store(i):
        return pltpu.make_async_copy(stages[i], mine_out(i), store_sem.at[i])

    for i in range(total):
        x_send(i).start()
    for i in range(total):
        own_share(i).start()
        load(i).start()

    def spread(i):
        x_send(i).wait_recv()
        if parts_of(i) == 4:
            first_send(i).start()
            second_send(i).start()
        load(i).wait()
        store(i).start()

    def relay(i):
        if parts_of(i) == 4:
            first_send(i).wait_recv()
            relay_send(i).start()

    def share(i):
        if parts_of(i) == 4:
            second_send(i).wait_recv()
            relay_send(i).wait_recv()
        far_share(i).start()

    def arrived(i):
        own_share(i).wait_recv()
        far_share(i).wait_recv()
        store(i).wait()

    for step in range(ready + 3):
        if step < ready:
            spread(step)
        elif step < total:
            spread(step)
        if 0 <= step - 1 < ready:
            relay(step - 1)
        if 0 <= step - 3 < ready:
            share(step - 3)
    for i in range(ready):
        arrived(i)
    place_small(landing_small, vectors, up_shifts, table)

    waiting = [functools.partial(spread, i) for i in range(ready + 3, total)]
    waiting += [functools.partial(relay, i) for i in range(ready, total)]
    waiting += [functools.partial(share, i) for i in range(ready, total)]
    points = 4
    per_point = -(-len(waiting) // points)

    def service(point):
        for act in waiting[point * per_point : (point + 1) * per_point]:
            act()

    forward_core(
        0, service, *forward_in, vectors, up_shifts, table, *targets[1:5], *forward_out,
        *forward_scratch,
    )
    for i in range(ready, total):
        arrived(i)
    for i in range(total):
        own_share(i).wait_send()
        far_share(i).wait_send()
        x_send(i).wait_send()
        if parts_of(i) == 4:
            first_send(i).wait_send()
            second_send(i).wait_send()
            relay_send(i).wait_send()


def place_small(landing, vectors, up_shifts, table):
    lanes = landing.shape[1]
    each = 2 * WIN
    shards = lanes // each

    def selected(rows, own, width):
        source = lax.broadcasted_iota(jnp.int32, (lanes, width), 0)
        target = lax.broadcasted_iota(jnp.int32, (lanes, width), 1)
        within = source % each
        picked = (within < own) & (target == source // each * own + within)
        return jnp.dot(
            landing[rows, :], picked.astype(jnp.float32).astype(jnp.bfloat16),
            preferred_element_type=jnp.float32,
        )

    layers = up_shifts.shape[0]
    width = vectors.shape[1]
    vectors[...] = selected(pl.ds(0, 16), width // shards, width)
    shift_rows = landing[16:32, :].astype(jnp.float32)
    runs = width // each
    for layer in range(layers):
        for shard in range(shards):
            for run in range(runs):
                start = shard * width + run * each
                up_shifts[layer : layer + 1, start : start + each] = shift_rows[
                    layer * runs + run : layer * runs + run + 1,
                    shard * each : (shard + 1) * each,
                ]
    table[...] = selected(pl.ds(32, table.shape[0]), NB // shards, WIN)


def small_rows(biases, ffn_in_bias, gains, tables):
    layers = biases.shape[0]
    each = 2 * WIN
    vectors = jnp.concatenate([biases, gains], axis=1).reshape(layers * 8, -1)
    vectors = jnp.pad(vectors, ((0, 16 - 8 * layers), (0, each - vectors.shape[1])))
    shifts = ffn_in_bias.reshape(-1, each)
    shifts = jnp.pad(shifts, ((0, 16 - shifts.shape[0]), (0, 0)))
    entries = jnp.swapaxes(tables, 2, 3)
    entries = jnp.pad(
        entries, ((0, 0), (0, 0), (0, 16 - H), (0, each - entries.shape[3]))
    ).reshape(layers * 48, each)
    return jnp.concatenate([vectors, shifts, entries], axis=0)


def open_layers(sources, small, shards, inputs, buckets, live, lengths):
    layers = sources[0].shape[0]
    rows, width = inputs.shape
    items = [(4, None)] + [(member, layer) for layer in range(layers) for member in range(4)]
    forms = [small.shape] + [sources[member].shape[1:] for member, _ in items[1:]]
    total = len(items)
    hidden = sources[2].shape[2]
    outs, scratch = forward_forms(rows, width, hidden)
    vmem, hbm, smem = memory_specs()
    shared = [
        jax.ShapeDtypeStruct((16, width), jnp.float32),
        jax.ShapeDtypeStruct((layers, hidden), jnp.float32),
        jax.ShapeDtypeStruct((layers * 48, WIN), jnp.float32),
    ]
    results = pl.pallas_call(
        functools.partial(opening_kernel, tuple(items)),
        out_shape=[
            jax.ShapeDtypeStruct((form[0] * shards, form[1]), jnp.bfloat16) for form in forms[1:]
        ]
        + shared
        + outs,
        in_specs=[hbm] * 5 + [vmem, vmem, vmem, smem],
        out_specs=[hbm] * (total - 1) + [vmem] * (3 + len(outs)),
        scratch_shapes=[pltpu.VMEM(form, jnp.bfloat16) for form in forms]
        + [
            pltpu.VMEM((small.shape[0], small.shape[1] * shards), jnp.bfloat16),
            pltpu.SemaphoreType.DMA((total,)),
            pltpu.SemaphoreType.DMA((total,)),
            pltpu.SemaphoreType.DMA((total, 6)),
            pltpu.SemaphoreType.DMA((total, 6)),
        ]
        + scratch,
        compiler_params=pltpu.CompilerParams(
            collective_id=0, has_side_effects=True, vmem_limit_bytes=58 * 1024 * 1024
        ),
    )(*sources, small, inputs, buckets, live, lengths)
    weights = [results[4 * layer : 4 * layer + 4] for layer in range(layers)]
    return weights, results[total - 1 : total + 2], results[total + 2 :]


def contract(left, right, left_axis, right_axis):
    return lax.dot_general(
        left, right, (((left_axis,), (right_axis,)), ((), ())),
        preferred_element_type=jnp.float32,
    )


def positions_of(axis):
    return lax.broadcasted_iota(jnp.int32, (WIN, WIN), axis)


def linear_bucket(offset):
    return jnp.clip(offset, -(NB // 2), NB // 2 - 1) + NB // 2


def lane_halves():
    lane = lax.broadcasted_iota(jnp.int32, (1, 2 * DH), 1)
    first = (lane < DH).astype(jnp.float32)
    return first.astype(jnp.bfloat16), (1.0 - first).astype(jnp.bfloat16)


def forward_kernel(layer, *refs):
    forward_core(layer, lambda point: None, *refs)


def forward_core(
    layer, service, x_ref, buckets, live, lengths, all_vectors, up_shifts, table, w_in_hbm,
    w_out_hbm, w_up_hbm, w_down_hbm, out_ref, q_ref, k_ref, v_ref, o_turned, p_ref, low_turned, n1_ref, r1_ref,
    slope_ref, g_turned, n2_ref, r2_ref, x_turned, w_in, w_out, w_up, w_down, allowed, y1, total,
    o_ref, low_ref, sem,
):
    loads = [
        pltpu.make_async_copy(source, target, sem.at[at])
        for at, (source, target) in enumerate(
            ((w_in_hbm, w_in), (w_out_hbm, w_out), (w_up_hbm, w_up), (w_down_hbm, w_down))
        )
    ]
    for load in loads:
        load.start()
    vectors = all_vectors.at[pl.ds(8 * layer, 8)]
    up_shift = up_shifts.at[pl.ds(layer, 1)]
    rows, width = x_ref.shape
    windows = rows // WIN
    row, column = positions_of(0), positions_of(1)
    offset = linear_bucket(column - row)
    first, second = lane_halves()
    for w in range(windows):
        row_doc, column_doc = jnp.zeros_like(row), jnp.zeros_like(column)
        end = 0
        for k in range(lengths.shape[1]):
            end = end + lengths[w, k]
            row_doc = row_doc + (row >= end).astype(jnp.int32)
            column_doc = column_doc + (column >= end).astype(jnp.int32)
        alive = jnp.broadcast_to(live[w : w + 1, :], (WIN, WIN))
        seen = (row_doc == column_doc) & ((alive == 1) | (row == column))
        allowed[w] = seen.astype(jnp.int32)

    loads[0].wait()
    inputs = x_ref[...]
    q_ref[...] = (
        (jnp.dot(inputs, w_in[:, :width], preferred_element_type=jnp.float32) + vectors[0:1, :])
        * DH ** (-0.5)
    ).astype(jnp.bfloat16)
    k_ref[...] = jnp.dot(
        inputs, w_in[:, width : 2 * width], preferred_element_type=jnp.float32
    ).astype(jnp.bfloat16)
    v_ref[...] = (
        jnp.dot(inputs, w_in[:, 2 * width :], preferred_element_type=jnp.float32)
        + vectors[1:2, :]
    ).astype(jnp.bfloat16)
    service(0)

    def attend(w, pair):
        span = pl.ds(w * WIN, WIN)
        lanes = pl.ds(pl.multiple_of(pair * 2 * DH, 2 * DH), 2 * DH)
        queries, keys, values = q_ref[span, lanes], k_ref[span, lanes], v_ref[span, lanes]
        mixed = []
        for side, half in enumerate((first, second)):
            head = pair * 2 + side
            scores = contract(queries * half, keys, 1, 1)
            bias = 0.0
            for kind, index in enumerate((offset, buckets[0, span, :], buckets[1, span, :])):
                entry = table[pl.ds(48 * layer + 16 * kind + head, 1), :]
                entries = jnp.broadcast_to(entry, (WIN, WIN))
                bias = bias + jnp.take_along_axis(
                    entries, index, axis=1, mode="promise_in_bounds"
                )
            scores = jnp.where(allowed[w] == 1, scores + bias, -1e30)
            exponent = jnp.exp(scores - jnp.max(scores, axis=-1, keepdims=True))
            probs = exponent / jnp.sum(exponent, axis=-1, keepdims=True)
            p_ref[w * H + head] = probs
            mixed.append(
                jnp.dot(
                    probs.astype(jnp.bfloat16), values * half, preferred_element_type=jnp.float32
                )
            )
        o_ref[span, lanes] = (mixed[0] + mixed[1]).astype(jnp.bfloat16)

    for w in range(windows):

        @pl.loop(0, H // 4)
        def _(quad, w=w):
            attend(w, quad * 2)
            attend(w, quad * 2 + 1)

        service(1 + w)

    x_turned[...] = jnp.transpose(inputs)
    o_turned[...] = jnp.transpose(o_ref[...])
    loads[1].wait()
    attended = (
        jnp.dot(o_ref[...], w_out[...], preferred_element_type=jnp.float32) + vectors[2:3, :]
    )
    first_norm, normed, inverse = norm_forward(
        inputs.astype(jnp.float32) + attended, vectors[6:7, :], vectors[3:4, :]
    )
    n1_ref[...] = normed
    r1_ref[...] = jnp.broadcast_to(inverse, r1_ref.shape)
    y1[...] = first_norm
    low = first_norm.astype(jnp.bfloat16)
    low_ref[...] = low
    low_turned[...] = jnp.transpose(low)
    total[...] = jnp.zeros_like(total)
    service(1 + windows)
    loads[2].wait()
    loads[3].wait()

    @pl.loop(0, w_up.shape[1] // width)
    def _(at):
        lanes = pl.ds(pl.multiple_of(at * width, width), width)
        hidden = (
            jnp.dot(low_ref[...], w_up[:, lanes], preferred_element_type=jnp.float32)
            + up_shift[:, lanes]
        )
        mass = 0.5 + 0.5 * lax.erf(hidden * 0.5**0.5)
        slope_ref[:, lanes] = mass + hidden * jnp.exp(-0.5 * hidden * hidden) * (
            0.5 / math.pi
        ) ** 0.5
        active = (hidden * mass).astype(jnp.bfloat16)
        g_turned[lanes, :] = jnp.transpose(active)
        total[...] += jnp.dot(active, w_down[lanes, :], preferred_element_type=jnp.float32)

    result, normed, inverse = norm_forward(
        y1[...] + (total[...] + vectors[4:5, :]), vectors[7:8, :], vectors[5:6, :]
    )
    n2_ref[...] = normed
    r2_ref[...] = jnp.broadcast_to(inverse, r2_ref.shape)
    if len(out_ref.shape) == 3:
        out_ref[0] = inputs
        out_ref[1] = result.astype(jnp.bfloat16)
    else:
        out_ref[...] = result.astype(jnp.bfloat16)


def forward_forms(rows, width, hidden):
    low, full = jnp.bfloat16, jnp.float32
    narrow = jax.ShapeDtypeStruct((rows, width), low)
    wide = jax.ShapeDtypeStruct((rows, width), full)
    column = jax.ShapeDtypeStruct((rows, WIN), full)
    turned = jax.ShapeDtypeStruct((width, rows), low)
    outs = [
        narrow, narrow, narrow, narrow, turned,
        jax.ShapeDtypeStruct((rows // WIN * H, WIN, WIN), full),
        turned, wide, column,
        jax.ShapeDtypeStruct((rows, hidden), full),
        jax.ShapeDtypeStruct((hidden, rows), low),
        wide, column, turned,
    ]
    scratch = [
        pltpu.VMEM((width, 3 * width), low), pltpu.VMEM((width, width), low),
        pltpu.VMEM((width, hidden), low), pltpu.VMEM((hidden, width), low),
        pltpu.VMEM((rows // WIN, WIN, WIN), jnp.int32),
        pltpu.VMEM((rows, width), full), pltpu.VMEM((rows, width), full),
        pltpu.VMEM((rows, width), low), pltpu.VMEM((rows, width), low),
        pltpu.SemaphoreType.DMA((4,)),
    ]
    return outs, scratch


def memory_specs():
    return [
        pl.BlockSpec(memory_space=space)
        for space in (
            pltpu.MemorySpace.VMEM, pltpu.MemorySpace.HBM, pltpu.MemorySpace.SMEM
        )
    ]


def forward_layer(layer, inputs, weights, shared, buckets, live, lengths):
    rows, width = inputs.shape
    outs, scratch = forward_forms(rows, width, weights[2].shape[1])
    outs[0] = jax.ShapeDtypeStruct((layer + 1, rows, width), jnp.bfloat16)
    vmem, hbm, smem = memory_specs()
    return pl.pallas_call(
        functools.partial(forward_kernel, layer),
        out_shape=outs,
        in_specs=[vmem, vmem, vmem, smem, vmem, vmem, vmem, hbm, hbm, hbm, hbm],
        out_specs=[vmem] * len(outs),
        scratch_shapes=scratch,
        compiler_params=pltpu.CompilerParams(vmem_limit_bytes=56 * 1024 * 1024),
    )(inputs, buckets, live, lengths, *shared, *weights)


def backward_kernel(
    layer, dz_ref, n2_ref, r2_ref, slope_ref, n1_ref, r1_ref, p_ref, q_ref, k_ref, v_ref, buckets,
    all_vectors, w_down_hbm, w_up_hbm, w_out_hbm, w_in_hbm, dx_ref, df_ref, du_ref, da_ref, dqkv_ref,
    small_ref, w_down, w_up, w_out, w_in, small, grad, mixed, spread, sem,
):
    loads = [
        pltpu.make_async_copy(source, target, sem.at[at])
        for at, (source, target) in enumerate(
            ((w_down_hbm, w_down), (w_up_hbm, w_up), (w_out_hbm, w_out), (w_in_hbm, w_in))
        )
    ]
    for load in loads:
        load.start()
    vectors = all_vectors.at[pl.ds(8 * layer, 8)]
    rows, width = dz_ref.shape
    windows = rows // WIN
    first, second = lane_halves()
    small[...] = jnp.zeros_like(small)
    spread[...] = jnp.zeros_like(spread)

    def add_row(at, values):
        small[pl.ds(at, 1), :] = jnp.sum(values, axis=0, keepdims=True)

    def norm_back(incoming, normed, inverse, gain_row):
        scaled = incoming * gain_row
        centred = (
            scaled
            - jnp.mean(scaled, axis=-1, keepdims=True)
            - normed * jnp.mean(scaled * normed, axis=-1, keepdims=True)
        )
        return centred * inverse

    incoming, normed = dz_ref[...], n2_ref[...]
    add_row(7, incoming * normed)
    add_row(5, incoming)
    grad_second = norm_back(incoming, normed, r2_ref[:, 0:1], vectors[7:8, :])
    grad[...] = grad_second
    branch_low = grad_second.astype(jnp.bfloat16)
    df_ref[...] = branch_low
    add_row(4, branch_low.astype(jnp.float32))
    loads[0].wait()
    loads[1].wait()

    @pl.loop(0, w_up.shape[1] // width)
    def _(at):
        lanes = pl.ds(pl.multiple_of(at * width, width), width)
        grad_active = contract(df_ref[...], w_down[lanes, :], 1, 1)
        hidden_low = (grad_active * slope_ref[:, lanes]).astype(jnp.bfloat16)
        du_ref[:, lanes] = hidden_low
        add_row(8 + at, hidden_low.astype(jnp.float32))
        grad[...] += contract(hidden_low, w_up[:, lanes], 1, 1)

    incoming, normed = grad[...], n1_ref[...]
    add_row(6, incoming * normed)
    add_row(3, incoming)
    grad_attended = norm_back(incoming, normed, r1_ref[:, 0:1], vectors[6:7, :])
    grad[...] = grad_attended
    attended_low = grad_attended.astype(jnp.bfloat16)
    da_ref[...] = attended_low
    add_row(2, attended_low.astype(jnp.float32))
    loads[2].wait()
    mixed[...] = contract(attended_low, w_out[...], 1, 1).astype(jnp.bfloat16)

    def attend(w, pair):
        span = pl.ds(w * WIN, WIN)
        start = pl.multiple_of(pair * 2 * DH, 2 * DH)
        lanes = pl.ds(start, 2 * DH)
        queries, keys, values = q_ref[span, lanes], k_ref[span, lanes], v_ref[span, lanes]
        outgoing = mixed[span, lanes]
        sums = [0.0, 0.0, 0.0]
        for side, half in enumerate((first, second)):
            head = pair * 2 + side
            probs = p_ref[w * H + head]
            own = outgoing * half
            grad_probs = contract(own, values, 1, 1)
            centred = grad_probs - jnp.sum(probs * grad_probs, axis=-1, keepdims=True)
            grad_scores = (probs * centred).astype(jnp.bfloat16)
            spread[pl.ds(head, WIN, stride=16), :] = grad_scores.astype(jnp.float32)
            sums[0] += jnp.dot(grad_scores, keys * half, preferred_element_type=jnp.float32)
            sums[1] += contract(grad_scores, queries * half, 0, 0)
            sums[2] += contract(probs.astype(jnp.bfloat16), own, 0, 0)
        scaled = sums[0].astype(jnp.bfloat16).astype(jnp.float32) * DH ** (-0.5)
        dqkv_ref[span, lanes] = scaled.astype(jnp.bfloat16)
        dqkv_ref[span, pl.ds(pl.multiple_of(start + width, 2 * DH), 2 * DH)] = sums[1].astype(
            jnp.bfloat16
        )
        dqkv_ref[span, pl.ds(pl.multiple_of(start + 2 * width, 2 * DH), 2 * DH)] = sums[2].astype(
            jnp.bfloat16
        )

    bucket = lax.broadcasted_iota(jnp.int32, (NB, WIN), 0)
    column = lax.broadcasted_iota(jnp.int32, (1, WIN), 1)
    group = 8
    for w in range(windows):

        @pl.loop(0, H // 4)
        def _(quad, w=w):
            attend(w, quad * 2)
            attend(w, quad * 2 + 1)

        def count_group(at, w=w):
            hits, terms = [], []
            for step in range(group):
                i = at * group + step
                indices = (
                    linear_bucket(column - i),
                    buckets[0, pl.ds(w * WIN + i, 1), :],
                    buckets[1, pl.ds(w * WIN + i, 1), :],
                )
                hits.append(
                    jnp.concatenate(
                        [(index == bucket).astype(jnp.float32) for index in indices], axis=0
                    ).astype(jnp.bfloat16)
                )
                terms.append(
                    spread[pl.ds(pl.multiple_of(i * 16, 16), 16), :].astype(jnp.bfloat16)
                )
            return contract(jnp.concatenate(terms, axis=1), jnp.concatenate(hits, axis=1), 1, 1)

        @pl.loop(0, WIN // group)
        def _(at):
            small[16:32, 0 : 3 * NB] += count_group(at)

    loads[3].wait()
    add_row(0, dqkv_ref[:, :width].astype(jnp.float32))
    add_row(1, dqkv_ref[:, 2 * width :].astype(jnp.float32))
    dx_ref[...] = grad[...] + contract(dqkv_ref[...], w_in[...], 1, 1)
    small_ref[...] = small[...].astype(jnp.bfloat16)


def backward_layer(layer, incoming, weights, vectors, kept, buckets):
    w_in, w_out, w_up, w_down = weights
    rows, width = incoming.shape
    hidden = w_up.shape[1]
    low, full = jnp.bfloat16, jnp.float32
    narrow = jax.ShapeDtypeStruct((rows, width), low)
    vmem, hbm, _ = memory_specs()
    q, k, v, _, p, _, n1, r1, slope, _, n2, r2, _ = kept
    return pl.pallas_call(
        functools.partial(backward_kernel, layer),
        out_shape=[
            jax.ShapeDtypeStruct((rows, width), full),
            narrow,
            jax.ShapeDtypeStruct((rows, hidden), low),
            narrow,
            jax.ShapeDtypeStruct((rows, 3 * width), low),
            jax.ShapeDtypeStruct((64, width), low),
        ],
        in_specs=[vmem] * 12 + [hbm] * 4,
        out_specs=[vmem] * 6,
        scratch_shapes=[
            pltpu.VMEM(w_down.shape, low), pltpu.VMEM(w_up.shape, low),
            pltpu.VMEM(w_out.shape, low), pltpu.VMEM(w_in.shape, low),
            pltpu.VMEM((64, width), full), pltpu.VMEM((rows, width), full),
            pltpu.VMEM((rows, width), low), pltpu.VMEM((WIN * 16, WIN), full),
            pltpu.SemaphoreType.DMA((4,)),
        ],
        compiler_params=pltpu.CompilerParams(vmem_limit_bytes=56 * 1024 * 1024),
    )(incoming, n2, r2, slope, n1, r1, p, q, k, v, buckets, vectors, w_down, w_up, w_out, w_in)


def local(
    tokens,
    out_grad,
    mlm_mask,
    live_mask,
    doc_lengths,
    layout_buckets,
    attn_in,
    attn_out,
    ffn_in,
    ffn_out,
    biases,
    ffn_in_bias,
    gains,
    tables,
):
    shards = lax.axis_size("fsdp")
    live = live_mask.reshape(-1, WIN)
    weights_list, shared, first = open_layers(
        (attn_in, attn_out, ffn_in, ffn_out), small_rows(biases, ffn_in_bias, gains, tables),
        shards, tokens, layout_buckets, live, doc_lengths,
    )
    current, *kept = first
    outputs, *kept_next = forward_layer(
        1, current, weights_list[1], shared, layout_buckets, live, doc_lengths
    )
    kept_list = [kept, kept_next]
    incoming = out_grad.astype(jnp.float32) * mlm_mask.astype(jnp.float32)[:, None]
    lefts, rights, smalls = [], [], []
    for layer in reversed(range(len(weights_list))):
        kept = kept_list[layer]
        incoming, df, du, da, dqkv, small = backward_layer(
            layer, incoming, weights_list[layer], shared[0], kept, layout_buckets
        )
        lefts = [kept[12], kept[3], kept[5], kept[9]] + lefts
        rights = [dqkv, da, du, df] + rights
        smalls = [small] + smalls
    summed = sum_gradients(lefts, rights, smalls, shards, lax.axis_size("dp"))
    return (outputs, incoming) + summed


def solution(mesh):
    return jax.shard_map(
        local,
        mesh=mesh,
        in_specs=(
            P(("dp", "fsdp"), None),
            P(("dp", "fsdp"), None),
            P(("dp", "fsdp")),
            P(("dp", "fsdp")),
            P(("dp", "fsdp"), None),
            P(None, ("dp", "fsdp"), None),
            P(None, "fsdp", None),
            P(None, "fsdp", None),
            P(None, "fsdp", None),
            P(None, "fsdp", None),
            P(None, None, "fsdp"),
            P(None, "fsdp"),
            P(None, None, "fsdp"),
            P(None, None, "fsdp", None),
        ),
        out_specs=(
            P(None, ("dp", "fsdp"), None),
            P(("dp", "fsdp"), None),
            P(None, "fsdp", None),
            P(None, "fsdp", None),
            P(None, "fsdp", None),
            P(None, "fsdp", None),
            P(None, None, "fsdp"),
            P(None, "fsdp"),
            P(None, None, "fsdp"),
            P(None, None, "fsdp", None),
        ),
        check_vma=False,
    )
```

```python
import functools
import math
from typing import NamedTuple

import jax
import jax.numpy as jnp
from jax import lax
from jax.experimental import pallas as pl
from jax.experimental.pallas import tpu as pltpu
from jax.sharding import PartitionSpec as P

H = 12
DH = 64
NB = 32
WIN = 128


EPSILON = 1e-05
LAG = 1
LAG_OWN = 2


def norm_forward(values, gain_row, shift_row):
    centre = values - jnp.mean(values, axis=-1, keepdims=True)
    spread = jnp.mean(centre * centre, axis=-1, keepdims=True)
    inverse = lax.rsqrt(spread + EPSILON)
    normed = centre * inverse
    return (normed * gain_row + shift_row, normed, inverse)


MESH = pl.DeviceIdType.MESH
CHUNK_TILES = 1


def add_rows(target, other):
    target[...] = (target[...].astype(jnp.float32) + other[...].astype(jnp.float32)).astype(
        jnp.bfloat16
    )


RING = 4


def reduce_kernel(high, chunk, segments, shards, layers, *refs):
    each = 4 * layers
    lefts, rights, smalls = refs[:each], refs[each : 2 * each], refs[2 * each : 2 * each + layers]
    spreads, buckets = refs[2 * each + layers : 2 * each + 2 * layers], refs[2 * each + 2 * layers]
    refs = refs[2 * each + 2 * layers + 1 :]
    members = len(refs) - 21
    targets = [
        refs[kind].at[layer] for layer in range(layers) for kind in range(4)
    ] + [refs[4].at[layer] for layer in range(layers)]
    (counts, small_all, left, right, ring, total, x_in, y_in, z_in, full, load_sem, ring_sem,
     core_sem, small_sem, x_sem, y_sem, z_sem, zg_sem, yg_sem, sent, out_sem) = refs[members:]
    dp = lax.axis_index("dp")
    shard = lax.axis_index("fsdp")
    y_at, z_at = lax.rem(dp, 2), lax.div(dp, 2)
    x_at, core = lax.div(shard, 2), lax.rem(shard, 2)
    core_peer = (dp, x_at * 2 + 1 - core)
    x_peer = (dp, (1 - x_at) * 2 + core)
    y_peer = (z_at * 2 + 1 - y_at, shard)
    z_of = [lax.rem(z_at + step, high) for step in range(high)]
    z_from = [lax.rem(z_at + high - step, high) for step in range(high)]
    z_peers = [(z_of[step] * 2 + y_at, shard) for step in range(high)]
    half = chunk // 2
    piece = half // high
    width = full.shape[2]
    count = full.shape[0]
    depth = width // shards
    down = rights[2].shape[1] // width
    blocks = layers * (8 + down)

    barrier = pltpu.get_barrier_semaphore()
    peers = [core_peer, x_peer, y_peer] + z_peers[1:]
    for peer in peers:
        pl.semaphore_signal(barrier, inc=1, device_id=peer, device_id_type=MESH)
    pl.semaphore_wait(barrier, len(peers))

    def remote(source, target, send_at, receive, peer):
        return pltpu.make_async_remote_copy(
            src_ref=source, dst_ref=target, send_sem=sent.at[send_at], recv_sem=receive,
            device_id=peer, device_id_type=MESH,
        )

    loads, at_left, at_right, first_block = [], 0, 0, []
    for layer in range(layers):
        for kind in range(4):
            member = 4 * layer + kind
            rows = lefts[member].shape[0]
            pairs = [(lefts[member], left.at[pl.ds(at_left, rows)])]
            for column in range(0, rights[member].shape[1], width):
                pairs.append((rights[member].at[:, pl.ds(column, width)], right.at[at_right]))
                at_right += 1
            at_left += rows
            loads.append([
                pltpu.make_async_copy(source, target, load_sem.at[member, at])
                for at, (source, target) in enumerate(pairs)
            ])
            first_block.append(layer * (8 + down) + (0, 3, 4, 4 + down)[kind])
    for load in loads:
        for copy in load:
            copy.start()

    def gradient(block, wanted):
        layer, b = lax.div(block, 8 + down), lax.rem(block, 8 + down)
        deep = b - 4 - down
        start = layer * (at_left // layers) + jnp.where(
            b < 3, 0, jnp.where(b < 4, width, jnp.where(deep < 0, 2 * width, 3 * width))
        )
        start = start + jnp.where(deep < 0, depth * wanted, down * depth * wanted + depth * deep)
        column = layer * (at_right // layers) + jnp.minimum(b, 4 + down)
        return jnp.dot(
            left[pl.ds(pl.multiple_of(start, 64), depth), :], right[column],
            preferred_element_type=jnp.float32,
        )

    def block_rows(block):
        return pl.ds(pl.multiple_of(block * depth, 64), depth)

    def chunk_rows_of(k):
        return pl.ds(pl.multiple_of(k * chunk, chunk), chunk)

    def wanted_of(j, side):
        return (x_at if j == 0 else 1 - x_at) * 2 + side

    def core_send(block, j):
        slot = lax.rem(block, RING)
        return pltpu.make_async_remote_copy(
            src_ref=ring.at[slot, j], dst_ref=total.at[j, block_rows(block)],
            send_sem=ring_sem.at[slot, j], recv_sem=core_sem.at[block, j],
            device_id=core_peer, device_id_type=MESH,
        )

    small_depth = smalls[0].shape[0]

    def small_rows_of(layer):
        return pl.ds(blocks * depth + layer * small_depth, small_depth)

    def small_send(layer, j):
        return pltpu.make_async_remote_copy(
            src_ref=small_all.at[layer], dst_ref=total.at[j, small_rows_of(layer)],
            send_sem=small_sem.at[0, layer, j], recv_sem=small_sem.at[1, layer, j],
            device_id=core_peer, device_id_type=MESH,
        )

    bucket = lax.broadcasted_iota(jnp.int32, (NB, WIN), 0)
    lane = lax.broadcasted_iota(jnp.int32, (1, WIN), 1)
    together = 8
    counting = WIN // together
    counts[...] = jnp.zeros_like(counts)

    def count_group(w, at):
        hits, terms = [], [[] for _ in range(layers)]
        for step in range(together):
            i = at * together + step
            indices = (
                linear_bucket(lane - i),
                buckets[0, pl.ds(w * WIN + i, 1), :],
                buckets[1, pl.ds(w * WIN + i, 1), :],
            )
            found = [(index == bucket).astype(jnp.float32) for index in indices]
            found.append(jnp.zeros((WIN - 3 * NB, WIN), jnp.float32))
            hits.append(jnp.concatenate(found, axis=0).astype(jnp.bfloat16))
            for layer in range(layers):
                terms[layer].append(spreads[layer][w, pl.ds(pl.multiple_of(i * 16, 16), 16), :])
        hits = jnp.concatenate(hits, axis=1)
        for layer in range(layers):
            counts[layer] += lax.dot_general(
                jnp.concatenate(terms[layer], axis=1), hits, (((1,), (1,)), ((), ())),
                preferred_element_type=jnp.float32,
            )

    def count_step(at):
        for w in range(spreads[0].shape[0]):
            count_group(w, at)

    def finish_smalls():
        for layer in range(layers):
            small_all[layer] = smalls[layer][...]
            small_all[layer, 16:32, 0:WIN] = counts[layer].astype(jnp.bfloat16)
            for j in (1, 0):
                small_send(layer, j).start()

    def stage_make(block):
        for member, first in enumerate(first_block):

            @pl.when(block == first)
            def _(member=member):
                for copy in loads[member]:
                    copy.wait()

        for j in (1, 0):

            @pl.when(block >= RING)
            def _(j=j):
                core_send(block, j).wait_send()

            ring[lax.rem(block, RING), j] = gradient(block, wanted_of(j, 1 - core)).astype(
                jnp.bfloat16
            )
            core_send(block, j).start()

    def stage_own(block):
        for j in (1, 0):
            own = gradient(block, wanted_of(j, core))
            core_send(block, j).wait_recv()
            place = total.at[j, block_rows(block)]
            place[...] = (place[...].astype(jnp.float32) + own).astype(jnp.bfloat16)

    def add_smalls():
        for layer in range(layers):
            for j in (1, 0):
                small_send(layer, j).wait_recv()
                add_rows(total.at[j, small_rows_of(layer)], small_all.at[layer])

    def x_send(k):
        return remote(total.at[1, chunk_rows_of(k)], x_in.at[k], 1, x_sem.at[k], x_peer)

    def y_rows(side):
        return pl.ds(pl.multiple_of(side * half, half), half)

    def y_part(k, side):
        return total.at[0, pl.ds(pl.multiple_of(k * chunk + side * half, half), half)]

    def y_send(k):
        return remote(y_part(k, 1 - y_at), y_in.at[k], 2, y_sem.at[k], y_peer)

    def z_rows(at):
        return pl.ds(pl.multiple_of(y_at * half + at * piece, piece), piece)

    def z_part(k, at):
        start = k * chunk + y_at * half + at * piece
        return total.at[0, pl.ds(pl.multiple_of(start, piece), piece)]

    def z_send(k, step):
        return remote(
            z_part(k, z_of[step]), z_in.at[k, step - 1], 3, z_sem.at[k, step - 1], z_peers[step]
        )

    def zg_send(k, step):
        mine = full.at[k, z_rows(z_at)]
        return remote(mine, mine, 4, zg_sem.at[k, step - 1], z_peers[step])

    def zg_arrival(k, step):
        theirs = full.at[k, z_rows(z_from[step])]
        return remote(theirs, theirs, 4, zg_sem.at[k, step - 1], z_peers[step])

    def yg_send(k):
        mine = full.at[k, y_rows(y_at)]
        return remote(mine, mine, 5, yg_sem.at[k], y_peer)

    def store_end(k):
        return pltpu.make_async_copy(full.at[k], full.at[k], out_sem.at[k])

    def stage_core(k):
        x_send(k).start()

    def stage_x(k):
        x_send(k).wait_recv()
        add_rows(total.at[0, chunk_rows_of(k)], x_in.at[k])
        y_send(k).start()

    def stage_y(k):
        y_send(k).wait_recv()
        add_rows(y_part(k, y_at), y_in.at[k])
        for step in range(1, high):
            z_send(k, step).start()

    def stage_z(k):
        summed = z_part(k, z_at)[...].astype(jnp.float32)
        for step in range(1, high):
            z_send(k, step).wait_recv()
            summed = summed + z_in[k, step - 1].astype(jnp.float32)
        full[k, z_rows(z_at), :] = summed.astype(jnp.bfloat16)
        for step in range(1, high):
            zg_send(k, step).start()

    def stage_spread(k):
        for step in range(1, high):
            zg_arrival(k, step).wait_recv()
        yg_send(k).start()

    def stage_store(k):
        yg_send(k).wait_recv()
        for segment in segments:

            @pl.when(k == segment.chunk)
            def _(segment=segment):
                target = targets[segment.member].at[
                    pl.ds(segment.row, segment.rows), pl.ds(segment.column, width)
                ]
                pltpu.make_async_copy(
                    full.at[segment.chunk, pl.ds(segment.at, segment.rows)], target,
                    out_sem.at[segment.chunk],
                ).start()

    def done(block):
        return jnp.where(
            block >= blocks, count, lax.div(jnp.maximum(block, 0) * depth, chunk)
        )

    stages = (stage_core, stage_x, stage_y, stage_z, stage_spread, stage_store)

    @pl.loop(0, blocks + LAG_OWN + 5 * LAG)
    def _(t):
        pl.when(t < blocks)(lambda: stage_make(t))
        own_at = t - LAG_OWN
        pl.when((own_at >= 0) & (own_at < blocks))(lambda: stage_own(own_at))
        pl.when((t >= 1) & (t <= counting))(lambda: count_step(t - 1))
        pl.when(t == counting + 1)(finish_smalls)
        pl.when(own_at == blocks - 1)(add_smalls)
        for at, stage in enumerate(stages):
            last = own_at - at * LAG + 1

            @pl.loop(done(last - 1), done(last))
            def _(k, stage=stage):
                stage(k)

    for block in range(max(0, blocks - RING), blocks):
        for j in (1, 0):
            core_send(block, j).wait_send()
    for layer in range(layers):
        for j in (1, 0):
            small_send(layer, j).wait_send()

    def all_sent(source, target, send_at, peer):
        remote(source, target, send_at, x_sem.at[0], peer).wait_send()

    all_sent(x_in, x_in, 1, x_peer)
    all_sent(y_in, y_in, 2, y_peer)
    all_sent(z_in, z_in, 3, z_peers[1])
    all_sent(z_in, z_in, 4, z_peers[1])
    all_sent(y_in, y_in, 5, y_peer)

    @pl.loop(0, count)
    def _(k):
        store_end(k).wait()


class Segment(NamedTuple):
    member: int
    row: int
    column: int
    rows: int
    chunk: int
    at: int


def plan_segments(forms, width, chunk):
    segments, place = [], 0
    for member, (depth, columns) in enumerate(forms):
        for column in range(0, columns, width):
            row = 0
            while row < depth:
                rows = min(depth - row, chunk - place % chunk)
                segments.append(
                    Segment(member, row, column, rows, place // chunk, place % chunk)
                )
                row, place = row + rows, place + rows
    return tuple(segments), place


def reduce_gradients(lefts, rights, smalls, spreads, buckets, shards, group, width):
    high = group // 2
    chunk = chunk_rows(group)
    layers = len(smalls)
    forms = [
        (left.shape[0] // shards, right.shape[1]) for left, right in zip(lefts, rights)
    ] + [small.shape for small in smalls]
    segments, used = plan_segments(forms, width, chunk)
    count = -(-used // chunk)
    piece = chunk // group
    depth = width // shards
    blocks = sum(rows * columns for rows, columns in forms[: 4 * layers]) // (depth * width)
    tokens = rights[0].shape[0]
    buffers = [
        (sum(left.shape[0] for left in lefts), tokens),
        (sum(right.shape[1] for right in rights) // width, tokens, width),
        (RING, 2, depth, width),
        (2, count * chunk, width),
        (count, chunk, width),
        (count, chunk // 2, width),
        (count, high - 1, piece, width),
        (count, chunk, width),
    ]
    semaphores = [(4 * layers, 1 + rights[2].shape[1] // width), (RING, 2), (blocks, 2),
                  (2, layers, 2), (count,), (count,), (count, high - 1), (count, high - 1),
                  (count,), (6,), (count,)]
    vmem, hbm, _ = memory_specs()
    return pl.pallas_call(
        functools.partial(reduce_kernel, high, chunk, segments, shards, layers),
        out_shape=[
            jax.ShapeDtypeStruct((layers,) + tuple(form), jnp.bfloat16)
            for form in forms[:4] + forms[-1:]
        ],
        in_specs=[hbm] * (8 * layers) + [vmem] * (2 * layers + 1),
        out_specs=[hbm] * 5,
        scratch_shapes=[
            pltpu.VMEM((layers, 16, WIN), jnp.float32),
            pltpu.VMEM((layers,) + smalls[0].shape, jnp.bfloat16),
        ]
        + [pltpu.VMEM(shape, jnp.bfloat16) for shape in buffers]
        + [pltpu.SemaphoreType.DMA(shape) for shape in semaphores],
        compiler_params=pltpu.CompilerParams(
            collective_id=1, has_side_effects=True, vmem_limit_bytes=64 * 1024 * 1024 - 65536
        ),
    )(*lefts, *rights, *smalls, *spreads, buckets)


def chunk_rows(group):
    return 16 * CHUNK_TILES * group


def widen_kernel(*refs):
    total = len(refs) // 2
    for source, target in zip(refs[:total], refs[total:]):
        target[...] = source[...].astype(jnp.float32)


def widen(arrays):
    steps = 4
    specs = [
        pl.BlockSpec((1, array.shape[1] // steps, array.shape[2]), lambda i, j: (i, j, 0))
        for array in arrays
    ]
    return pl.pallas_call(
        widen_kernel,
        grid=(arrays[0].shape[0], steps),
        out_shape=[jax.ShapeDtypeStruct(array.shape, jnp.float32) for array in arrays],
        in_specs=specs,
        out_specs=specs,
        compiler_params=pltpu.CompilerParams(vmem_limit_bytes=64 * 1024 * 1024 - 65536),
    )(*arrays)


def sum_gradients(lefts, rights, smalls, spreads, buckets, shards, group):
    width = smalls[0].shape[1]
    layers = len(smalls)
    reduced = reduce_gradients(
        lefts, rights, smalls, spreads, buckets, shards, group, width
    )
    spans = widen(reduced[:4])
    small = reduced[4].astype(jnp.float32)
    depth = width // shards
    shard = lax.axis_index("fsdp")
    rows = lax.dynamic_slice_in_dim(small[:, :8], shard * depth, depth, axis=2)
    up_shift = lax.dynamic_slice_in_dim(small, 8 + shard, 1, axis=1)[:, 0]
    table = small[:, 16 : 16 + H, : 3 * NB].reshape(layers, H, 3, NB)
    table = lax.dynamic_slice_in_dim(table, shard * (NB // shards), NB // shards, axis=3)
    return tuple(spans) + (
        rows[:, :6], up_shift, rows[:, 6:], jnp.transpose(table, (0, 2, 3, 1)),
    )


def opening_kernel(items, *refs):
    total = len(items)
    ready = 1 + 4
    sources, forward_in = refs[:5], refs[5:9]
    outs = refs[9 : 9 + total - 1 + 3 + 14]
    vectors, up_shifts, table = outs[total - 1 : total + 2]
    forward_out = outs[total + 2 :]
    rest = refs[9 + len(outs) :]
    stages, rest = rest[:total], rest[total:]
    landing_small, load_sem, store_sem, send_sem, arrive = rest[:5]
    forward_scratch = rest[5:]
    targets = (landing_small,) + tuple(outs[: total - 1])
    dp = lax.axis_index("dp")
    shard = lax.axis_index("fsdp")
    x_at, core = lax.div(shard, 2), lax.rem(shard, 2)
    bits = (lax.rem(dp, 2), lax.rem(lax.div(dp, 2), 2))
    core_peer = (dp, x_at * 2 + 1 - core)
    other = (1 - x_at) * 2 + core
    x_peer = (dp, other)
    dp_peers = [
        (dp + 1 - 2 * bits[0], shard),
        (dp + 2 - 4 * bits[1], shard),
    ]
    barrier = pltpu.get_barrier_semaphore()
    for peer in [core_peer, x_peer] + dp_peers:
        pl.semaphore_signal(barrier, inc=1, device_id=peer, device_id_type=MESH)
    pl.semaphore_wait(barrier, 4)

    def copy(source, target, item, kind, peer):
        return pltpu.make_async_remote_copy(
            src_ref=source, dst_ref=target, send_sem=send_sem.at[item, kind],
            recv_sem=arrive.at[item, kind], device_id=peer, device_id_type=MESH,
        )

    def shard_of(i):
        member, layer = items[i]
        return sources[member] if layer is None else sources[member].at[layer]

    def depth_of(i):
        return stages[i].shape[0]

    def parts_of(i):
        return 1 if i == 0 else 4

    def small_lanes(at):
        size = stages[0].shape[1]
        return landing_small.at[:, pl.ds(pl.multiple_of(at * size, size), size)]

    def mine_out(i):
        if i == 0:
            return small_lanes(shard)
        n = depth_of(i)
        return targets[i].at[pl.ds(pl.multiple_of(shard * n, 16), n)]

    def other_out(i, quarter):
        n = depth_of(i)
        part = n // parts_of(i)
        return targets[i].at[pl.ds(pl.multiple_of(other * n + quarter * part, 16), part)]

    def other_whole(i):
        if i == 0:
            return small_lanes(other)
        n = depth_of(i)
        return targets[i].at[pl.ds(pl.multiple_of(other * n, 16), n)]

    def order_of(i):
        return (0, 1) if i % 2 == 0 else (1, 0)

    def quarter_of(i, flips):
        if parts_of(i) == 1:
            return 0
        now = [bits[axis] if axis not in flips else 1 - bits[axis] for axis in (0, 1)]
        return now[1] * 2 + now[0]

    def x_send(i):
        if i == 0:
            return copy(shard_of(i), small_lanes(shard), i, 0, x_peer)
        n = depth_of(i)
        part = n // parts_of(i)
        start = pl.multiple_of(quarter_of(i, ()) * part, 16)
        rows = pl.ds(start, part)
        landing = targets[i].at[pl.ds(pl.multiple_of(shard * n + start, 16), part)]
        return copy(shard_of(i).at[rows], landing, i, 0, x_peer)

    def first_send(i):
        mine = other_out(i, quarter_of(i, ()))
        return copy(mine, mine, i, 1, dp_peers[order_of(i)[0]])

    def second_send(i):
        mine = other_out(i, quarter_of(i, ()))
        return copy(mine, mine, i, 2, dp_peers[order_of(i)[1]])

    def relay_send(i):
        mine = other_out(i, quarter_of(i, (order_of(i)[0],)))
        return copy(mine, mine, i, 3, dp_peers[order_of(i)[1]])

    def own_share(i):
        return copy(shard_of(i), mine_out(i), i, 4, core_peer)

    def far_share(i):
        return copy(other_whole(i), other_whole(i), i, 5, core_peer)

    def load(i):
        return pltpu.make_async_copy(shard_of(i), stages[i], load_sem.at[i])

    def store(i):
        return pltpu.make_async_copy(stages[i], mine_out(i), store_sem.at[i])

    for i in range(total):
        x_send(i).start()
    for i in range(total):
        own_share(i).start()
        load(i).start()

    def spread(i):
        x_send(i).wait_recv()
        if parts_of(i) == 4:
            first_send(i).start()
            second_send(i).start()
        load(i).wait()
        store(i).start()

    def relay(i):
        if parts_of(i) == 4:
            first_send(i).wait_recv()
            relay_send(i).start()

    def share(i):
        if parts_of(i) == 4:
            second_send(i).wait_recv()
            relay_send(i).wait_recv()
        far_share(i).start()

    def arrived(i):
        own_share(i).wait_recv()
        far_share(i).wait_recv()
        store(i).wait()

    for step in range(ready + 3):
        if step < ready:
            spread(step)
        elif step < total:
            spread(step)
        if 0 <= step - 1 < ready:
            relay(step - 1)
        if 0 <= step - 3 < ready:
            share(step - 3)
    for i in range(ready):
        arrived(i)
    place_small(landing_small, vectors, up_shifts, table)

    waiting = [functools.partial(spread, i) for i in range(ready + 3, total)]
    waiting += [functools.partial(relay, i) for i in range(ready, total)]
    waiting += [functools.partial(share, i) for i in range(ready, total)]
    points = 4
    per_point = -(-len(waiting) // points)

    def service(point):
        for act in waiting[point * per_point : (point + 1) * per_point]:
            act()

    forward_core(
        0, service, *forward_in, vectors, up_shifts, table, *targets[1:5], *forward_out,
        *forward_scratch,
    )
    for i in range(ready, total):
        arrived(i)
    for i in range(total):
        own_share(i).wait_send()
        far_share(i).wait_send()
        x_send(i).wait_send()
        if parts_of(i) == 4:
            first_send(i).wait_send()
            second_send(i).wait_send()
            relay_send(i).wait_send()


def place_small(landing, vectors, up_shifts, table):
    lanes = landing.shape[1]
    each = 2 * WIN
    shards = lanes // each

    def selected(rows, own, width):
        source = lax.broadcasted_iota(jnp.int32, (lanes, width), 0)
        target = lax.broadcasted_iota(jnp.int32, (lanes, width), 1)
        within = source % each
        picked = (within < own) & (target == source // each * own + within)
        return jnp.dot(
            landing[rows, :], picked.astype(jnp.float32).astype(jnp.bfloat16),
            preferred_element_type=jnp.float32,
        )

    layers = up_shifts.shape[0]
    width = vectors.shape[1]
    vectors[...] = selected(pl.ds(0, 16), width // shards, width)
    shift_rows = landing[16:32, :].astype(jnp.float32)
    runs = width // each
    for layer in range(layers):
        for shard in range(shards):
            for run in range(runs):
                start = shard * width + run * each
                up_shifts[layer : layer + 1, start : start + each] = shift_rows[
                    layer * runs + run : layer * runs + run + 1,
                    shard * each : (shard + 1) * each,
                ]
    table[...] = selected(pl.ds(32, table.shape[0]), NB // shards, WIN)


def small_rows(biases, ffn_in_bias, gains, tables):
    layers = biases.shape[0]
    each = 2 * WIN
    vectors = jnp.concatenate([biases, gains], axis=1).reshape(layers * 8, -1)
    vectors = jnp.pad(vectors, ((0, 16 - 8 * layers), (0, each - vectors.shape[1])))
    shifts = ffn_in_bias.reshape(-1, each)
    shifts = jnp.pad(shifts, ((0, 16 - shifts.shape[0]), (0, 0)))
    entries = jnp.swapaxes(tables, 2, 3)
    entries = jnp.pad(
        entries, ((0, 0), (0, 0), (0, 16 - H), (0, each - entries.shape[3]))
    ).reshape(layers * 48, each)
    return jnp.concatenate([vectors, shifts, entries], axis=0)


def open_layers(sources, small, shards, inputs, buckets, live, lengths):
    layers = sources[0].shape[0]
    rows, width = inputs.shape
    items = [(4, None)] + [(member, layer) for layer in range(layers) for member in range(4)]
    forms = [small.shape] + [sources[member].shape[1:] for member, _ in items[1:]]
    total = len(items)
    hidden = sources[2].shape[2]
    outs, scratch = forward_forms(rows, width, hidden)
    vmem, hbm, smem = memory_specs()
    shared = [
        jax.ShapeDtypeStruct((16, width), jnp.float32),
        jax.ShapeDtypeStruct((layers, hidden), jnp.float32),
        jax.ShapeDtypeStruct((layers * 48, WIN), jnp.float32),
    ]
    results = pl.pallas_call(
        functools.partial(opening_kernel, tuple(items)),
        out_shape=[
            jax.ShapeDtypeStruct((form[0] * shards, form[1]), jnp.bfloat16) for form in forms[1:]
        ]
        + shared
        + outs,
        in_specs=[hbm] * 5 + [vmem, vmem, vmem, smem],
        out_specs=[hbm] * (total - 1) + [vmem] * (3 + len(outs)),
        scratch_shapes=[pltpu.VMEM(form, jnp.bfloat16) for form in forms]
        + [
            pltpu.VMEM((small.shape[0], small.shape[1] * shards), jnp.bfloat16),
            pltpu.SemaphoreType.DMA((total,)),
            pltpu.SemaphoreType.DMA((total,)),
            pltpu.SemaphoreType.DMA((total, 6)),
            pltpu.SemaphoreType.DMA((total, 6)),
        ]
        + scratch,
        compiler_params=pltpu.CompilerParams(
            collective_id=0, has_side_effects=True, vmem_limit_bytes=58 * 1024 * 1024
        ),
    )(*sources, small, inputs, buckets, live, lengths)
    weights = [results[4 * layer : 4 * layer + 4] for layer in range(layers)]
    return weights, results[total - 1 : total + 2], results[total + 2 :]


def contract(left, right, left_axis, right_axis):
    return lax.dot_general(
        left, right, (((left_axis,), (right_axis,)), ((), ())),
        preferred_element_type=jnp.float32,
    )


def positions_of(axis):
    return lax.broadcasted_iota(jnp.int32, (WIN, WIN), axis)


def linear_bucket(offset):
    return jnp.clip(offset, -(NB // 2), NB // 2 - 1) + NB // 2


def lane_halves():
    lane = lax.broadcasted_iota(jnp.int32, (1, 2 * DH), 1)
    first = (lane < DH).astype(jnp.float32)
    return first.astype(jnp.bfloat16), (1.0 - first).astype(jnp.bfloat16)


def forward_kernel(layer, *refs):
    forward_core(layer, lambda point: None, *refs)


def forward_core(
    layer, service, x_ref, buckets, live, lengths, all_vectors, up_shifts, table, w_in_hbm,
    w_out_hbm, w_up_hbm, w_down_hbm, out_ref, q_ref, k_ref, v_ref, o_turned, p_ref, low_turned, n1_ref, r1_ref,
    slope_ref, g_turned, n2_ref, r2_ref, x_turned, w_in, w_out, w_up, w_down, allowed, y1, total,
    o_ref, low_ref, sem,
):
    loads = [
        pltpu.make_async_copy(source, target, sem.at[at])
        for at, (source, target) in enumerate(
            ((w_in_hbm, w_in), (w_out_hbm, w_out), (w_up_hbm, w_up), (w_down_hbm, w_down))
        )
    ]
    for load in loads:
        load.start()
    vectors = all_vectors.at[pl.ds(8 * layer, 8)]
    up_shift = up_shifts.at[pl.ds(layer, 1)]
    rows, width = x_ref.shape
    windows = rows // WIN
    row, column = positions_of(0), positions_of(1)
    offset = linear_bucket(column - row)
    first, second = lane_halves()
    for w in range(windows):
        row_doc, column_doc = jnp.zeros_like(row), jnp.zeros_like(column)
        end = 0
        for k in range(lengths.shape[1]):
            end = end + lengths[w, k]
            row_doc = row_doc + (row >= end).astype(jnp.int32)
            column_doc = column_doc + (column >= end).astype(jnp.int32)
        alive = jnp.broadcast_to(live[w : w + 1, :], (WIN, WIN))
        seen = (row_doc == column_doc) & ((alive == 1) | (row == column))
        allowed[w] = seen.astype(jnp.int32)

    loads[0].wait()
    inputs = x_ref[...]
    q_ref[...] = (
        (jnp.dot(inputs, w_in[:, :width], preferred_element_type=jnp.float32) + vectors[0:1, :])
        * DH ** (-0.5)
    ).astype(jnp.bfloat16)
    k_ref[...] = jnp.dot(
        inputs, w_in[:, width : 2 * width], preferred_element_type=jnp.float32
    ).astype(jnp.bfloat16)
    v_ref[...] = (
        jnp.dot(inputs, w_in[:, 2 * width :], preferred_element_type=jnp.float32)
        + vectors[1:2, :]
    ).astype(jnp.bfloat16)
    service(0)

    def attend(w, pair):
        span = pl.ds(w * WIN, WIN)
        lanes = pl.ds(pl.multiple_of(pair * 2 * DH, 2 * DH), 2 * DH)
        queries, keys, values = q_ref[span, lanes], k_ref[span, lanes], v_ref[span, lanes]
        mixed = []
        for side, half in enumerate((first, second)):
            head = pair * 2 + side
            scores = contract(queries * half, keys, 1, 1)
            bias = 0.0
            for kind, index in enumerate((offset, buckets[0, span, :], buckets[1, span, :])):
                entry = table[pl.ds(48 * layer + 16 * kind + head, 1), :]
                entries = jnp.broadcast_to(entry, (WIN, WIN))
                bias = bias + jnp.take_along_axis(
                    entries, index, axis=1, mode="promise_in_bounds"
                )
            scores = jnp.where(allowed[w] == 1, scores + bias, -1e30)
            exponent = jnp.exp(scores - jnp.max(scores, axis=-1, keepdims=True))
            probs = exponent / jnp.sum(exponent, axis=-1, keepdims=True)
            p_ref[w * H + head] = probs
            mixed.append(
                jnp.dot(
                    probs.astype(jnp.bfloat16), values * half, preferred_element_type=jnp.float32
                )
            )
        o_ref[span, lanes] = (mixed[0] + mixed[1]).astype(jnp.bfloat16)

    for w in range(windows):

        @pl.loop(0, H // 4)
        def _(quad, w=w):
            attend(w, quad * 2)
            attend(w, quad * 2 + 1)

        service(1 + w)

    x_turned[...] = jnp.transpose(inputs)
    o_turned[...] = jnp.transpose(o_ref[...])
    loads[1].wait()
    attended = (
        jnp.dot(o_ref[...], w_out[...], preferred_element_type=jnp.float32) + vectors[2:3, :]
    )
    first_norm, normed, inverse = norm_forward(
        inputs.astype(jnp.float32) + attended, vectors[6:7, :], vectors[3:4, :]
    )
    n1_ref[...] = normed
    r1_ref[...] = jnp.broadcast_to(inverse, r1_ref.shape)
    y1[...] = first_norm
    low = first_norm.astype(jnp.bfloat16)
    low_ref[...] = low
    low_turned[...] = jnp.transpose(low)
    total[...] = jnp.zeros_like(total)
    service(1 + windows)
    loads[2].wait()
    loads[3].wait()

    @pl.loop(0, w_up.shape[1] // width)
    def _(at):
        lanes = pl.ds(pl.multiple_of(at * width, width), width)
        hidden = (
            jnp.dot(low_ref[...], w_up[:, lanes], preferred_element_type=jnp.float32)
            + up_shift[:, lanes]
        )
        mass = 0.5 + 0.5 * lax.erf(hidden * 0.5**0.5)
        slope_ref[:, lanes] = mass + hidden * jnp.exp(-0.5 * hidden * hidden) * (
            0.5 / math.pi
        ) ** 0.5
        active = (hidden * mass).astype(jnp.bfloat16)
        g_turned[lanes, :] = jnp.transpose(active)
        total[...] += jnp.dot(active, w_down[lanes, :], preferred_element_type=jnp.float32)

    result, normed, inverse = norm_forward(
        y1[...] + (total[...] + vectors[4:5, :]), vectors[7:8, :], vectors[5:6, :]
    )
    n2_ref[...] = normed
    r2_ref[...] = jnp.broadcast_to(inverse, r2_ref.shape)
    if len(out_ref.shape) == 3:
        out_ref[0] = inputs
        out_ref[1] = result.astype(jnp.bfloat16)
    else:
        out_ref[...] = result.astype(jnp.bfloat16)


def forward_forms(rows, width, hidden):
    low, full = jnp.bfloat16, jnp.float32
    narrow = jax.ShapeDtypeStruct((rows, width), low)
    wide = jax.ShapeDtypeStruct((rows, width), full)
    column = jax.ShapeDtypeStruct((rows, WIN), full)
    turned = jax.ShapeDtypeStruct((width, rows), low)
    outs = [
        narrow, narrow, narrow, narrow, turned,
        jax.ShapeDtypeStruct((rows // WIN * H, WIN, WIN), full),
        turned, wide, column,
        jax.ShapeDtypeStruct((rows, hidden), full),
        jax.ShapeDtypeStruct((hidden, rows), low),
        wide, column, turned,
    ]
    scratch = [
        pltpu.VMEM((width, 3 * width), low), pltpu.VMEM((width, width), low),
        pltpu.VMEM((width, hidden), low), pltpu.VMEM((hidden, width), low),
        pltpu.VMEM((rows // WIN, WIN, WIN), jnp.int32),
        pltpu.VMEM((rows, width), full), pltpu.VMEM((rows, width), full),
        pltpu.VMEM((rows, width), low), pltpu.VMEM((rows, width), low),
        pltpu.SemaphoreType.DMA((4,)),
    ]
    return outs, scratch


def memory_specs():
    return [
        pl.BlockSpec(memory_space=space)
        for space in (
            pltpu.MemorySpace.VMEM, pltpu.MemorySpace.HBM, pltpu.MemorySpace.SMEM
        )
    ]


def forward_layer(layer, inputs, weights, shared, buckets, live, lengths):
    rows, width = inputs.shape
    outs, scratch = forward_forms(rows, width, weights[2].shape[1])
    outs[0] = jax.ShapeDtypeStruct((layer + 1, rows, width), jnp.bfloat16)
    vmem, hbm, smem = memory_specs()
    return pl.pallas_call(
        functools.partial(forward_kernel, layer),
        out_shape=outs,
        in_specs=[vmem, vmem, vmem, smem, vmem, vmem, vmem, hbm, hbm, hbm, hbm],
        out_specs=[vmem] * len(outs),
        scratch_shapes=scratch,
        compiler_params=pltpu.CompilerParams(vmem_limit_bytes=56 * 1024 * 1024),
    )(inputs, buckets, live, lengths, *shared, *weights)


def backward_kernel(
    layer, dz_ref, n2_ref, r2_ref, slope_ref, n1_ref, r1_ref, p_ref, q_ref, k_ref, v_ref,
    all_vectors, w_down_hbm, w_up_hbm, w_out_hbm, w_in_hbm, dx_ref, df_ref, du_ref, da_ref, dqkv_ref,
    small_ref, spread_ref, w_down, w_up, w_out, w_in, small, grad, mixed, spread, sem,
):
    loads = [
        pltpu.make_async_copy(source, target, sem.at[at])
        for at, (source, target) in enumerate(
            ((w_down_hbm, w_down), (w_up_hbm, w_up), (w_out_hbm, w_out), (w_in_hbm, w_in))
        )
    ]
    for load in loads:
        load.start()
    vectors = all_vectors.at[pl.ds(8 * layer, 8)]
    rows, width = dz_ref.shape
    windows = rows // WIN
    first, second = lane_halves()
    small[...] = jnp.zeros_like(small)
    spread[...] = jnp.zeros_like(spread)

    def add_row(at, values):
        small[pl.ds(at, 1), :] = jnp.sum(values, axis=0, keepdims=True)

    def norm_back(incoming, normed, inverse, gain_row):
        scaled = incoming * gain_row
        centred = (
            scaled
            - jnp.mean(scaled, axis=-1, keepdims=True)
            - normed * jnp.mean(scaled * normed, axis=-1, keepdims=True)
        )
        return centred * inverse

    incoming, normed = dz_ref[...], n2_ref[...]
    add_row(7, incoming * normed)
    add_row(5, incoming)
    grad_second = norm_back(incoming, normed, r2_ref[:, 0:1], vectors[7:8, :])
    grad[...] = grad_second
    branch_low = grad_second.astype(jnp.bfloat16)
    df_ref[...] = branch_low
    add_row(4, branch_low.astype(jnp.float32))
    loads[0].wait()
    loads[1].wait()

    @pl.loop(0, w_up.shape[1] // width)
    def _(at):
        lanes = pl.ds(pl.multiple_of(at * width, width), width)
        grad_active = contract(df_ref[...], w_down[lanes, :], 1, 1)
        hidden_low = (grad_active * slope_ref[:, lanes]).astype(jnp.bfloat16)
        du_ref[:, lanes] = hidden_low
        add_row(8 + at, hidden_low.astype(jnp.float32))
        grad[...] += contract(hidden_low, w_up[:, lanes], 1, 1)

    incoming, normed = grad[...], n1_ref[...]
    add_row(6, incoming * normed)
    add_row(3, incoming)
    grad_attended = norm_back(incoming, normed, r1_ref[:, 0:1], vectors[6:7, :])
    grad[...] = grad_attended
    attended_low = grad_attended.astype(jnp.bfloat16)
    da_ref[...] = attended_low
    add_row(2, attended_low.astype(jnp.float32))
    loads[2].wait()
    mixed[...] = contract(attended_low, w_out[...], 1, 1).astype(jnp.bfloat16)

    def attend(w, pair):
        span = pl.ds(w * WIN, WIN)
        start = pl.multiple_of(pair * 2 * DH, 2 * DH)
        lanes = pl.ds(start, 2 * DH)
        queries, keys, values = q_ref[span, lanes], k_ref[span, lanes], v_ref[span, lanes]
        outgoing = mixed[span, lanes]
        sums = [0.0, 0.0, 0.0]
        for side, half in enumerate((first, second)):
            head = pair * 2 + side
            probs = p_ref[w * H + head]
            own = outgoing * half
            grad_probs = contract(own, values, 1, 1)
            centred = grad_probs - jnp.sum(probs * grad_probs, axis=-1, keepdims=True)
            grad_scores = (probs * centred).astype(jnp.bfloat16)
            spread[pl.ds(head, WIN, stride=16), :] = grad_scores.astype(jnp.float32)
            sums[0] += jnp.dot(grad_scores, keys * half, preferred_element_type=jnp.float32)
            sums[1] += contract(grad_scores, queries * half, 0, 0)
            sums[2] += contract(probs.astype(jnp.bfloat16), own, 0, 0)
        scaled = sums[0].astype(jnp.bfloat16).astype(jnp.float32) * DH ** (-0.5)
        dqkv_ref[span, lanes] = scaled.astype(jnp.bfloat16)
        dqkv_ref[span, pl.ds(pl.multiple_of(start + width, 2 * DH), 2 * DH)] = sums[1].astype(
            jnp.bfloat16
        )
        dqkv_ref[span, pl.ds(pl.multiple_of(start + 2 * width, 2 * DH), 2 * DH)] = sums[2].astype(
            jnp.bfloat16
        )

    for w in range(windows):

        @pl.loop(0, H // 4)
        def _(quad, w=w):
            attend(w, quad * 2)
            attend(w, quad * 2 + 1)

        spread_ref[w] = spread[...].astype(jnp.bfloat16)

    loads[3].wait()
    add_row(0, dqkv_ref[:, :width].astype(jnp.float32))
    add_row(1, dqkv_ref[:, 2 * width :].astype(jnp.float32))
    dx_ref[...] = grad[...] + contract(dqkv_ref[...], w_in[...], 1, 1)
    small_ref[...] = small[...].astype(jnp.bfloat16)


def backward_layer(layer, incoming, weights, vectors, kept):
    w_in, w_out, w_up, w_down = weights
    rows, width = incoming.shape
    hidden = w_up.shape[1]
    low, full = jnp.bfloat16, jnp.float32
    narrow = jax.ShapeDtypeStruct((rows, width), low)
    vmem, hbm, _ = memory_specs()
    q, k, v, _, p, _, n1, r1, slope, _, n2, r2, _ = kept
    return pl.pallas_call(
        functools.partial(backward_kernel, layer),
        out_shape=[
            jax.ShapeDtypeStruct((rows, width), full),
            narrow,
            jax.ShapeDtypeStruct((rows, hidden), low),
            narrow,
            jax.ShapeDtypeStruct((rows, 3 * width), low),
            jax.ShapeDtypeStruct((64, width), low),
            jax.ShapeDtypeStruct((rows // WIN, WIN * 16, WIN), low),
        ],
        in_specs=[vmem] * 11 + [hbm] * 4,
        out_specs=[vmem] * 7,
        scratch_shapes=[
            pltpu.VMEM(w_down.shape, low), pltpu.VMEM(w_up.shape, low),
            pltpu.VMEM(w_out.shape, low), pltpu.VMEM(w_in.shape, low),
            pltpu.VMEM((64, width), full), pltpu.VMEM((rows, width), full),
            pltpu.VMEM((rows, width), low), pltpu.VMEM((WIN * 16, WIN), full),
            pltpu.SemaphoreType.DMA((4,)),
        ],
        compiler_params=pltpu.CompilerParams(vmem_limit_bytes=56 * 1024 * 1024),
    )(incoming, n2, r2, slope, n1, r1, p, q, k, v, vectors, w_down, w_up, w_out, w_in)


def local(
    tokens,
    out_grad,
    mlm_mask,
    live_mask,
    doc_lengths,
    layout_buckets,
    attn_in,
    attn_out,
    ffn_in,
    ffn_out,
    biases,
    ffn_in_bias,
    gains,
    tables,
):
    shards = lax.axis_size("fsdp")
    live = live_mask.reshape(-1, WIN)
    weights_list, shared, first = open_layers(
        (attn_in, attn_out, ffn_in, ffn_out), small_rows(biases, ffn_in_bias, gains, tables),
        shards, tokens, layout_buckets, live, doc_lengths,
    )
    current, *kept = first
    outputs, *kept_next = forward_layer(
        1, current, weights_list[1], shared, layout_buckets, live, doc_lengths
    )
    kept_list = [kept, kept_next]
    incoming = out_grad.astype(jnp.float32) * mlm_mask.astype(jnp.float32)[:, None]
    lefts, rights, smalls, spreads = [], [], [], []
    for layer in reversed(range(len(weights_list))):
        kept = kept_list[layer]
        incoming, df, du, da, dqkv, small, spread = backward_layer(
            layer, incoming, weights_list[layer], shared[0], kept
        )
        lefts = [kept[12], kept[3], kept[5], kept[9]] + lefts
        rights = [dqkv, da, du, df] + rights
        smalls = [small] + smalls
        spreads = [spread] + spreads
    summed = sum_gradients(
        lefts, rights, smalls, spreads, layout_buckets, shards, lax.axis_size("dp")
    )
    return (outputs, incoming) + summed


def solution(mesh):
    return jax.shard_map(
        local,
        mesh=mesh,
        in_specs=(
            P(("dp", "fsdp"), None),
            P(("dp", "fsdp"), None),
            P(("dp", "fsdp")),
            P(("dp", "fsdp")),
            P(("dp", "fsdp"), None),
            P(None, ("dp", "fsdp"), None),
            P(None, "fsdp", None),
            P(None, "fsdp", None),
            P(None, "fsdp", None),
            P(None, "fsdp", None),
            P(None, None, "fsdp"),
            P(None, "fsdp"),
            P(None, None, "fsdp"),
            P(None, None, "fsdp", None),
        ),
        out_specs=(
            P(None, ("dp", "fsdp"), None),
            P(("dp", "fsdp"), None),
            P(None, "fsdp", None),
            P(None, "fsdp", None),
            P(None, "fsdp", None),
            P(None, "fsdp", None),
            P(None, None, "fsdp"),
            P(None, "fsdp"),
            P(None, None, "fsdp"),
            P(None, None, "fsdp", None),
        ),
        check_vma=False,
    )
```
